256 devices in a mesh: img: 8 (over y, x_lo), cls: 8 (over z), emb: 4 (over x_hi, core).
Axes of the slice: x: 4 (x_hi: 2, x_lo: 2; x = x_hi * 2 + x_lo), y: 4, z: 8, core: 2. Of those that a mesh axis runs over, the one named last changes fastest.
Arguments:
- regions: bfloat16 [8192, 1024], P('img', 'emb'), may hold values from -8 to 8
- table: bfloat16 [21504, 1024], P('cls', 'emb'), may hold values from -1 to 1
- shift: float32 [8192], P('img'), may hold values from -0.5 to 0.1
- scale: float32 [8192], P('img'), may hold values from 2 to 20
- labels: int32 [8192], P('img'), may hold values from -1 to 21503, as said below
- valid: int32 [16, 21504], P('img', 'cls'), may hold values 0 or 1
Outputs:
- loss: float32 [], replicated
- region_grad: bfloat16 [8192, 1024], P('img', 'emb')
- table_grad: bfloat16 [21504, 1024], P('cls', 'emb')
The draws below stay inside these ranges and needn't reach their ends.
Inputs may be any that keep to these rules, and one draw needn't show every extreme that they name: `labels`: -1 marks background; the first region of every image is foreground.
All inputs are finite; a program needn't handle non-finite values. No bound on the sum of `valid` on one device may be relied on, other than what follows from the above.
Results may differ from the reference program's by a relative error of at most 0.0034.
Values may be sent and summed in bfloat16 or wider, within the bound.
No kernel may reach another device: no remote copies, remote signals or barrier semaphores. Data moves between devices by JAX's collectives and lax.ppermute only.
A program may use at most 64 MiB of HBM per device.

```python
import math
import jax
import jax.numpy as jnp
from jax import lax

D = 1024
CLASSES = 21504
REG_IMG = 512
IMG_DEV = 2
IMAGES = 16
REGIONS = 8192


cluster_count = 64


def make_labels(key):
    key_fg = jax.random.fold_in(key, 11)
    key_cls = jax.random.fold_in(key, 23)
    position = jnp.arange(REGIONS, dtype=jnp.int32)
    image = position // REG_IMG
    within = position % REG_IMG
    threshold = 150 + 350 * image // max(IMAGES - 1, 1)
    roll = jax.random.randint(key_fg, (REGIONS,), 0, 1000, dtype=jnp.int32)
    chosen = jax.random.randint(key_cls, (REGIONS,), 0, CLASSES, dtype=jnp.int32)
    foreground = (roll < threshold) | (within == 0)
    return jnp.where(foreground, chosen, -1).astype(jnp.int32)


def make_table(key):
    key_dir = jax.random.fold_in(key, 41)
    key_own = jax.random.fold_in(key, 43)
    directions = jax.random.normal(key_dir, (cluster_count, D), jnp.float32)
    directions = directions * lax_rsqrt(jnp.sum(directions * directions, axis=1, keepdims=True))
    own = jax.random.normal(key_own, (CLASSES, D), jnp.float32)
    mixing = 0.6
    own = own * lax_rsqrt(jnp.sum(own * own, axis=1, keepdims=True))
    cluster = jnp.arange(CLASSES, dtype=jnp.int32) % cluster_count
    shared = directions[cluster]
    mixed = mixing * shared + (1.0 - mixing * mixing) ** 0.5 * own
    mixed = mixed * lax_rsqrt(jnp.sum(mixed * mixed, axis=1, keepdims=True))
    return (mixed, directions)


def lax_rsqrt(value):
    return 1.0 / jnp.sqrt(value)


def draw_labels(key, part):
    return make_labels(key)


def draw_table(key, part):
    mixed, directions = make_table(key)
    return jnp.clip(mixed, -1.0, 1.0).astype(jnp.bfloat16)


def draw_regions(key, part):
    labels = make_labels(key)
    mixed, directions = make_table(key)
    foreground = labels >= 0
    safe_labels = jnp.maximum(labels, 0)
    background = jax.random.randint(jax.random.fold_in(key, 31), (REGIONS,), 0, cluster_count, dtype=jnp.int32)
    aim = jnp.where(foreground[:, None], mixed[safe_labels], directions[background])
    key_str = jax.random.fold_in(key, 53)
    key_noise = jax.random.fold_in(key, 59)
    key_mag = jax.random.fold_in(key, 61)
    strength = jax.random.uniform(key_str, (REGIONS, 1), jnp.float32, 0.5, 1.2)
    noise = jax.random.normal(key_noise, (REGIONS, D), jnp.float32)
    magnitude = jnp.exp(jax.random.uniform(key_mag, (REGIONS, 1), jnp.float32, -1.386, 0.0))
    region = magnitude * (strength * aim * D ** 0.5 + noise)
    return jnp.clip(region, -8.0, 8.0).astype(jnp.bfloat16)


def place_ends(drawn, own_key, least, largest):
    extent = drawn.shape
    index_at = [jax.random.randint(jax.random.fold_in(own_key, axis), (), 0, extent[axis]) for axis in range(len(extent))]
    drawn = drawn.at[tuple(index_at)].set(least)
    longest = extent.index(max(extent))
    index_at[longest] = (index_at[longest] + 1) % extent[longest]
    return drawn.at[tuple(index_at)].set(largest)


def steps_of(stream_key, shape, cuts, least, top_value):
    def one(dim, parts):
        heights = jax.random.uniform(jax.random.fold_in(jax.random.fold_in(stream_key, 6), dim), (parts,), jnp.float32, least / len(cuts), top_value / len(cuts))
        return jnp.repeat(jnp.exp(heights), shape[dim] // parts).reshape((-1,) + (1,) * (len(shape) - dim - 1))

    factor_of = one(*cuts[0])
    for cut in cuts[1:]:
        factor_of = factor_of * one(*cut)
    return factor_of


def setup_inputs(seed: int = 0) -> dict:
    key_list = jax.random.split(jax.random.key(seed), 7)
    regions = draw_regions(jax.random.fold_in(key_list[6], 71), 0)
    table = draw_table(jax.random.fold_in(key_list[6], 71), 0)
    shift = jnp.clip(-0.5 + 0.6 * jax.random.uniform(key_list[2], (REGIONS,), jnp.float32) ** steps_of(key_list[2], (REGIONS,), ((0, 8),), -0.2, 0.2), -0.5, 0.1)
    scale = jnp.clip(jnp.exp(math.log(20.0) - 2.3025851 * jax.random.uniform(key_list[3], (REGIONS,), jnp.float32) ** steps_of(key_list[3], (REGIONS,), ((0, 8),), -0.2, 0.2)), 2.0, 20.0)
    labels = draw_labels(jax.random.fold_in(key_list[6], 71), 0)
    valid = place_ends((jax.random.randint(key_list[5], (IMAGES, CLASSES), 0, 4) < 3).astype(jnp.int32), jax.random.fold_in(key_list[5], 1), 0, 1)
    return dict(regions=regions, table=table, shift=shift, scale=scale, labels=labels, valid=valid)


def focal(logit, target):
    prob = jax.nn.sigmoid(logit)
    return -0.25 * target * (1.0 - prob) ** 2 * jax.nn.log_sigmoid(logit) - 0.75 * (1.0 - target) * prob ** 2 * jax.nn.log_sigmoid(-logit)

def reference(regions, table, shift, scale, labels, valid):
    rows = IMG_DEV * REG_IMG
    blocks = REGIONS // rows
    count = jnp.sum((labels >= 0).astype(jnp.float32))
    factor = REGIONS / count
    class_ids = jnp.arange(CLASSES, dtype=jnp.int32)

    def step(carry, index):
        total, table_acc = carry
        start = (index * rows).astype(jnp.int32)
        block = lax.dynamic_slice_in_dim(regions, start, rows, 0).astype(jnp.float32)
        inv = lax.rsqrt(lax.optimization_barrier(jnp.sum(block * block, axis=1)) + 1e-06)
        unit = block * inv[:, None]
        unit_b = unit.astype(jnp.bfloat16)
        cosine = jnp.dot(unit_b, table.T, preferred_element_type=jnp.float32)
        shift_b = lax.dynamic_slice_in_dim(shift, start, rows, 0)
        scale_b = lax.dynamic_slice_in_dim(scale, start, rows, 0)
        label_b = lax.dynamic_slice_in_dim(labels, start, rows, 0)
        valid_b = lax.dynamic_slice_in_dim(valid, (index * IMG_DEV).astype(jnp.int32), IMG_DEV, 0).astype(jnp.float32)
        image_ids = jnp.arange(rows, dtype=jnp.int32) // REG_IMG
        onehot = (image_ids[:, None] == jnp.arange(IMG_DEV, dtype=jnp.int32)[None, :]).astype(jnp.float32)
        mask = jnp.dot(onehot, valid_b, preferred_element_type=jnp.float32)
        logit = (cosine + shift_b[:, None]) * scale_b[:, None]
        target = (label_b[:, None] == class_ids[None, :]).astype(jnp.float32)
        term, pullback = jax.vjp(lambda value: focal(value, target), logit)
        dlogit = pullback(jnp.ones_like(term))[0]
        total = total + jnp.sum(term * mask)
        dscore = (dlogit * mask * scale_b[:, None] * factor).astype(jnp.bfloat16)
        dunit = jnp.dot(dscore, table, preferred_element_type=jnp.float32)
        radial = lax.optimization_barrier(jnp.sum(unit * dunit, axis=1))
        grad_b = (inv[:, None] * (dunit - unit * radial[:, None])).astype(jnp.bfloat16)
        table_acc = table_acc + jnp.dot(dscore.T, unit_b, preferred_element_type=jnp.float32)
        return ((total, table_acc), grad_b)
    init = (jnp.zeros((), jnp.float32), jnp.zeros((CLASSES, D), jnp.float32))
    (total, table_acc), grads = lax.scan(step, init, jnp.arange(blocks, dtype=jnp.int32))
    loss = total / count / CLASSES
    return (loss, grads.reshape(REGIONS, D), table_acc.astype(jnp.bfloat16))
```

```python
import functools

import jax
import jax.numpy as jnp
from jax import lax
from jax.experimental import pallas as pl
from jax.experimental.pallas import tpu as pltpu
from jax.sharding import Mesh
from jax.sharding import PartitionSpec as P

CLASSES = 21504
REGIONS = 8192
EMB = ("emb_0", "emb_1")
IMG = ("img_0", "img_1")
F32 = jnp.float32
BF16 = jnp.bfloat16
NT = (((1,), (1,)), ((), ()))
TN = (((0,), (0,)), ((), ()))


def vmem(n):
    return [pl.BlockSpec(memory_space=pltpu.VMEM)] * n


def params():
    return pltpu.CompilerParams(vmem_limit_bytes=56 * 1024 * 1024)


def swap(x, axis):
    return lax.ppermute(x, axis, [(0, 1), (1, 0)])


def split3(value):
    hi = value.astype(BF16).astype(F32)
    mid = (value - hi).astype(BF16).astype(F32)
    lo = value - hi - mid
    lane = lax.broadcasted_iota(jnp.int32, (8, 256), 1)
    row = lax.broadcasted_iota(jnp.int32, (8, 256), 0)
    packed = jnp.where(lane == 0, hi, jnp.where(lane == 1, mid, jnp.where(lane == 2, lo, 0.0)))
    return jnp.where(row == 0, packed, 0.0)


def unit_kernel(a, b, c, d, out):
    blocks = [r[...].astype(F32) for r in (a, b, c, d)]
    squares = sum(jnp.sum(v * v, axis=1, keepdims=True) for v in blocks)
    inv = lax.rsqrt(squares + 1e-06)
    for q, v in enumerate(blocks):
        out[:, 256 * q : 256 * q + 256] = (v * inv).astype(BF16)


def make_unit(blocks):
    rows = blocks[0].shape[0]
    tile = 256
    return pl.pallas_call(
        unit_kernel,
        grid=(rows // tile,),
        in_specs=[pl.BlockSpec((tile, 256), lambda i: (i, 0))] * 4,
        out_specs=pl.BlockSpec((tile, 1024), lambda i: (i, 0)),
        out_shape=jax.ShapeDtypeStruct((rows, 1024), BF16),
        compiler_params=params(),
    )(*blocks)


def focal_kernel(s, t0, t1, t2, t3, unit, lane_f, labels, mask, dscore, loss):
    i = pl.program_id(0)
    tile = t0.shape[0]
    rows = unit.shape[0]
    cosine = sum(
        lax.dot_general(t[...], unit[:, 256 * q : 256 * q + 256], NT, preferred_element_type=F32)
        for q, t in enumerate((t0, t1, t2, t3))
    )
    logit = (cosine + lane_f[0:1, :]) * lane_f[1:2, :]
    ids = s[1] + i * tile + lax.broadcasted_iota(jnp.int32, (tile, rows), 0)
    target = labels[...] == ids
    m = jnp.where(target, -logit, logit)
    e = jnp.exp(-jnp.abs(m))
    r = 1.0 / (1.0 + e)
    er = e * r
    positive = m >= 0.0
    prob = jnp.where(positive, r, er)
    rest = jnp.where(positive, er, r)
    series = e * (1.0 - e * (0.5 - e * (1.0 / 3.0 - e * 0.25)))
    soft = jnp.maximum(m, 0.0) + jnp.where(e < 2e-3, series, jnp.log(1.0 + e))
    half = rows // 2
    column = lax.broadcasted_iota(jnp.int32, (tile, rows), 1)
    on = jnp.where(column < half, mask[:, 0:1], mask[:, 1:2])
    weight = jnp.where(target, 0.25, 0.75) * on * prob * prob
    slope = weight * (2.0 * rest * soft + prob)
    slope = jnp.where(target, -slope, slope)
    dscore[...] = (slope * lane_f[2:3, :]).astype(BF16)
    term = weight * soft

    @pl.when(i == 0)
    def _():
        loss[...] = jnp.zeros_like(loss)

    loss[...] += jnp.sum(term.reshape(tile // 8, 8, rows), axis=0)


def make_focal(scalars, tables, unit, lane_f, labels, mask):
    rows = unit.shape[0]
    classes = mask.shape[0]
    tile = 96
    steps = classes // tile
    whole = lambda i, s: (0, 0)
    return pl.pallas_call(
        focal_kernel,
        grid_spec=pltpu.PrefetchScalarGridSpec(
            num_scalar_prefetch=1,
            grid=(steps,),
            in_specs=[pl.BlockSpec((tile, 256), lambda i, s: (s[0] * steps + i, 0))] * 4
            + [
                pl.BlockSpec((rows, 1024), whole),
                pl.BlockSpec((8, rows), whole),
                pl.BlockSpec((1, rows), whole),
                pl.BlockSpec((tile, 2), lambda i, s: (i, 0)),
            ],
            out_specs=[
                pl.BlockSpec((tile, rows), lambda i, s: (i, 0)),
                pl.BlockSpec((8, rows), whole),
            ],
        ),
        out_shape=[
            jax.ShapeDtypeStruct((classes, rows), BF16),
            jax.ShapeDtypeStruct((8, rows), F32),
        ],
        compiler_params=params(),
    )(scalars, *tables, unit, lane_f, labels, mask)


def table_kernel(dscore, unit, loss, out):
    acc = jnp.dot(dscore[...], unit[...], preferred_element_type=F32)
    extra = split3(jnp.sum(loss[...]))
    for j in range(8):
        size = min(88, acc.shape[0] - 88 * j)
        part = acc[88 * j : 88 * j + size]
        if size < 88:
            part = jnp.concatenate([part, jnp.zeros((88 - size, part.shape[1]), F32)], axis=0)
        out[j] = jnp.concatenate([part, extra], axis=0).astype(BF16)


def make_table(dscore, unit, loss):
    classes, rows = dscore.shape
    return pl.pallas_call(
        table_kernel,
        grid=(4,),
        in_specs=[
            pl.BlockSpec((classes, rows), lambda i: (0, 0)),
            pl.BlockSpec((rows, 256), lambda i: (0, i)),
            pl.BlockSpec((8, rows), lambda i: (0, 0)),
        ],
        out_specs=pl.BlockSpec((8, 96, 256), lambda i: (0, 0, i)),
        out_shape=jax.ShapeDtypeStruct((8, 96, 1024), BF16),
        compiler_params=params(),
    )(dscore, unit, loss)


def region_kernel(s, own, other, t0, t1, t2, t3, *refs):
    outs, acc = refs[:8], refs[8]
    k = s[0]
    z = s[2]
    half = other.shape[0]
    mine = own[...]
    theirs = other[...]
    mine_at = pl.multiple_of(k * half, 32)
    theirs_at = pl.multiple_of((1 - k) * half, 32)
    for q, t in enumerate((t0, t1, t2, t3)):
        acc[:, 256 * q : 256 * q + 256] = lax.dot_general(
            mine, t[pl.ds(mine_at, half), :], TN, preferred_element_type=F32
        ) + lax.dot_general(theirs, t[pl.ds(theirs_at, half), :], TN, preferred_element_type=F32)
    for d in range(8):
        at = pl.multiple_of(64 * ((z + d) % 8), 64)
        outs[d][...] = acc[pl.ds(at, 64), :].astype(BF16)


def make_region(scalars, own, other, tables):
    return pl.pallas_call(
        region_kernel,
        in_specs=[pl.BlockSpec(memory_space=pltpu.SMEM)] + vmem(6),
        out_specs=vmem(8),
        out_shape=[jax.ShapeDtypeStruct((64, 1024), BF16)] * 8,
        scratch_shapes=[pltpu.VMEM((512, 1024), F32)],
        compiler_params=params(),
    )(scalars, own, other, *tables)


def merge_kernel(s, a, b, c, d, tables, *refs):
    terms, out = refs[:8], refs[8]
    e = s[3]
    blocks = [r[...].astype(F32) for r in (a, b, c, d)]
    squares = sum(jnp.sum(v * v, axis=1, keepdims=True) for v in blocks)
    inv = lax.rsqrt(squares + 1e-06)
    dunit = sum(t[...].astype(F32) for t in terms)
    units = [v * inv for v in blocks]
    radial = sum(
        jnp.sum(u * dunit[:, 256 * q : 256 * q + 256], axis=1, keepdims=True)
        for q, u in enumerate(units)
    )
    total = sum(tables[j].astype(F32) for j in range(8))
    loss = jnp.sum(total[88:89, 0:3])
    extra = split3(loss).astype(BF16)
    for q, u in enumerate(units):
        cols = slice(256 * q, 256 * q + 256)
        grad = inv * (dunit[:, cols] - u * radial)
        to = e ^ q
        out[to, 0:64, :] = grad.astype(BF16)
        out[to, 64:152, :] = total[0:88, cols].astype(BF16)
        out[to, 152:160, :] = extra


def make_merge(scalars, blocks, tables, terms):
    return pl.pallas_call(
        merge_kernel,
        grid_spec=pltpu.PrefetchScalarGridSpec(
            num_scalar_prefetch=1,
            grid=(1,),
            in_specs=[pl.BlockSpec((64, 256), lambda i, s: (s[0] * 8 + s[2], 0))] * 4
            + [pl.BlockSpec((8, 96, 1024), lambda i, s: (0, 0, 0))]
            + [pl.BlockSpec((64, 1024), lambda i, s: (0, 0))] * 8,
            out_specs=pl.BlockSpec((4, 160, 256), lambda i, s: (0, 0, 0)),
        ),
        out_shape=jax.ShapeDtypeStruct((4, 160, 256), BF16),
        compiler_params=params(),
    )(scalars, *blocks, tables, *terms)


def share_kernel(pieces, region, table):
    for k in range(2):
        both = pieces[k, 0:64, :].astype(F32) + pieces[2 + k, 0:64, :].astype(F32)
        region[64 * k : 64 * k + 64, :] = both.astype(BF16)
    loss = sum(jnp.sum(pieces[e, 152:160, :].astype(F32)) for e in range(4))
    region[128:136, :] = split3(loss).astype(BF16)
    for j in range(8):
        for e in range(4):
            table[j, e] = pieces[e, 64:152, :]


def make_share(pieces):
    return pl.pallas_call(
        share_kernel,
        in_specs=vmem(1),
        out_specs=vmem(2),
        out_shape=[
            jax.ShapeDtypeStruct((136, 256), BF16),
            jax.ShapeDtypeStruct((8, 4, 88, 256), BF16),
        ],
        compiler_params=params(),
    )(pieces)


def final_kernel(s, tables, *refs):
    regions, (region_out, table_out, loss_out) = refs[:8], refs[8:]
    z = s[2]
    total = jnp.zeros((1, 1), F32)
    for d in range(8):
        source = (z + 8 - d) % 8
        for k in range(2):
            region_out[k, source] = regions[d][64 * k : 64 * k + 64, :]
        total += jnp.sum(regions[d][128:136, :].astype(F32), keepdims=True)
    loss_out[...] = jnp.broadcast_to(total, loss_out.shape)
    for e in range(4):
        for j in range(8):
            size = min(88, 672 - 88 * j)
            at = 672 * e + 88 * j
            table_out[at : at + size, :] = tables[j, e, 0:size, :]


def make_final(scalars, tables, regions):
    return pl.pallas_call(
        final_kernel,
        in_specs=[pl.BlockSpec(memory_space=pltpu.SMEM)] + vmem(9),
        out_specs=vmem(3),
        out_shape=[
            jax.ShapeDtypeStruct((2, 8, 64, 256), BF16),
            jax.ShapeDtypeStruct((2688, 256), BF16),
            jax.ShapeDtypeStruct((8, 128), F32),
        ],
        compiler_params=params(),
    )(scalars, tables, *regions)


def along_cls(x, distance):
    return lax.ppermute(x, "cls", [(i, (i + distance) % 8) for i in range(8)])


def shards(regions, table, shift, scale, labels, valid):
    rows = regions.shape[0]
    xh = lax.axis_index("emb_0")
    k = lax.axis_index("emb_1")
    z = lax.axis_index("cls")
    j = lax.axis_index(IMG)
    e = 2 * xh + k
    scalars = jnp.stack([k, z * 2688 + e * 672, z, e]).astype(jnp.int32)

    t_send = lax.dynamic_slice_in_dim(table, (1 - xh) * 1344 + 168 * j, 168, 0)
    t_got = swap(t_send, "emb_0")
    t_own = lax.dynamic_slice_in_dim(table, xh * 1344, 1344, 0)
    local = jnp.sum((labels >= 0).astype(F32))
    high = jnp.floor(local / 32.0)
    lane = lax.broadcasted_iota(jnp.int32, (8, 256), 1)
    extra = jnp.where(lane == 0, high, jnp.where(lane == 1, local - 32.0 * high, 0.0)).astype(BF16)
    message = jnp.concatenate([t_got, extra], axis=0)
    t_all = lax.all_to_all(
        jnp.broadcast_to(message, (8, 176, 256)), IMG, split_axis=0, concat_axis=0, tiled=True
    )
    t_far = t_all[:, :168].reshape(1344, 256)
    count = jnp.sum(t_all[:, 168, 0].astype(F32) * 32.0 + t_all[:, 168, 1].astype(F32))
    r_far = swap(regions, "emb_0")
    r_near = swap(regions, "emb_1")
    r_both = swap(r_far, "emb_1")
    t_near = swap(t_own, "emb_1")
    t_both = swap(t_far, "emb_1")
    blocks = (regions, r_near, r_far, r_both)
    tables = (t_own, t_near, t_far, t_both)
    unit = make_unit(blocks)

    factor = REGIONS / count
    zero = jnp.zeros((5, rows), F32)
    lane_f = jnp.concatenate([shift[None], scale[None], (scale * factor)[None], zero], axis=0)
    mask = lax.dynamic_slice_in_dim(valid, e * 672, 672, 1).astype(F32).T
    dscore, loss = make_focal(scalars, tables, unit, lane_f, labels[None], mask)

    mine = lax.dynamic_slice_in_dim(dscore, k * 512, 512, 1)
    theirs = swap(lax.dynamic_slice_in_dim(dscore, (1 - k) * 512, 512, 1), "emb_1")
    table_terms = lax.all_to_all(
        make_table(dscore, unit, loss), IMG, split_axis=0, concat_axis=0, tiled=True
    )
    chunks = make_region(scalars, mine, theirs, tables)
    terms = [chunks[0]] + [along_cls(chunks[d], d) for d in range(1, 8)]
    merged = make_merge(scalars, blocks, table_terms, terms)
    pieces = lax.all_to_all(merged, EMB, split_axis=0, concat_axis=0, tiled=True)
    region_share, table_share = make_share(pieces)
    table_all = lax.all_to_all(
        table_share, IMG, split_axis=0, concat_axis=0, tiled=True
    )
    region_all = [region_share] + [along_cls(region_share, d) for d in range(1, 8)]
    region_grad, table_grad, total = make_final(scalars, table_all, region_all)
    return (total[0, 0] / count / CLASSES, region_grad.reshape(rows, 256), table_grad)


def solution(mesh):
    torus = Mesh(
        mesh.devices.reshape(4, 2, mesh.shape["cls"], 2, 2),
        ("img_0", "img_1", "cls", "emb_0", "emb_1"),
    )
    return jax.shard_map(
        shards,
        mesh=torus,
        in_specs=(P(IMG, EMB), P("cls", EMB), P(IMG), P(IMG), P(IMG), P(IMG, "cls")),
        out_specs=(P(), P(IMG, EMB), P("cls", EMB)),
        check_vma=False,
    )
```

```python
import jax
import jax.numpy as jnp
from jax import lax
from jax.experimental import pallas as pl
from jax.experimental.pallas import tpu as pltpu
from jax.sharding import Mesh
from jax.sharding import PartitionSpec as P

CLASSES = 21504
REGIONS = 8192
EMB = ("emb_0", "emb_1")
IMG = ("img_0", "img_1")
CLS = ("cls_0", "cls_1")
NEAR = ("cls_1", "emb_0", "emb_1")
F32 = jnp.float32
BF16 = jnp.bfloat16
NT = (((1,), (1,)), ((), ()))
TN = (((0,), (0,)), ((), ()))

K, BASE, E, Y, XL, ZH = range(6)


def vmem(n):
    return [pl.BlockSpec(memory_space=pltpu.VMEM)] * n


def smem():
    return pl.BlockSpec(memory_space=pltpu.SMEM)


def params():
    return pltpu.CompilerParams(vmem_limit_bytes=16 * 1024 * 1024)


def cost(flops):
    return pl.CostEstimate(flops=int(flops), bytes_accessed=1 << 20, transcendentals=0)


def swap(x, axis):
    return lax.ppermute(x, axis, [(0, 1), (1, 0)])


def split3(value, width):
    hi = value.astype(BF16).astype(F32)
    mid = (value - hi).astype(BF16).astype(F32)
    lo = value - hi - mid
    lane = lax.broadcasted_iota(jnp.int32, (8, width), 1)
    row = lax.broadcasted_iota(jnp.int32, (8, width), 0)
    packed = jnp.where(lane == 0, hi, jnp.where(lane == 1, mid, jnp.where(lane == 2, lo, 0.0)))
    return jnp.where(row == 0, packed, 0.0)


def unit_kernel(a, b, c, d, out, scale):
    blocks = [r[...].astype(F32) for r in (a, b, c, d)]
    squares = sum(jnp.sum(v * v, axis=1, keepdims=True) for v in blocks)
    inv = lax.rsqrt(squares + 1e-06)
    scale[...] = jnp.broadcast_to(inv, scale.shape)
    for q, v in enumerate(blocks):
        out[:, 256 * q : 256 * q + 256] = (v * inv).astype(BF16)


def make_unit(blocks):
    rows = blocks[0].shape[0]
    tile = 256
    return pl.pallas_call(
        unit_kernel,
        grid=(rows // tile,),
        in_specs=[pl.BlockSpec((tile, 256), lambda i: (i, 0))] * 4,
        out_specs=[
            pl.BlockSpec((tile, 1024), lambda i: (i, 0)),
            pl.BlockSpec((tile, 128), lambda i: (i, 0)),
        ],
        out_shape=[
            jax.ShapeDtypeStruct((rows, 1024), BF16),
            jax.ShapeDtypeStruct((rows, 128), F32),
        ],
        compiler_params=params(),
        cost_estimate=cost(2e7),
        name="unit",
    )(*blocks)


def focal_kernel(s, t0, t1, t2, t3, unit, lane_f, labels, mask, dscore, loss, acc):
    i = pl.program_id(0)
    tile = t0.shape[0]
    rows = unit.shape[0]
    acc[...] = sum(
        lax.dot_general(t[...], unit[:, 256 * q : 256 * q + 256], NT, preferred_element_type=F32)
        for q, t in enumerate((t0, t1, t2, t3))
    )
    shift = lane_f[0:1, :]
    scale = lane_f[1:2, :]
    factor = lane_f[2:3, :]
    wanted = labels[...] - (s[BASE] + i * tile)
    step = 16

    def body(g, total):
        at = pl.multiple_of(g * step, step)
        logit = (acc[pl.ds(at, step), :] + shift) * scale
        ids = lax.broadcasted_iota(jnp.int32, (step, rows), 0)
        target = (wanted - at) == ids
        m = jnp.where(target, -logit, logit)
        e = jnp.exp(-jnp.abs(m))
        r = 1.0 / (1.0 + e)
        er = e * r
        positive = m >= 0.0
        prob = jnp.where(positive, r, er)
        rest = jnp.where(positive, er, r)
        series = e * (1.0 - e * (0.5 - e * (1.0 / 3.0 - e * 0.25)))
        soft = jnp.maximum(m, 0.0) + jnp.where(e < 2e-3, series, jnp.log(1.0 + e))
        weight = jnp.where(target, 0.25, 0.75) * mask[pl.ds(at, step), :] * (prob * prob)
        slope = weight * (2.0 * rest * soft + prob)
        slope = jnp.where(target, -slope, slope)
        dscore[pl.ds(at, step), :] = (slope * factor).astype(BF16)
        term = weight * soft
        return total + term[0:8, :] + term[8:16, :]

    total = lax.fori_loop(0, tile // step, body, jnp.zeros((8, rows), F32))

    @pl.when(i == 0)
    def _():
        loss[...] = jnp.zeros_like(loss)

    loss[...] += total


def make_focal(scalars, tables, unit, lane_f, labels, mask):
    rows = unit.shape[0] // 2
    classes = mask.shape[0]
    tile = 192
    whole = lambda i, s: (0, 0)
    return pl.pallas_call(
        focal_kernel,
        grid_spec=pltpu.PrefetchScalarGridSpec(
            num_scalar_prefetch=1,
            grid=(classes // tile,),
            in_specs=[pl.BlockSpec((tile, 256), lambda i, s: (i, 0))] * 4
            + [
                pl.BlockSpec((rows, 1024), lambda i, s: (s[K], 0)),
                pl.BlockSpec((8, rows), lambda i, s: (0, s[K])),
                pl.BlockSpec((1, rows), lambda i, s: (0, s[K])),
                pl.BlockSpec((tile, 1), lambda i, s: (i, 0)),
            ],
            out_specs=[
                pl.BlockSpec((tile, rows), lambda i, s: (i, 0)),
                pl.BlockSpec((8, rows), whole),
            ],
            scratch_shapes=[pltpu.VMEM((tile, rows), F32)],
        ),
        out_shape=[
            jax.ShapeDtypeStruct((classes, rows), BF16),
            jax.ShapeDtypeStruct((8, rows), F32),
        ],
        compiler_params=params(),
        cost_estimate=cost(1.4e9),
        name="focal",
    )(scalars, *tables, unit, lane_f, labels, mask)


def region_kernel(s, dscore, t0, t1, t2, t3, a, b, c, d, inv_ref, out, acc):
    inv = inv_ref[:, 0:1]
    ds = dscore[...]
    along = 0.0
    for q, (t, r) in enumerate(zip((t0, t1, t2, t3), (a, b, c, d))):
        part = lax.dot_general(ds, t[...], TN, preferred_element_type=F32)
        acc[:, 256 * q : 256 * q + 256] = part
        along += jnp.sum(part * r[...].astype(F32), axis=1, keepdims=True)
    back = inv * inv * along
    for q, r in enumerate((a, b, c, d)):
        cols = slice(256 * q, 256 * q + 256)
        grad = inv * (acc[:, cols] - r[...].astype(F32) * back)
        out[:, :, cols] = grad.reshape(out.shape[0], 64, 256).astype(BF16)


def make_region(scalars, dscore, tables, blocks, inv):
    classes, rows = dscore.shape
    tile = 128
    steps = rows // tile
    return pl.pallas_call(
        region_kernel,
        grid_spec=pltpu.PrefetchScalarGridSpec(
            num_scalar_prefetch=1,
            grid=(steps,),
            in_specs=[pl.BlockSpec((classes, tile), lambda i, s: (0, i))]
            + [pl.BlockSpec((classes, 256), lambda i, s: (0, 0))] * 4
            + [pl.BlockSpec((tile, 256), lambda i, s: (s[K] * steps + i, 0))] * 4
            + [pl.BlockSpec((tile, 128), lambda i, s: (s[K] * steps + i, 0))],
            out_specs=pl.BlockSpec((tile // 64, 64, 1024), lambda i, s: (i, 0, 0)),
            scratch_shapes=[pltpu.VMEM((tile, 1024), F32)],
        ),
        out_shape=jax.ShapeDtypeStruct((8, 64, 1024), BF16),
        compiler_params=params(),
        cost_estimate=cost(1.4e9),
        name="region",
    )(scalars, dscore, *tables, *blocks, inv)


def table_kernel(s, dscore, other, unit, loss, *refs):
    outs, acc = refs[:8], refs[8]
    half, rows = other.shape
    mine = dscore[pl.ds(pl.multiple_of(s[K] * half, 32), half), :]
    theirs = other[...]
    mine_at = pl.multiple_of(s[K] * rows, rows)
    theirs_at = pl.multiple_of((1 - s[K]) * rows, rows)
    extra = split3(jnp.sum(loss[...]), 128).astype(BF16)
    for dy in range(4):
        cols = pl.ds(pl.multiple_of(256 * ((s[Y] + dy) % 4), 256), 256)
        acc[...] = jnp.dot(
            mine, unit[pl.ds(mine_at, rows), cols], preferred_element_type=F32
        ) + jnp.dot(theirs, unit[pl.ds(theirs_at, rows), cols], preferred_element_type=F32)
        for dx in range(2):
            at = pl.multiple_of(128 * (s[XL] ^ dx), 128)
            out = outs[2 * dy + dx]
            out[0:half, :] = acc[:, pl.ds(at, 128)].astype(BF16)
            out[half : half + 8, :] = extra


def make_table(scalars, dscore, other, unit, loss):
    half = other.shape[0]
    return pl.pallas_call(
        table_kernel,
        in_specs=[smem()] + vmem(4),
        out_specs=vmem(8),
        out_shape=[jax.ShapeDtypeStruct((half + 8, 128), BF16)] * 8,
        scratch_shapes=[pltpu.VMEM((half, 256), F32)],
        compiler_params=params(),
        cost_estimate=cost(1.4e9),
        name="table",
    )(scalars, dscore, other, unit, loss)


def table_sum_kernel(*refs):
    terms, (out, loss) = refs[:8], refs[8:]
    half = out.shape[0]
    out[...] = sum(t[0:half, :].astype(F32) for t in terms).astype(BF16)
    loss[...] = sum(t[half : half + 8, :].astype(F32) for t in terms)


def make_table_sum(terms):
    half = terms[0].shape[0] - 8
    return pl.pallas_call(
        table_sum_kernel,
        in_specs=vmem(8),
        out_specs=vmem(2),
        out_shape=[jax.ShapeDtypeStruct((half, 128), BF16), jax.ShapeDtypeStruct((8, 128), F32)],
        compiler_params=params(),
        cost_estimate=cost(1e7),
        name="table_sum",
    )(*terms)


def merge_kernel(s, terms, loss, out):
    total = sum(terms[z].astype(F32) for z in range(8)).astype(BF16)
    extra = split3(jnp.sum(loss[...]), 256).astype(BF16)
    for q in range(4):
        to = s[E] ^ q
        for near in range(2):
            out[near, to, 0:64, :] = total[:, 256 * q : 256 * q + 256]
            out[near, to, 64:72, :] = extra


def make_merge(scalars, terms, loss):
    return pl.pallas_call(
        merge_kernel,
        in_specs=[smem()] + vmem(2),
        out_specs=vmem(1)[0],
        out_shape=jax.ShapeDtypeStruct((2, 4, 72, 256), BF16),
        compiler_params=params(),
        cost_estimate=cost(1e7),
        name="merge",
    )(scalars, terms, loss)


def share_kernel(pieces, out):
    for near in range(2):
        for k in range(2):
            both = pieces[near, 0, k, 0:64, :].astype(F32) + pieces[near, 1, k, 0:64, :].astype(F32)
            at = 128 * near + 64 * k
            out[at : at + 64, :] = both.astype(BF16)
    loss = sum(
        jnp.sum(pieces[near, x, k, 64:72, :].astype(F32))
        for near in range(2)
        for x in range(2)
        for k in range(2)
    )
    out[256:264, :] = split3(loss, 256).astype(BF16)


def make_share(pieces):
    return pl.pallas_call(
        share_kernel,
        in_specs=vmem(1),
        out_specs=vmem(1)[0],
        out_shape=jax.ShapeDtypeStruct((264, 256), BF16),
        compiler_params=params(),
        cost_estimate=cost(1e7),
        name="share",
    )(pieces)


def final_kernel(s, count, tables, *refs):
    regions, (region_out, table_out, loss_out) = refs[:4], refs[4:]
    total = 0.0
    for d in range(4):
        source = (s[ZH] + 4 - d) % 4
        for near in range(2):
            for k in range(2):
                at = 128 * near + 64 * k
                region_out[k, source, near] = regions[d][at : at + 64, :]
        total += jnp.sum(regions[d][256:264, :].astype(F32))
    loss_out[0, 0] = total / count[0] / CLASSES
    for y in range(4):
        at = pl.multiple_of(672 * (s[E] ^ y), 32)
        for x in range(2):
            table_out[pl.ds(at, 672), 128 * x : 128 * x + 128] = tables[2 * y + x]


def make_final(scalars, count, tables, regions):
    return pl.pallas_call(
        final_kernel,
        in_specs=[smem(), smem()] + vmem(5),
        out_specs=vmem(2) + [smem()],
        out_shape=[
            jax.ShapeDtypeStruct((2, 4, 2, 64, 256), BF16),
            jax.ShapeDtypeStruct((2688, 256), BF16),
            jax.ShapeDtypeStruct((1, 1), F32),
        ],
        compiler_params=params(),
        cost_estimate=cost(1e7),
        name="final",
    )(scalars, count, tables, *regions)


def over_img(x, dy, dx):
    pairs = [
        (2 * y + xl, 2 * ((y + dy) % 4) + (xl ^ dx)) for y in range(4) for xl in range(2)
    ]
    return lax.ppermute(x, IMG, pairs)


def to_owner(x):
    axes = ("img_0",) + EMB
    return lax.ppermute(x, axes, [(4 * y + e, 4 * y + (e ^ y)) for y in range(4) for e in range(4)])


def exchange(x, axes):
    return lax.all_to_all(x, axes, split_axis=0, concat_axis=0, tiled=True)


def shards(regions, table, shift, scale, labels, valid):
    rows = regions.shape[0]
    y = lax.axis_index("img_0")
    xl = lax.axis_index("img_1")
    xh = lax.axis_index("emb_0")
    k = lax.axis_index("emb_1")
    zh = lax.axis_index("cls_0")
    z = lax.axis_index(CLS)
    j = 2 * y + xl
    e = 2 * xh + k
    scalars = jnp.stack([k, z * 2688 + xh * 1344, e, y, xl, zh]).astype(jnp.int32)

    t_send = lax.dynamic_slice_in_dim(table, (1 - xh) * 1344 + 168 * j, 168, 0)
    t_send, regions_in = lax.optimization_barrier((t_send, regions))
    t_got = swap(t_send, "emb_0")
    t_own = lax.dynamic_slice_in_dim(table, xh * 1344, 1344, 0)
    local = jnp.sum((labels >= 0).astype(F32))
    high = jnp.floor(local / 32.0)
    lane = lax.broadcasted_iota(jnp.int32, (8, 256), 1)
    extra = jnp.where(lane == 0, high, jnp.where(lane == 1, local - 32.0 * high, 0.0)).astype(BF16)
    message = jnp.concatenate([t_got, extra], axis=0)
    t_all = exchange(jnp.broadcast_to(message, (8, 176, 256)), IMG)
    t_far = t_all[:, :168].reshape(1344, 256)
    count = jnp.sum(t_all[:, 168, 0].astype(F32) * 32.0 + t_all[:, 168, 1].astype(F32))
    r_far = swap(regions_in, "emb_0")
    r_near = swap(regions, "emb_1")
    r_both = swap(r_far, "emb_1")
    t_near = swap(t_own, "emb_1")
    t_both = swap(t_far, "emb_1")
    blocks = (regions, r_near, r_far, r_both)
    tables = (t_own, t_near, t_far, t_both)
    unit, inv = make_unit(blocks)

    factor = REGIONS / count
    zero = jnp.zeros((5, rows), F32)
    lane_f = jnp.concatenate([shift[None], scale[None], (scale * factor)[None], zero], axis=0)
    mask = lax.dynamic_slice(valid, (k, xh * 1344), (1, 1344)).astype(F32).T
    dscore, loss = make_focal(scalars, tables, unit, lane_f, labels[None], mask)

    theirs = swap(lax.dynamic_slice_in_dim(dscore, (1 - k) * 672, 672, 0), "emb_1")
    terms = exchange(make_region(scalars, dscore, tables, blocks, inv), CLS)
    chunks = make_table(scalars, dscore, theirs, unit, loss)
    chunks = [chunks[0]] + [over_img(chunks[o], o // 2, o % 2) for o in range(1, 8)]
    table_part, loss_part = make_table_sum(chunks)
    table_part = to_owner(table_part)
    merged = make_merge(scalars, terms, loss_part)
    pieces = exchange(merged.reshape(8, 72, 256), NEAR).reshape(2, 2, 2, 72, 256)
    table_all = exchange(jnp.broadcast_to(table_part, (8, 672, 128)), IMG)
    share = make_share(pieces)
    shares = [share] + [
        lax.ppermute(share, "cls_0", [(i, (i + d) % 4) for i in range(4)]) for d in range(1, 4)
    ]
    region_grad, table_grad, total = make_final(scalars, count.reshape(1), table_all, shares)
    return (total[0, 0], region_grad.reshape(rows, 256), table_grad)


def solution(mesh):
    torus = Mesh(
        mesh.devices.reshape(4, 2, 4, 2, 2, 2),
        ("img_0", "img_1", "cls_0", "cls_1", "emb_0", "emb_1"),
    )
    return jax.shard_map(
        shards,
        mesh=torus,
        in_specs=(P(IMG, EMB), P(CLS, EMB), P(IMG), P(IMG), P(IMG), P(IMG, CLS)),
        out_specs=(P(), P(IMG, EMB), P(CLS, EMB)),
        check_vma=False,
    )
```

```python
import jax
import jax.numpy as jnp
from jax import lax
from jax.experimental import pallas as pl
from jax.experimental.pallas import tpu as pltpu
from jax.sharding import Mesh
from jax.sharding import PartitionSpec as P

CLASSES = 21504
REGIONS = 8192
EMB = ("emb_0", "emb_1")
IMG = ("img_0", "img_1")
CLS = ("cls",)
CLS_EMB = CLS + EMB
F32 = jnp.float32
BF16 = jnp.bfloat16
NT = (((1,), (1,)), ((), ()))
TN = (((0,), (0,)), ((), ()))

K, BASE, E, Y, XL, Z = range(6)


PART = 336


def vmem(n):
    return [pl.BlockSpec(memory_space=pltpu.VMEM)] * n


def smem():
    return pl.BlockSpec(memory_space=pltpu.SMEM)


def params(mebibytes=16):
    return pltpu.CompilerParams(vmem_limit_bytes=mebibytes * 1024 * 1024)


def cost(flops):
    return pl.CostEstimate(flops=int(flops), bytes_accessed=1 << 20, transcendentals=0)


def swap(x, axis):
    return lax.ppermute(x, axis, [(0, 1), (1, 0)])


def split3(value, width):
    hi = value.astype(BF16).astype(F32)
    mid = (value - hi).astype(BF16).astype(F32)
    lo = value - hi - mid
    lane = lax.broadcasted_iota(jnp.int32, (8, width), 1)
    row = lax.broadcasted_iota(jnp.int32, (8, width), 0)
    packed = jnp.where(lane == 0, hi, jnp.where(lane == 1, mid, jnp.where(lane == 2, lo, 0.0)))
    return jnp.where(row == 0, packed, 0.0)


def unit_kernel(a, b, c, d, out, scale):
    blocks = [r[...].astype(F32) for r in (a, b, c, d)]
    squares = sum(jnp.sum(v * v, axis=1, keepdims=True) for v in blocks)
    inv = lax.rsqrt(squares + 1e-06)
    scale[...] = jnp.broadcast_to(inv, scale.shape)
    for q, v in enumerate(blocks):
        out[:, 256 * q : 256 * q + 256] = (v * inv).astype(BF16)


def make_unit(blocks):
    rows = blocks[0].shape[0]
    tile = 256
    return pl.pallas_call(
        unit_kernel,
        grid=(rows // tile,),
        in_specs=[pl.BlockSpec((tile, 256), lambda i: (i, 0))] * 4,
        out_specs=[
            pl.BlockSpec((tile, 1024), lambda i: (i, 0)),
            pl.BlockSpec((tile, 128), lambda i: (i, 0)),
        ],
        out_shape=[
            jax.ShapeDtypeStruct((rows, 1024), BF16),
            jax.ShapeDtypeStruct((rows, 128), F32),
        ],
        compiler_params=params(),
        cost_estimate=cost(2e7),
        name="unit",
    )(*blocks)


def message_kernel(part, mine, theirs, out):
    count = mine[...] + theirs[...]
    high = jnp.floor(count / 32.0)
    lane = lax.broadcasted_iota(jnp.int32, (8, 128), 1)
    extra = jnp.where(lane == 0, high, jnp.where(lane == 1, count - 32.0 * high, 0.0))
    extra = jnp.concatenate([extra, jnp.zeros((8, 128), F32)], axis=1).astype(BF16)
    for y in range(4):
        out[y, 0:PART, :] = part[...]
        out[y, PART : PART + 8, :] = extra


def make_message(part, mine, theirs):
    return pl.pallas_call(
        message_kernel,
        in_specs=vmem(3),
        out_specs=vmem(1)[0],
        out_shape=jax.ShapeDtypeStruct((4, PART + 8, 256), BF16),
        compiler_params=params(),
        name="message",
    )(part, mine, theirs)


def read_count(far):
    lane = lax.broadcasted_iota(jnp.int32, (1, 256), 1)
    row = sum(far[y, PART : PART + 8, :].astype(F32)[0:1, :] for y in range(4))
    return jnp.sum(jnp.where(lane == 0, 32.0 * row, jnp.where(lane == 1, row, 0.0)))


def focal_kernel(s, t0, t1, t2, t3, unit, lane_f, labels, mask, keep, send, loss, count_out, acc):
    rows = unit.shape[0]
    half = keep.shape[0]
    count = read_count(t2)
    count_out[0, 0] = count
    u = [unit[:, 256 * q : 256 * q + 256] for q in range(4)]

    def dot(t, q):
        return lax.dot_general(t, u[q], NT, preferred_element_type=F32)

    for c in range(4):
        at = slice(PART * c, PART * c + PART)
        acc[at, :] = (
            dot(t0[at, :], 0) + dot(t1[at, :], 1) + dot(t2[c, 0:PART, :], 2) + dot(t3[c, 0:PART, :], 3)
        )
    shift = lane_f[0:1, :]
    scale = lane_f[1:2, :]
    factor = scale * (REGIONS / count)
    step = 32

    def part(out, start, total):
        wanted = labels[...] - (s[BASE] + start)

        def body(g, total):
            to = pl.multiple_of(g * step, step)
            at = pl.multiple_of(start + to, step)
            logit = (acc[pl.ds(at, step), :] + shift) * scale
            ids = lax.broadcasted_iota(jnp.int32, (step, rows), 0)
            target = (wanted - to) == ids
            m = jnp.where(target, -logit, logit)
            e = jnp.exp(-jnp.abs(m))
            r = 1.0 / (1.0 + e)
            er = e * r
            positive = m >= 0.0
            prob = jnp.where(positive, r, er)
            rest = jnp.where(positive, er, r)
            series = e * (1.0 - e * (0.5 - e * (1.0 / 3.0 - e * 0.25)))
            soft = jnp.maximum(m, 0.0) + jnp.where(e < 2e-3, series, jnp.log(1.0 + e))
            weight = jnp.where(target, 0.25, 0.75) * mask[pl.ds(at, step), :] * (prob * prob)
            slope = weight * (2.0 * rest * soft + prob)
            slope = jnp.where(target, -slope, slope)
            out[pl.ds(to, step), :] = (slope * factor).astype(BF16)
            term = weight * soft
            return total + sum(term[8 * i : 8 * i + 8, :] for i in range(step // 8))

        return lax.fori_loop(0, half // step, body, total)

    total = part(send, (1 - s[K]) * half, jnp.zeros((8, rows), F32))
    total = part(keep, s[K] * half, total)
    loss[...] = sum(total[:, 128 * i : 128 * i + 128] for i in range(4))


def make_focal(scalars, tables, unit, lane_f, labels, mask):
    rows = unit.shape[0] // 2
    classes = mask.shape[0]
    whole = lambda i, s: (0, 0)
    cube = lambda i, s: (0, 0, 0)
    return pl.pallas_call(
        focal_kernel,
        grid_spec=pltpu.PrefetchScalarGridSpec(
            num_scalar_prefetch=1,
            grid=(1,),
            in_specs=[pl.BlockSpec((classes, 256), whole)] * 2
            + [pl.BlockSpec((4, PART + 8, 256), cube)] * 2
            + [
                pl.BlockSpec((rows, 1024), lambda i, s: (s[K], 0)),
                pl.BlockSpec((8, rows), lambda i, s: (0, s[K])),
                pl.BlockSpec((1, rows), lambda i, s: (0, s[K])),
                pl.BlockSpec((classes, 1), whole),
            ],
            out_specs=[
                pl.BlockSpec((classes // 2, rows), whole),
                pl.BlockSpec((classes // 2, rows), whole),
                pl.BlockSpec((8, 128), whole),
                smem(),
            ],
            scratch_shapes=[pltpu.VMEM((classes, rows), F32)],
        ),
        out_shape=[
            jax.ShapeDtypeStruct((classes // 2, rows), BF16),
            jax.ShapeDtypeStruct((classes // 2, rows), BF16),
            jax.ShapeDtypeStruct((8, 128), F32),
            jax.ShapeDtypeStruct((1, 1), F32),
        ],
        compiler_params=params(24),
        cost_estimate=cost(1.4e9),
        name="focal",
    )(scalars, *tables, unit, lane_f, labels, mask)


def region_kernel(s, keep, send, k0, k1, k2, k3, o0, o1, o2, o3, a, b, c, d, inv_ref, out, acc):
    inv = inv_ref[:, 0:1]
    mine = keep[...]
    theirs = send[...]

    def dot(g, t):
        return lax.dot_general(g, t, TN, preferred_element_type=F32)

    along = 0.0
    rows = (a, b, c, d)
    for q, (t, o) in enumerate(zip((k0, k1, k2, k3), (o0, o1, o2, o3))):
        if q < 2:
            part = dot(mine, t[...]) + dot(theirs, o[...])
        else:
            part = sum(
                dot(g[PART * i : PART * i + PART, :], x[i, 0:PART, :])
                for g, x in ((mine, t), (theirs, o))
                for i in range(2)
            )
        acc[:, 256 * q : 256 * q + 256] = part
        along += jnp.sum(part * rows[q][...].astype(F32), axis=1, keepdims=True)
    back = inv * inv * along
    for q, r in enumerate(rows):
        grad = inv * (acc[:, 256 * q : 256 * q + 256] - r[...].astype(F32) * back)
        to = s[E] ^ q
        for i in range(out.shape[0]):
            out[i, to] = grad[64 * i : 64 * i + 64, :].astype(BF16)


def make_region(scalars, keep, send, tables, blocks, inv):
    half, rows = keep.shape
    tile = 128
    steps = rows // tile
    flat = lambda f: pl.BlockSpec((half, 256), lambda i, s: (f(s), 0))
    cube = lambda f: pl.BlockSpec((2, PART + 8, 256), lambda i, s: (f(s), 0, 0))
    own = lambda s: s[K]
    other = lambda s: 1 - s[K]
    return pl.pallas_call(
        region_kernel,
        grid_spec=pltpu.PrefetchScalarGridSpec(
            num_scalar_prefetch=1,
            grid=(steps,),
            in_specs=[pl.BlockSpec((half, tile), lambda i, s: (0, i))] * 2
            + [flat(own)] * 2
            + [cube(own)] * 2
            + [flat(other)] * 2
            + [cube(other)] * 2
            + [pl.BlockSpec((tile, 256), lambda i, s: (s[K] * steps + i, 0))] * 4
            + [pl.BlockSpec((tile, 128), lambda i, s: (s[K] * steps + i, 0))],
            out_specs=pl.BlockSpec((tile // 64, 4, 64, 256), lambda i, s: (i, 0, 0, 0)),
            scratch_shapes=[pltpu.VMEM((tile, 1024), F32)],
        ),
        out_shape=jax.ShapeDtypeStruct((8, 4, 64, 256), BF16),
        compiler_params=params(),
        cost_estimate=cost(1.4e9),
        name="region",
    )(scalars, keep, send, *tables, *tables, *blocks, inv)


def table_kernel(s, keep, other, unit, l0, l1, l2, l3, *refs):
    outs, acc = refs[:8], refs[8]
    half, rows = other.shape
    mine = keep[...]
    theirs = other[...]
    mine_at = pl.multiple_of(s[K] * rows, rows)
    theirs_at = pl.multiple_of((1 - s[K]) * rows, rows)
    loss = jnp.sum(l0[...] + l1[...] + l2[...] + l3[...])
    extra = split3(loss, 128).astype(BF16)
    for dy in range(4):
        cols = pl.ds(pl.multiple_of(256 * ((s[Y] + dy) % 4), 256), 256)
        acc[...] = jnp.dot(
            mine, unit[pl.ds(mine_at, rows), cols], preferred_element_type=F32
        ) + jnp.dot(theirs, unit[pl.ds(theirs_at, rows), cols], preferred_element_type=F32)
        for dx in range(2):
            at = pl.multiple_of(128 * (s[XL] ^ dx), 128)
            out = outs[2 * dy + dx]
            out[0:half, :] = acc[:, pl.ds(at, 128)].astype(BF16)
            out[half : half + 8, :] = extra


def make_table(scalars, keep, other, unit, losses):
    half = other.shape[0]
    return pl.pallas_call(
        table_kernel,
        in_specs=[smem()] + vmem(7),
        out_specs=vmem(8),
        out_shape=[jax.ShapeDtypeStruct((half + 8, 128), BF16)] * 8,
        scratch_shapes=[pltpu.VMEM((half, 256), F32)],
        compiler_params=params(),
        cost_estimate=cost(1.4e9),
        name="table",
    )(scalars, keep, other, unit, *losses)


def table_sum_kernel(*refs):
    terms, (out, loss) = refs[:8], refs[8:]
    half = out.shape[1]
    total = sum(t[0:half, :].astype(F32) for t in terms).astype(BF16)
    for j in range(8):
        out[j] = total
    loss[...] = sum(t[half : half + 8, :].astype(F32) for t in terms)


def make_table_sum(terms):
    half = terms[0].shape[0] - 8
    return pl.pallas_call(
        table_sum_kernel,
        in_specs=vmem(8),
        out_specs=vmem(2),
        out_shape=[jax.ShapeDtypeStruct((8, half, 128), BF16), jax.ShapeDtypeStruct((8, 128), F32)],
        compiler_params=params(),
        cost_estimate=cost(1e7),
        name="table_sum",
    )(*terms)


def share_kernel(pieces, loss, out):
    for k in range(2):
        total = sum(
            pieces[z, x, k].astype(F32) for z in range(8) for x in range(2)
        )
        out[64 * k : 64 * k + 64, :] = total.astype(BF16)
    out[128:136, :] = split3(jnp.sum(loss[...]), 256).astype(BF16)


def make_share(pieces, loss):
    return pl.pallas_call(
        share_kernel,
        in_specs=vmem(2),
        out_specs=vmem(1)[0],
        out_shape=jax.ShapeDtypeStruct((136, 256), BF16),
        compiler_params=params(),
        cost_estimate=cost(1e7),
        name="share",
    )(pieces, loss)


def final_kernel(s, count, tables, *refs):
    regions, (region_out, table_out, loss_out) = refs[:8], refs[8:]
    total = 0.0
    for d in range(8):
        source = (s[Z] + 8 - d) % 8
        for k in range(2):
            region_out[k, source] = regions[d][64 * k : 64 * k + 64, :]
        total += jnp.sum(regions[d][128:136, :].astype(F32))
    loss_out[0, 0] = total / count[0, 0] / CLASSES
    for y in range(4):
        at = pl.multiple_of(672 * (s[E] ^ y), 32)
        for x in range(2):
            table_out[pl.ds(at, 672), 128 * x : 128 * x + 128] = tables[2 * y + x]


def make_final(scalars, count, tables, regions):
    return pl.pallas_call(
        final_kernel,
        in_specs=[smem(), smem()] + vmem(9),
        out_specs=vmem(2) + [smem()],
        out_shape=[
            jax.ShapeDtypeStruct((2, 8, 64, 256), BF16),
            jax.ShapeDtypeStruct((2688, 256), BF16),
            jax.ShapeDtypeStruct((1, 1), F32),
        ],
        compiler_params=params(),
        cost_estimate=cost(1e7),
        name="final",
    )(scalars, count, tables, *regions)


def to_owner(x, dy, dx):
    pairs = []
    for y in range(4):
        for xl in range(2):
            for e in range(4):
                to = (y + dy) % 4
                pairs.append((8 * y + 4 * xl + e, 8 * to + 4 * (xl ^ dx) + (e ^ to)))
    return lax.ppermute(x, IMG + EMB, pairs)


def along_cls(x, d):
    return lax.ppermute(x, CLS, [(i, (i + d) % 8) for i in range(8)])


def exchange(x, axes):
    return lax.all_to_all(x, axes, split_axis=0, concat_axis=0, tiled=True)


def shards(regions, table, shift, scale, labels, valid):
    rows = regions.shape[0]
    y = lax.axis_index("img_0")
    xl = lax.axis_index("img_1")
    xh = lax.axis_index("emb_0")
    k = lax.axis_index("emb_1")
    z = lax.axis_index(CLS)
    scalars = jnp.stack([k, z * 2688 + xh * 1344, 2 * xh + k, y, xl, z]).astype(jnp.int32)

    t_send = lax.dynamic_slice_in_dim(table, (1 - xh) * 1344 + PART * y, PART, 0)
    t_send, regions_in = lax.optimization_barrier((t_send, regions))
    t_got = swap(t_send, "emb_0")
    local = jnp.broadcast_to(jnp.sum((labels >= 0).astype(F32)), (8, 128))
    t_far = exchange(make_message(t_got, local, swap(local, "img_1")), "img_0")
    t_own = lax.dynamic_slice_in_dim(table, xh * 1344, 1344, 0)
    r_far = swap(regions_in, "emb_0")
    r_near = swap(regions, "emb_1")
    r_both = swap(r_far, "emb_1")
    t_near = swap(t_own, "emb_1")
    t_both = swap(t_far, "emb_1")
    blocks = (regions, r_near, r_far, r_both)
    tables = (t_own, t_near, t_far, t_both)
    unit, inv = make_unit(blocks)

    lane_f = jnp.concatenate([shift[None], scale[None], jnp.zeros((6, rows), F32)], axis=0)
    mask = lax.dynamic_slice(valid, (k, xh * 1344), (1, 1344)).astype(F32).T
    keep, send, loss, count = make_focal(scalars, tables, unit, lane_f, labels[None], mask)

    theirs = swap(send, "emb_1")
    losses = [loss, swap(loss, "emb_0"), swap(loss, "emb_1")]
    losses.append(lax.ppermute(loss, EMB, [(i, i ^ 3) for i in range(4)]))
    terms = make_region(scalars, keep, send, tables, blocks, inv)
    pieces = exchange(terms.reshape(32, 64, 256), CLS_EMB).reshape(8, 2, 2, 64, 256)
    chunks = make_table(scalars, keep, theirs, unit, losses)
    chunks = [to_owner(chunks[o], o // 2, o % 2) for o in range(8)]
    table_part, loss_part = make_table_sum(chunks)
    share = make_share(pieces, loss_part)
    table_part, share = lax.optimization_barrier((table_part, share))
    table_all = exchange(table_part, IMG)
    shares = [share] + [along_cls(share, d) for d in range(1, 8)]
    region_grad, table_grad, total = make_final(scalars, count, table_all, shares)
    return (total[0, 0], region_grad.reshape(rows, 256), table_grad)


def solution(mesh):
    torus = Mesh(
        mesh.devices.reshape(4, 2, mesh.shape["cls"], 2, 2),
        ("img_0", "img_1", "cls", "emb_0", "emb_1"),
    )
    return jax.shard_map(
        shards,
        mesh=torus,
        in_specs=(P(IMG, EMB), P(CLS, EMB), P(IMG), P(IMG), P(IMG), P(IMG, CLS)),
        out_specs=(P(), P(IMG, EMB), P(CLS, EMB)),
        check_vma=False,
    )
```

```python
import jax
import jax.numpy as jnp
from jax import lax
from jax.experimental import pallas as pl
from jax.experimental.pallas import tpu as pltpu
from jax.sharding import Mesh
from jax.sharding import PartitionSpec as P

CLASSES = 21504
REGIONS = 8192
EMB = ("emb_0", "emb_1")
IMG = ("img_0", "img_1")
CLS = ("cls",)
CLS_EMB = CLS + EMB[:1]
F32 = jnp.float32
BF16 = jnp.bfloat16
NT = (((1,), (1,)), ((), ()))
TN = (((0,), (0,)), ((), ()))

K, BASE, E, Y, XL, Z = range(6)


PART = 336


def vmem(n):
    return [pl.BlockSpec(memory_space=pltpu.VMEM)] * n


def in_hbm(shape, dtype):
    return pltpu.HBM(shape, dtype)


def smem():
    return pl.BlockSpec(memory_space=pltpu.SMEM)


def params(mebibytes=16):
    return pltpu.CompilerParams(vmem_limit_bytes=mebibytes * 1024 * 1024)


def cost(flops):
    return pl.CostEstimate(flops=int(flops), bytes_accessed=1 << 20, transcendentals=0)


def swap(x, axis):
    return lax.ppermute(x, axis, [(0, 1), (1, 0)])


def split3(value, width):
    hi = value.astype(BF16).astype(F32)
    mid = (value - hi).astype(BF16).astype(F32)
    lo = value - hi - mid
    lane = lax.broadcasted_iota(jnp.int32, (8, width), 1)
    row = lax.broadcasted_iota(jnp.int32, (8, width), 0)
    packed = jnp.where(lane == 0, hi, jnp.where(lane == 1, mid, jnp.where(lane == 2, lo, 0.0)))
    return jnp.where(row == 0, packed, 0.0)


def unit_kernel(a, b, c, d, out, scale):
    blocks = [r[...].astype(F32) for r in (a, b, c, d)]
    squares = sum(jnp.sum(v * v, axis=1, keepdims=True) for v in blocks)
    inv = lax.rsqrt(squares + 1e-06)
    scale[...] = jnp.broadcast_to(inv, scale.shape)
    for q, v in enumerate(blocks):
        out[:, 256 * q : 256 * q + 256] = (v * inv).astype(BF16)


def make_unit(blocks):
    rows = blocks[0].shape[0]
    tile = 256
    return pl.pallas_call(
        unit_kernel,
        grid=(rows // tile,),
        in_specs=[pl.BlockSpec((tile, 256), lambda i: (i, 0))] * 4,
        out_specs=[
            pl.BlockSpec((tile, 1024), lambda i: (i, 0)),
            pl.BlockSpec((tile, 128), lambda i: (i, 0)),
        ],
        out_shape=[
            jax.ShapeDtypeStruct((rows, 1024), BF16),
            jax.ShapeDtypeStruct((rows, 128), F32),
        ],
        compiler_params=params(),
        cost_estimate=cost(2e7),
        name="unit",
    )(*blocks)


def rows_kernel(s, x, out):
    out[...] = x[...]


def take_rows(x, at, rows):
    return pl.pallas_call(
        rows_kernel,
        grid_spec=pltpu.PrefetchScalarGridSpec(
            num_scalar_prefetch=1,
            grid=(1,),
            in_specs=[pl.BlockSpec((rows, 256), lambda i, s: (s[0], 0))],
            out_specs=pl.BlockSpec((rows, 256), lambda i, s: (0, 0)),
        ),
        out_shape=jax.ShapeDtypeStruct((rows, 256), BF16),
        compiler_params=params(),
        name="rows",
    )(at.reshape(1), x)


def message_kernel(part, mine, theirs, out):
    count = mine[...] + theirs[...]
    high = jnp.floor(count / 32.0)
    lane = lax.broadcasted_iota(jnp.int32, (8, 128), 1)
    extra = jnp.where(lane == 0, high, jnp.where(lane == 1, count - 32.0 * high, 0.0))
    extra = jnp.concatenate([extra, jnp.zeros((8, 128), F32)], axis=1).astype(BF16)
    for y in range(4):
        out[y, 0:PART, :] = part[...]
        out[y, PART : PART + 8, :] = extra


def make_message(part, mine, theirs):
    return pl.pallas_call(
        message_kernel,
        in_specs=vmem(3),
        out_specs=vmem(1)[0],
        out_shape=in_hbm((4, PART + 8, 256), BF16),
        compiler_params=params(),
        name="message",
    )(part, mine, theirs)


def read_count(far):
    lane = lax.broadcasted_iota(jnp.int32, (1, 256), 1)
    row = sum(far[y, PART : PART + 8, :].astype(F32)[0:1, :] for y in range(4))
    return jnp.sum(jnp.where(lane == 0, 32.0 * row, jnp.where(lane == 1, row, 0.0)))


def focal_kernel(s, t0, t1, t2, t3, unit, lane_f, labels, mask, keep, send, loss, count_out, acc):
    rows = unit.shape[0]
    half = keep.shape[0]
    count = read_count(t2)
    count_out[0, 0] = count
    u = [unit[:, 256 * q : 256 * q + 256] for q in range(4)]

    def dot(t, q):
        return lax.dot_general(t, u[q], NT, preferred_element_type=F32)

    for c in range(4):
        at = slice(PART * c, PART * c + PART)
        acc[at, :] = (
            dot(t0[at, :], 0) + dot(t1[at, :], 1) + dot(t2[c, 0:PART, :], 2) + dot(t3[c, 0:PART, :], 3)
        )
    shift = lane_f[0:1, :]
    scale = lane_f[1:2, :]
    factor = scale * (REGIONS / count)
    step = 32

    def part(out, start, total):
        wanted = labels[...] - (s[BASE] + start)

        def body(g, total):
            to = pl.multiple_of(g * step, step)
            at = pl.multiple_of(start + to, step)
            logit = (acc[pl.ds(at, step), :] + shift) * scale
            ids = lax.broadcasted_iota(jnp.int32, (step, rows), 0)
            target = (wanted - to) == ids
            m = jnp.where(target, -logit, logit)
            e = jnp.exp(-jnp.abs(m))
            r = 1.0 / (1.0 + e)
            er = e * r
            positive = m >= 0.0
            prob = jnp.where(positive, r, er)
            rest = jnp.where(positive, er, r)
            series = e * (1.0 - e * (0.5 - e * (1.0 / 3.0 - e * 0.25)))
            soft = jnp.maximum(m, 0.0) + jnp.where(e < 2e-3, series, jnp.log(1.0 + e))
            weight = jnp.where(target, 0.25, 0.75) * mask[pl.ds(at, step), :] * (prob * prob)
            slope = weight * (2.0 * rest * soft + prob)
            slope = jnp.where(target, -slope, slope)
            out[pl.ds(to, step), :] = (slope * factor).astype(BF16)
            term = weight * soft
            return total + sum(term[8 * i : 8 * i + 8, :] for i in range(step // 8))

        return lax.fori_loop(0, half // step, body, total)

    total = part(send, (1 - s[K]) * half, jnp.zeros((8, rows), F32))
    total = part(keep, s[K] * half, total)
    loss[...] = sum(total[:, 128 * i : 128 * i + 128] for i in range(4))


def make_focal(scalars, tables, unit, lane_f, labels, mask):
    rows = unit.shape[0] // 2
    classes = mask.shape[0]
    whole = lambda i, s: (0, 0)
    cube = lambda i, s: (0, 0, 0)
    return pl.pallas_call(
        focal_kernel,
        grid_spec=pltpu.PrefetchScalarGridSpec(
            num_scalar_prefetch=1,
            grid=(1,),
            in_specs=[pl.BlockSpec((classes, 256), whole)] * 2
            + [pl.BlockSpec((4, PART + 8, 256), cube)] * 2
            + [
                pl.BlockSpec((rows, 1024), lambda i, s: (s[K], 0)),
                pl.BlockSpec((8, rows), lambda i, s: (0, s[K])),
                pl.BlockSpec((1, rows), lambda i, s: (0, s[K])),
                pl.BlockSpec((classes, 1), whole),
            ],
            out_specs=[
                pl.BlockSpec((classes // 2, rows), whole),
                pl.BlockSpec((classes // 2, rows), whole),
                pl.BlockSpec((8, 128), whole),
                smem(),
            ],
            scratch_shapes=[pltpu.VMEM((classes, rows), F32)],
        ),
        out_shape=[
            jax.ShapeDtypeStruct((classes // 2, rows), BF16),
            jax.ShapeDtypeStruct((classes // 2, rows), BF16),
            jax.ShapeDtypeStruct((8, 128), F32),
            jax.ShapeDtypeStruct((1, 1), F32),
        ],
        compiler_params=params(24),
        cost_estimate=cost(1.4e9),
        name="focal",
    )(scalars, *tables, unit, lane_f, labels, mask)


def region_kernel(s, keep, send, k0, k1, k2, k3, o0, o1, o2, o3, a, b, c, d, inv_ref, out, acc):
    inv = inv_ref[:, 0:1]
    mine = keep[...]
    theirs = send[...]

    def dot(g, t):
        return lax.dot_general(g, t, TN, preferred_element_type=F32)

    along = 0.0
    rows = (a, b, c, d)
    for q, (t, o) in enumerate(zip((k0, k1, k2, k3), (o0, o1, o2, o3))):
        if q < 2:
            part = dot(mine, t[...]) + dot(theirs, o[...])
        else:
            part = sum(
                dot(g[PART * i : PART * i + PART, :], x[i, 0:PART, :])
                for g, x in ((mine, t), (theirs, o))
                for i in range(2)
            )
        acc[:, 256 * q : 256 * q + 256] = part
        along += jnp.sum(part * rows[q][...].astype(F32), axis=1, keepdims=True)
    back = inv * inv * along
    for q, r in enumerate(rows):
        grad = inv * (acc[:, 256 * q : 256 * q + 256] - r[...].astype(F32) * back)
        to = s[E] ^ q
        for i in range(out.shape[0]):
            out[i, to] = grad[64 * i : 64 * i + 64, :].astype(BF16)


def make_region(scalars, keep, send, tables, blocks, inv):
    half, rows = keep.shape
    tile = 256
    steps = rows // tile
    flat = lambda f: pl.BlockSpec((half, 256), lambda i, s: (f(s), 0))
    cube = lambda f: pl.BlockSpec((2, PART + 8, 256), lambda i, s: (f(s), 0, 0))
    own = lambda s: s[K]
    other = lambda s: 1 - s[K]
    return pl.pallas_call(
        region_kernel,
        grid_spec=pltpu.PrefetchScalarGridSpec(
            num_scalar_prefetch=1,
            grid=(steps,),
            in_specs=[pl.BlockSpec((half, tile), lambda i, s: (0, i))] * 2
            + [flat(own)] * 2
            + [cube(own)] * 2
            + [flat(other)] * 2
            + [cube(other)] * 2
            + [pl.BlockSpec((tile, 256), lambda i, s: (s[K] * steps + i, 0))] * 4
            + [pl.BlockSpec((tile, 128), lambda i, s: (s[K] * steps + i, 0))],
            out_specs=pl.BlockSpec((tile // 64, 4, 64, 256), lambda i, s: (i, 0, 0, 0)),
            scratch_shapes=[pltpu.VMEM((tile, 1024), F32)],
        ),
        out_shape=in_hbm((8, 4, 64, 256), BF16),
        compiler_params=params(),
        cost_estimate=cost(1.4e9),
        name="region",
    )(scalars, keep, send, *tables, *tables, *blocks, inv)


def table_kernel(s, keep, other, unit, l0, l1, l2, l3, *refs):
    outs, acc = refs[:8], refs[8]
    half, rows = other.shape
    mine = keep[...]
    theirs = other[...]
    mine_at = pl.multiple_of(s[K] * rows, rows)
    theirs_at = pl.multiple_of((1 - s[K]) * rows, rows)
    loss = jnp.sum(l0[...] + l1[...] + l2[...] + l3[...])
    extra = split3(loss, 128).astype(BF16)
    for dy in range(4):
        cols = pl.ds(pl.multiple_of(256 * ((s[Y] + dy) % 4), 256), 256)
        acc[...] = jnp.dot(
            mine, unit[pl.ds(mine_at, rows), cols], preferred_element_type=F32
        ) + jnp.dot(theirs, unit[pl.ds(theirs_at, rows), cols], preferred_element_type=F32)
        for dx in range(2):
            at = pl.multiple_of(128 * (s[XL] ^ dx), 128)
            out = outs[2 * dy + dx]
            out[0:half, :] = acc[:, pl.ds(at, 128)].astype(BF16)
            out[half : half + 8, :] = extra


def make_table(scalars, keep, other, unit, losses):
    half = other.shape[0]
    return pl.pallas_call(
        table_kernel,
        in_specs=[smem()] + vmem(7),
        out_specs=vmem(8),
        out_shape=[jax.ShapeDtypeStruct((half + 8, 128), BF16)] * 8,
        scratch_shapes=[pltpu.VMEM((half, 256), F32)],
        compiler_params=params(),
        cost_estimate=cost(1.4e9),
        name="table",
    )(scalars, keep, other, unit, *losses)


def table_sum_kernel(*refs):
    terms, (out, loss) = refs[:8], refs[8:]
    half = out.shape[1]
    total = sum(t[0:half, :].astype(F32) for t in terms).astype(BF16)
    for j in range(8):
        out[j] = total
    loss[...] = sum(t[half : half + 8, :].astype(F32) for t in terms)


def make_table_sum(terms):
    half = terms[0].shape[0] - 8
    return pl.pallas_call(
        table_sum_kernel,
        in_specs=vmem(8),
        out_specs=vmem(2),
        out_shape=[in_hbm((8, half, 128), BF16), jax.ShapeDtypeStruct((8, 128), F32)],
        compiler_params=params(),
        cost_estimate=cost(1e7),
        name="table_sum",
    )(*terms)


def region_sum_kernel(s, pieces, mine, theirs):
    totals = [
        sum(pieces[z, x, k].astype(F32) for z in range(8) for x in range(2)) for k in range(2)
    ]
    first = s[K] == 0
    mine[...] = jnp.where(first, totals[0], totals[1]).astype(BF16)
    theirs[...] = jnp.where(first, totals[1], totals[0]).astype(BF16)


def make_region_sum(scalars, pieces):
    return pl.pallas_call(
        region_sum_kernel,
        in_specs=[smem()] + vmem(1),
        out_specs=vmem(2),
        out_shape=[jax.ShapeDtypeStruct((64, 256), BF16)] * 2,
        compiler_params=params(),
        cost_estimate=cost(1e7),
        name="region_sum",
    )(scalars, pieces)


def share_kernel(s, mine, other, loss, out):
    out[pl.ds(pl.multiple_of(64 * s[K], 64), 64), :] = mine[...]
    out[pl.ds(pl.multiple_of(64 * (1 - s[K]), 64), 64), :] = other[...]
    out[128:136, :] = split3(jnp.sum(loss[...]), 256).astype(BF16)


def make_share(scalars, mine, other, loss):
    return pl.pallas_call(
        share_kernel,
        in_specs=[smem()] + vmem(3),
        out_specs=vmem(1)[0],
        out_shape=jax.ShapeDtypeStruct((136, 256), BF16),
        compiler_params=params(),
        cost_estimate=cost(1e7),
        name="share",
    )(scalars, mine, other, loss)


def final_kernel(s, count, tables, *refs):
    regions, (region_out, table_out, loss_out) = refs[:8], refs[8:]
    total = 0.0
    for d in range(8):
        source = (s[Z] + 8 - d) % 8
        for k in range(2):
            region_out[k, source] = regions[d][64 * k : 64 * k + 64, :]
        total += jnp.sum(regions[d][128:136, :].astype(F32))
    loss_out[0, 0] = total / count[0, 0] / CLASSES
    for y in range(4):
        at = pl.multiple_of(672 * (s[E] ^ y), 32)
        for x in range(2):
            table_out[pl.ds(at, 672), 128 * x : 128 * x + 128] = tables[2 * y + x]


def make_final(scalars, count, tables, regions):
    return pl.pallas_call(
        final_kernel,
        in_specs=[smem(), smem()] + vmem(9),
        out_specs=vmem(2) + [smem()],
        out_shape=[
            jax.ShapeDtypeStruct((2, 8, 64, 256), BF16),
            jax.ShapeDtypeStruct((2688, 256), BF16),
            jax.ShapeDtypeStruct((1, 1), F32),
        ],
        compiler_params=params(),
        cost_estimate=cost(1e7),
        name="final",
    )(scalars, count, tables, *regions)


def to_owner(x, dy, dx):
    pairs = []
    for y in range(4):
        for xl in range(2):
            for e in range(4):
                to = (y + dy) % 4
                pairs.append((8 * y + 4 * xl + e, 8 * to + 4 * (xl ^ dx) + (e ^ to)))
    return lax.ppermute(x, IMG + EMB, pairs)


def along_cls(x, d):
    return lax.ppermute(x, CLS, [(i, (i + d) % 8) for i in range(8)])


def exchange(x, axes):
    return lax.all_to_all(x, axes, split_axis=0, concat_axis=0, tiled=True)


def shards(regions, table, shift, scale, labels, valid):
    rows = regions.shape[0]
    y = lax.axis_index("img_0")
    xl = lax.axis_index("img_1")
    xh = lax.axis_index("emb_0")
    k = lax.axis_index("emb_1")
    z = lax.axis_index(CLS)
    scalars = jnp.stack([k, z * 2688 + xh * 1344, 2 * xh + k, y, xl, z]).astype(jnp.int32)

    t_send = take_rows(pltpu.with_memory_space_constraint(table, pltpu.HBM), 4 * (1 - xh) + y, PART)
    t_send, regions_in = lax.optimization_barrier((t_send, regions))
    t_got = swap(t_send, "emb_0")
    r_far = swap(regions_in, "emb_0")
    r_near = swap(regions_in, "emb_1")
    local = jnp.broadcast_to(jnp.sum((labels >= 0).astype(F32)), (8, 128))
    t_far = exchange(make_message(t_got, local, swap(local, "img_1")), "img_0")
    t_own = lax.dynamic_slice_in_dim(table, xh * 1344, 1344, 0)
    t_near = swap(t_own, "emb_1")
    r_both = swap(r_far, "emb_1")
    t_both = swap(t_far, "emb_1")
    blocks = (regions, r_near, r_far, r_both)
    tables = (t_own, t_near, t_far, t_both)
    unit, inv = make_unit(blocks)

    lane_f = jnp.concatenate([shift[None], scale[None], jnp.zeros((6, rows), F32)], axis=0)
    mask = lax.dynamic_slice(valid, (k, xh * 1344), (1, 1344)).astype(F32).T
    keep, send, loss, count = make_focal(scalars, tables, unit, lane_f, labels[None], mask)

    theirs = swap(send, "emb_1")
    loss_0 = swap(loss, "emb_0")
    loss_1 = swap(loss, "emb_1")
    loss_2 = lax.ppermute(loss, EMB, [(i, i ^ 3) for i in range(4)])
    terms = make_region(scalars, keep, send, tables, blocks, inv)
    pieces = exchange(terms.reshape(16, 128, 256), CLS_EMB).reshape(8, 2, 2, 64, 256)
    chunks = make_table(scalars, keep, theirs, unit, [loss, loss_0, loss_1, loss_2])
    chunks = [to_owner(chunks[o], o // 2, o % 2) for o in range(8)]
    table_part, loss_part = make_table_sum(chunks)
    mine, other = make_region_sum(scalars, pieces)
    share = make_share(scalars, mine, swap(other, "emb_1"), loss_part)
    table_part, share = lax.optimization_barrier((table_part, share))
    table_all = exchange(table_part, IMG)
    shares = [share] + [along_cls(share, d) for d in range(1, 8)]
    region_grad, table_grad, total = make_final(scalars, count, table_all, shares)
    return (total[0, 0], region_grad.reshape(rows, 256), table_grad)


def solution(mesh):
    torus = Mesh(
        mesh.devices.reshape(4, 2, mesh.shape["cls"], 2, 2),
        ("img_0", "img_1", "cls", "emb_0", "emb_1"),
    )
    return jax.shard_map(
        shards,
        mesh=torus,
        in_specs=(P(IMG, EMB), P(CLS, EMB), P(IMG), P(IMG), P(IMG), P(IMG, CLS)),
        out_specs=(P(), P(IMG, EMB), P(CLS, EMB)),
        check_vma=False,
    )
```

```python
import jax
import jax.numpy as jnp
from jax import lax
from jax.experimental import pallas as pl
from jax.experimental.pallas import tpu as pltpu
from jax.sharding import Mesh
from jax.sharding import PartitionSpec as P

CLASSES = 21504
REGIONS = 8192
EMB = ("emb_0", "emb_1")
IMG = ("img_0", "img_1")
CLS = ("cls_0", "cls_1")
NEAR = ("cls_1", "emb_0", "emb_1")
F32 = jnp.float32
BF16 = jnp.bfloat16
NT = (((1,), (1,)), ((), ()))
TN = (((0,), (0,)), ((), ()))

K, BASE, E, Y, XL, ZH = range(6)


PART = 336


def vmem(n):
    return [pl.BlockSpec(memory_space=pltpu.VMEM)] * n


def in_hbm(shape, dtype):
    return pltpu.HBM(shape, dtype)


def smem():
    return pl.BlockSpec(memory_space=pltpu.SMEM)


def params(mebibytes=16):
    return pltpu.CompilerParams(vmem_limit_bytes=mebibytes * 1024 * 1024)


def cost(flops):
    return pl.CostEstimate(flops=int(flops), bytes_accessed=1 << 20, transcendentals=0)


def swap(x, axis):
    return lax.ppermute(x, axis, [(0, 1), (1, 0)])


def split3(value, width):
    hi = value.astype(BF16).astype(F32)
    mid = (value - hi).astype(BF16).astype(F32)
    lo = value - hi - mid
    lane = lax.broadcasted_iota(jnp.int32, (8, width), 1)
    row = lax.broadcasted_iota(jnp.int32, (8, width), 0)
    packed = jnp.where(lane == 0, hi, jnp.where(lane == 1, mid, jnp.where(lane == 2, lo, 0.0)))
    return jnp.where(row == 0, packed, 0.0)


def unit_kernel(a, b, c, d, out, scale):
    blocks = [r[...].astype(F32) for r in (a, b, c, d)]
    squares = sum(jnp.sum(v * v, axis=1, keepdims=True) for v in blocks)
    inv = lax.rsqrt(squares + 1e-06)
    scale[...] = jnp.broadcast_to(inv, scale.shape)
    for q, v in enumerate(blocks):
        out[:, 256 * q : 256 * q + 256] = (v * inv).astype(BF16)


def make_unit(blocks):
    rows = blocks[0].shape[0]
    tile = 256
    return pl.pallas_call(
        unit_kernel,
        grid=(rows // tile,),
        in_specs=[pl.BlockSpec((tile, 256), lambda i: (i, 0))] * 4,
        out_specs=[
            pl.BlockSpec((tile, 1024), lambda i: (i, 0)),
            pl.BlockSpec((tile, 128), lambda i: (i, 0)),
        ],
        out_shape=[
            jax.ShapeDtypeStruct((rows, 1024), BF16),
            jax.ShapeDtypeStruct((rows, 128), F32),
        ],
        compiler_params=params(),
        cost_estimate=cost(2e7),
        name="unit",
    )(*blocks)


def rows_kernel(s, x, out):
    out[...] = x[...]


def take_rows(x, at, rows):
    return pl.pallas_call(
        rows_kernel,
        grid_spec=pltpu.PrefetchScalarGridSpec(
            num_scalar_prefetch=1,
            grid=(1,),
            in_specs=[pl.BlockSpec((rows, 256), lambda i, s: (s[0], 0))],
            out_specs=pl.BlockSpec((rows, 256), lambda i, s: (0, 0)),
        ),
        out_shape=jax.ShapeDtypeStruct((rows, 256), BF16),
        compiler_params=params(),
        name="rows",
    )(at.reshape(1), x)


def message_kernel(part, mine, theirs, out):
    count = mine[...] + theirs[...]
    high = jnp.floor(count / 32.0)
    lane = lax.broadcasted_iota(jnp.int32, (8, 128), 1)
    extra = jnp.where(lane == 0, high, jnp.where(lane == 1, count - 32.0 * high, 0.0))
    extra = jnp.concatenate([extra, jnp.zeros((8, 128), F32)], axis=1).astype(BF16)
    for y in range(4):
        out[y, 0:PART, :] = part[...]
        out[y, PART : PART + 8, :] = extra


def make_message(part, mine, theirs):
    return pl.pallas_call(
        message_kernel,
        in_specs=vmem(3),
        out_specs=vmem(1)[0],
        out_shape=in_hbm((4, PART + 8, 256), BF16),
        compiler_params=params(),
        name="message",
    )(part, mine, theirs)


def read_count(far):
    lane = lax.broadcasted_iota(jnp.int32, (1, 256), 1)
    row = sum(far[y, PART : PART + 8, :].astype(F32)[0:1, :] for y in range(4))
    return jnp.sum(jnp.where(lane == 0, 32.0 * row, jnp.where(lane == 1, row, 0.0)))


def focal_kernel(s, t0, t1, t2, t3, unit, lane_f, labels, mask, keep, send, loss, count_out, acc):
    rows = unit.shape[0]
    half = keep.shape[0]
    count = read_count(t2)
    count_out[0, 0] = count
    u = [unit[:, 256 * q : 256 * q + 256] for q in range(4)]

    def dot(t, q):
        return lax.dot_general(t, u[q], NT, preferred_element_type=F32)

    for c in range(4):
        at = slice(PART * c, PART * c + PART)
        acc[at, :] = (
            dot(t0[at, :], 0) + dot(t1[at, :], 1) + dot(t2[c, 0:PART, :], 2) + dot(t3[c, 0:PART, :], 3)
        )
    shift = lane_f[0:1, :]
    scale = lane_f[1:2, :]
    factor = scale * (REGIONS / count)
    step = 32

    def part(out, start, total):
        wanted = labels[...] - (s[BASE] + start)

        def body(g, total):
            to = pl.multiple_of(g * step, step)
            at = pl.multiple_of(start + to, step)
            logit = (acc[pl.ds(at, step), :] + shift) * scale
            ids = lax.broadcasted_iota(jnp.int32, (step, rows), 0)
            target = (wanted - to) == ids
            m = jnp.where(target, -logit, logit)
            e = jnp.exp(-jnp.abs(m))
            r = 1.0 / (1.0 + e)
            er = e * r
            positive = m >= 0.0
            prob = jnp.where(positive, r, er)
            rest = jnp.where(positive, er, r)
            series = e * (1.0 - e * (0.5 - e * (1.0 / 3.0 - e * 0.25)))
            soft = jnp.maximum(m, 0.0) + jnp.where(e < 2e-3, series, jnp.log(1.0 + e))
            weight = jnp.where(target, 0.25, 0.75) * mask[pl.ds(at, step), :] * (prob * prob)
            slope = weight * (2.0 * rest * soft + prob)
            slope = jnp.where(target, -slope, slope)
            out[pl.ds(to, step), :] = (slope * factor).astype(BF16)
            term = weight * soft
            return total + sum(term[8 * i : 8 * i + 8, :] for i in range(step // 8))

        return lax.fori_loop(0, half // step, body, total)

    total = part(send, (1 - s[K]) * half, jnp.zeros((8, rows), F32))
    total = part(keep, s[K] * half, total)
    loss[...] = sum(total[:, 128 * i : 128 * i + 128] for i in range(4))


def make_focal(scalars, tables, unit, lane_f, labels, mask):
    rows = unit.shape[0] // 2
    classes = mask.shape[0]
    whole = lambda i, s: (0, 0)
    cube = lambda i, s: (0, 0, 0)
    return pl.pallas_call(
        focal_kernel,
        grid_spec=pltpu.PrefetchScalarGridSpec(
            num_scalar_prefetch=1,
            grid=(1,),
            in_specs=[pl.BlockSpec((classes, 256), whole)] * 2
            + [pl.BlockSpec((4, PART + 8, 256), cube)] * 2
            + [
                pl.BlockSpec((rows, 1024), lambda i, s: (s[K], 0)),
                pl.BlockSpec((8, rows), lambda i, s: (0, s[K])),
                pl.BlockSpec((1, rows), lambda i, s: (0, s[K])),
                pl.BlockSpec((classes, 1), whole),
            ],
            out_specs=[
                pl.BlockSpec((classes // 2, rows), whole),
                pl.BlockSpec((classes // 2, rows), whole),
                pl.BlockSpec((8, 128), whole),
                smem(),
            ],
            scratch_shapes=[pltpu.VMEM((classes, rows), F32)],
        ),
        out_shape=[
            jax.ShapeDtypeStruct((classes // 2, rows), BF16),
            jax.ShapeDtypeStruct((classes // 2, rows), BF16),
            jax.ShapeDtypeStruct((8, 128), F32),
            jax.ShapeDtypeStruct((1, 1), F32),
        ],
        compiler_params=params(24),
        cost_estimate=cost(1.4e9),
        name="focal",
    )(scalars, *tables, unit, lane_f, labels, mask)


def region_kernel(s, keep, send, t0, t1, t2, t3, loss, a, b, c, d, inv_ref, out, acc):
    half = keep.shape[0]
    k = s[K]
    tile = acc.shape[0]
    blocks = (a, b, c, d)
    extra = split3(jnp.sum(loss[...]), 256).astype(BF16)
    mine_at = pl.multiple_of(k * half, 32)
    theirs_at = pl.multiple_of((1 - k) * half, 32)

    def dot(g, t):
        return lax.dot_general(g, t, TN, preferred_element_type=F32)

    for i in range(keep.shape[1] // tile):
        rows = slice(tile * i, tile * i + tile)
        mine = keep[:, rows]
        theirs = send[:, rows]
        inv = inv_ref[rows, 0:1]
        along = 0.0
        for q, t in enumerate((t0, t1, t2, t3)):
            if q < 2:
                part = dot(mine, t[pl.ds(mine_at, half), :]) + dot(theirs, t[pl.ds(theirs_at, half), :])
            else:
                part = sum(
                    dot(g[PART * p : PART * p + PART, :], t[2 * at + p, 0:PART, :])
                    for g, at in ((mine, k), (theirs, 1 - k))
                    for p in range(2)
                )
            acc[:, 256 * q : 256 * q + 256] = part
            along += jnp.sum(part * blocks[q][rows, :].astype(F32), axis=1, keepdims=True)
        back = inv * inv * along
        for q, r in enumerate(blocks):
            cols = slice(256 * q, 256 * q + 256)
            grad = inv * (acc[:, cols] - r[rows, :].astype(F32) * back)
            for p in range(tile // 64):
                z = tile // 64 * i + p
                out[z, 0:64, cols] = grad[64 * p : 64 * p + 64, :].astype(BF16)
                out[z, 64:72, cols] = extra


def make_region(scalars, keep, send, tables, loss, blocks, inv):
    half, rows = keep.shape
    flat = pl.BlockSpec((2 * half, 256), lambda i, s: (0, 0))
    cube = pl.BlockSpec((4, PART + 8, 256), lambda i, s: (0, 0, 0))
    return pl.pallas_call(
        region_kernel,
        grid_spec=pltpu.PrefetchScalarGridSpec(
            num_scalar_prefetch=1,
            grid=(1,),
            in_specs=[pl.BlockSpec((half, rows), lambda i, s: (0, 0))] * 2
            + [flat] * 2
            + [cube] * 2
            + [pl.BlockSpec((8, 128), lambda i, s: (0, 0))]
            + [pl.BlockSpec((rows, 256), lambda i, s: (s[K], 0))] * 4
            + [pl.BlockSpec((rows, 128), lambda i, s: (s[K], 0))],
            out_specs=pl.BlockSpec((8, 72, 1024), lambda i, s: (0, 0, 0)),
            scratch_shapes=[pltpu.VMEM((256, 1024), F32)],
        ),
        out_shape=in_hbm((8, 72, 1024), BF16),
        compiler_params=params(24),
        cost_estimate=cost(1.4e9),
        name="region",
    )(scalars, keep, send, *tables, loss, *blocks, inv)


def table_kernel(s, keep, other, unit, *refs):
    outs, acc = refs[:8], refs[8]
    _, rows = other.shape
    mine = keep[...]
    theirs = other[...]
    mine_at = pl.multiple_of(s[K] * rows, rows)
    theirs_at = pl.multiple_of((1 - s[K]) * rows, rows)
    for dy in range(4):
        cols = pl.ds(pl.multiple_of(256 * ((s[Y] + dy) % 4), 256), 256)
        acc[...] = jnp.dot(
            mine, unit[pl.ds(mine_at, rows), cols], preferred_element_type=F32
        ) + jnp.dot(theirs, unit[pl.ds(theirs_at, rows), cols], preferred_element_type=F32)
        for dx in range(2):
            at = pl.multiple_of(128 * (s[XL] ^ dx), 128)
            outs[2 * dy + dx][...] = acc[:, pl.ds(at, 128)].astype(BF16)


def make_table(scalars, keep, other, unit):
    half = other.shape[0]
    return pl.pallas_call(
        table_kernel,
        in_specs=[smem()] + vmem(3),
        out_specs=vmem(8),
        out_shape=[jax.ShapeDtypeStruct((half, 128), BF16)] * 8,
        scratch_shapes=[pltpu.VMEM((half, 256), F32)],
        compiler_params=params(),
        cost_estimate=cost(1.4e9),
        name="table",
    )(scalars, keep, other, unit)


def table_sum_kernel(*refs):
    terms, out = refs[:8], refs[8]
    out[...] = sum(t[...].astype(F32) for t in terms).astype(BF16)


def make_table_sum(terms):
    return pl.pallas_call(
        table_sum_kernel,
        in_specs=vmem(8),
        out_specs=vmem(1)[0],
        out_shape=jax.ShapeDtypeStruct(terms[0].shape, BF16),
        compiler_params=params(),
        cost_estimate=cost(1e7),
        name="table_sum",
    )(*terms)


def merge_kernel(s, terms, out):
    total = sum(terms[z].astype(F32) for z in range(8))
    loss = jnp.sum(total[64:72, 0:256])
    extra = split3(loss, 256).astype(BF16)
    total = total[0:64, :].astype(BF16)
    for q in range(4):
        to = s[E] ^ q
        for near in range(2):
            out[near, to, 0:64, :] = total[:, 256 * q : 256 * q + 256]
            out[near, to, 64:72, :] = extra


def make_merge(scalars, terms):
    return pl.pallas_call(
        merge_kernel,
        in_specs=[smem()] + vmem(1),
        out_specs=vmem(1)[0],
        out_shape=in_hbm((2, 4, 72, 256), BF16),
        compiler_params=params(),
        cost_estimate=cost(1e7),
        name="merge",
    )(scalars, terms)


def share_kernel(pieces, chunk, out, message):
    half = chunk.shape[0]
    for near in range(2):
        for k in range(2):
            both = pieces[near, 0, k, 0:64, :].astype(F32) + pieces[near, 1, k, 0:64, :].astype(F32)
            at = 128 * near + 64 * k
            out[at : at + 64, :] = both.astype(BF16)
    loss = sum(jnp.sum(pieces[0, x, k, 64:72, :].astype(F32)) for x in range(2) for k in range(2))
    extra = split3(loss, 128).astype(BF16)
    rows = chunk[...]
    for j in range(8):
        message[j, 0:half, :] = rows
        message[j, half : half + 8, :] = extra


def make_share(pieces, chunk):
    half = chunk.shape[0]
    return pl.pallas_call(
        share_kernel,
        in_specs=vmem(2),
        out_specs=vmem(2),
        out_shape=[jax.ShapeDtypeStruct((256, 256), BF16), in_hbm((8, half + 8, 128), BF16)],
        compiler_params=params(),
        cost_estimate=cost(1e7),
        name="share",
    )(pieces, chunk)


def final_kernel(s, count, tables, *refs):
    regions, (region_out, table_out, loss_out) = refs[:4], refs[4:]
    total = sum(jnp.sum(tables[j, 672:680, :].astype(F32)) for j in range(8))
    for d in range(4):
        source = (s[ZH] + 4 - d) % 4
        for near in range(2):
            for k in range(2):
                at = 128 * near + 64 * k
                region_out[k, source, near] = regions[d][at : at + 64, :]
    loss_out[0, 0] = total / count[0, 0] / CLASSES
    for y in range(4):
        at = pl.multiple_of(672 * (s[E] ^ y), 32)
        for x in range(2):
            table_out[pl.ds(at, 672), 128 * x : 128 * x + 128] = tables[2 * y + x, 0:672, :]


def make_final(scalars, count, tables, regions):
    return pl.pallas_call(
        final_kernel,
        in_specs=[smem(), smem()] + vmem(5),
        out_specs=vmem(2) + [smem()],
        out_shape=[
            jax.ShapeDtypeStruct((2, 4, 2, 64, 256), BF16),
            jax.ShapeDtypeStruct((2688, 256), BF16),
            jax.ShapeDtypeStruct((1, 1), F32),
        ],
        compiler_params=params(),
        cost_estimate=cost(1e7),
        name="final",
    )(scalars, count, tables, *regions)


def over_img(x, dy, dx):
    pairs = [
        (2 * y + xl, 2 * ((y + dy) % 4) + (xl ^ dx)) for y in range(4) for xl in range(2)
    ]
    return lax.ppermute(x, IMG, pairs)


def to_owner(x):
    axes = ("img_0",) + EMB
    return lax.ppermute(x, axes, [(4 * y + e, 4 * y + (e ^ y)) for y in range(4) for e in range(4)])


def exchange(x, axes):
    return lax.all_to_all(x, axes, split_axis=0, concat_axis=0, tiled=True)


def shards(regions, table, shift, scale, labels, valid):
    rows = regions.shape[0]
    y = lax.axis_index("img_0")
    xl = lax.axis_index("img_1")
    xh = lax.axis_index("emb_0")
    k = lax.axis_index("emb_1")
    zh = lax.axis_index("cls_0")
    z = lax.axis_index(CLS)
    scalars = jnp.stack([k, z * 2688 + xh * 1344, 2 * xh + k, y, xl, zh]).astype(jnp.int32)

    t_send = take_rows(pltpu.with_memory_space_constraint(table, pltpu.HBM), 4 * (1 - xh) + y, PART)
    t_send, regions_in = lax.optimization_barrier((t_send, regions))
    t_got = swap(t_send, "emb_0")
    r_far = swap(regions_in, "emb_0")
    r_near = swap(regions_in, "emb_1")
    local = jnp.broadcast_to(jnp.sum((labels >= 0).astype(F32)), (8, 128))
    t_far = exchange(make_message(t_got, local, swap(local, "img_1")), "img_0")
    t_own = lax.dynamic_slice_in_dim(table, xh * 1344, 1344, 0)
    t_near = swap(t_own, "emb_1")
    r_both = swap(r_far, "emb_1")
    t_both = swap(t_far, "emb_1")
    blocks = (regions, r_near, r_far, r_both)
    tables = (t_own, t_near, t_far, t_both)
    unit, inv = make_unit(blocks)

    lane_f = jnp.concatenate([shift[None], scale[None], jnp.zeros((6, rows), F32)], axis=0)
    mask = lax.dynamic_slice(valid, (k, xh * 1344), (1, 1344)).astype(F32).T
    keep, send, loss, count = make_focal(scalars, tables, unit, lane_f, labels[None], mask)

    theirs = swap(send, "emb_1")
    terms = exchange(make_region(scalars, keep, send, tables, loss, blocks, inv), CLS)
    chunks = list(make_table(scalars, keep, theirs, unit))
    for o in range(1, 8):
        chunks[o] = over_img(chunks[o], o // 2, o % 2)
    table_part = to_owner(make_table_sum(chunks))
    merged = make_merge(scalars, terms)
    pieces = exchange(merged.reshape(8, 72, 256), NEAR).reshape(2, 2, 2, 72, 256)
    share, message = make_share(pieces, table_part)
    table_all = exchange(message, IMG)
    shares = [share] + [
        lax.ppermute(share, "cls_0", [(i, (i + d) % 4) for i in range(4)]) for d in range(1, 4)
    ]
    region_grad, table_grad, total = make_final(scalars, count, table_all, shares)
    return (total[0, 0], region_grad.reshape(rows, 256), table_grad)


def solution(mesh):
    torus = Mesh(
        mesh.devices.reshape(4, 2, 4, 2, 2, 2),
        ("img_0", "img_1", "cls_0", "cls_1", "emb_0", "emb_1"),
    )
    return jax.shard_map(
        shards,
        mesh=torus,
        in_specs=(P(IMG, EMB), P(CLS, EMB), P(IMG), P(IMG), P(IMG), P(IMG, CLS)),
        out_specs=(P(), P(IMG, EMB), P(CLS, EMB)),
        check_vma=False,
    )
```

```python
import jax
import jax.numpy as jnp
from jax import lax
from jax.experimental import pallas as pl
from jax.experimental.pallas import tpu as pltpu
from jax.sharding import Mesh
from jax.sharding import PartitionSpec as P

CLASSES = 21504
REGIONS = 8192
EMB = ("emb_0", "emb_1")
IMG = ("img_0", "img_1")
CLS = ("cls_0", "cls_1")
NEAR = ("cls_1", "emb_0", "emb_1")
F32 = jnp.float32
BF16 = jnp.bfloat16
NT = (((1,), (1,)), ((), ()))
TN = (((0,), (0,)), ((), ()))

K, BASE, E, Y, XL, ZH = range(6)


PART = 336


def vmem(n):
    return [pl.BlockSpec(memory_space=pltpu.VMEM)] * n


def in_hbm(shape, dtype):
    return pltpu.HBM(shape, dtype)


def smem():
    return pl.BlockSpec(memory_space=pltpu.SMEM)


def params(mebibytes=16):
    return pltpu.CompilerParams(vmem_limit_bytes=mebibytes * 1024 * 1024)


def cost(flops):
    return pl.CostEstimate(flops=int(flops), bytes_accessed=1 << 20, transcendentals=0)


def swap(x, axis):
    return lax.ppermute(x, axis, [(0, 1), (1, 0)])


def split3(value, width):
    hi = value.astype(BF16).astype(F32)
    mid = (value - hi).astype(BF16).astype(F32)
    lo = value - hi - mid
    lane = lax.broadcasted_iota(jnp.int32, (8, width), 1)
    row = lax.broadcasted_iota(jnp.int32, (8, width), 0)
    packed = jnp.where(lane == 0, hi, jnp.where(lane == 1, mid, jnp.where(lane == 2, lo, 0.0)))
    return jnp.where(row == 0, packed, 0.0)


def unit_kernel(a, b, c, d, out, scale):
    blocks = [r[...].astype(F32) for r in (a, b, c, d)]
    squares = sum(jnp.sum(v * v, axis=1, keepdims=True) for v in blocks)
    inv = lax.rsqrt(squares + 1e-06)
    scale[...] = jnp.broadcast_to(inv, scale.shape)
    for q, v in enumerate(blocks):
        out[:, 256 * q : 256 * q + 256] = (v * inv).astype(BF16)


def make_unit(blocks):
    rows = blocks[0].shape[0]
    tile = 256
    return pl.pallas_call(
        unit_kernel,
        grid=(rows // tile,),
        in_specs=[pl.BlockSpec((tile, 256), lambda i: (i, 0))] * 4,
        out_specs=[
            pl.BlockSpec((tile, 1024), lambda i: (i, 0)),
            pl.BlockSpec((tile, 128), lambda i: (i, 0)),
        ],
        out_shape=[
            jax.ShapeDtypeStruct((rows, 1024), BF16),
            jax.ShapeDtypeStruct((rows, 128), F32),
        ],
        compiler_params=params(),
        cost_estimate=cost(2e7),
        name="unit",
    )(*blocks)


def rows_kernel(s, x, out):
    out[...] = x[...]


def take_rows(x, at, rows):
    return pl.pallas_call(
        rows_kernel,
        grid_spec=pltpu.PrefetchScalarGridSpec(
            num_scalar_prefetch=1,
            grid=(1,),
            in_specs=[pl.BlockSpec((rows, 256), lambda i, s: (s[0], 0))],
            out_specs=pl.BlockSpec((rows, 256), lambda i, s: (0, 0)),
        ),
        out_shape=jax.ShapeDtypeStruct((rows, 256), BF16),
        compiler_params=params(),
        name="rows",
    )(at.reshape(1), x)


def message_kernel(part, mine, theirs, out):
    count = mine[...] + theirs[...]
    high = jnp.floor(count / 32.0)
    lane = lax.broadcasted_iota(jnp.int32, (8, 128), 1)
    extra = jnp.where(lane == 0, high, jnp.where(lane == 1, count - 32.0 * high, 0.0))
    extra = jnp.concatenate([extra, jnp.zeros((8, 128), F32)], axis=1).astype(BF16)
    for y in range(4):
        out[y, 0:PART, :] = part[...]
        out[y, PART : PART + 8, :] = extra


def make_message(part, mine, theirs):
    return pl.pallas_call(
        message_kernel,
        in_specs=vmem(3),
        out_specs=vmem(1)[0],
        out_shape=in_hbm((4, PART + 8, 256), BF16),
        compiler_params=params(),
        name="message",
    )(part, mine, theirs)


def read_count(far):
    lane = lax.broadcasted_iota(jnp.int32, (1, 256), 1)
    row = sum(far[y, PART : PART + 8, :].astype(F32)[0:1, :] for y in range(4))
    return jnp.sum(jnp.where(lane == 0, 32.0 * row, jnp.where(lane == 1, row, 0.0)))


def focal_kernel(s, t0, t1, t2, t3, unit, lane_f, labels, mask, keep, send, loss, count_out, acc):
    rows = unit.shape[0]
    half = keep.shape[0]
    count = read_count(t2)
    count_out[0, 0] = count
    u = [unit[:, 256 * q : 256 * q + 256] for q in range(4)]

    def dot(t, q):
        return lax.dot_general(t, u[q], NT, preferred_element_type=F32)

    for c in range(4):
        at = slice(PART * c, PART * c + PART)
        acc[at, :] = (
            dot(t0[at, :], 0) + dot(t1[at, :], 1) + dot(t2[c, 0:PART, :], 2) + dot(t3[c, 0:PART, :], 3)
        )
    shift = lane_f[0:1, :]
    scale = lane_f[1:2, :]
    factor = scale * (REGIONS / count)
    step = 32

    def part(out, start, total):
        wanted = labels[...] - (s[BASE] + start)

        def body(g, total):
            to = pl.multiple_of(g * step, step)
            at = pl.multiple_of(start + to, step)
            logit = (acc[pl.ds(at, step), :] + shift) * scale
            ids = lax.broadcasted_iota(jnp.int32, (step, rows), 0)
            target = (wanted - to) == ids
            m = jnp.where(target, -logit, logit)
            e = jnp.exp(-jnp.abs(m))
            r = 1.0 / (1.0 + e)
            er = e * r
            positive = m >= 0.0
            prob = jnp.where(positive, r, er)
            rest = jnp.where(positive, er, r)
            series = e * (1.0 - e * (0.5 - e * (1.0 / 3.0 - e * 0.25)))
            soft = jnp.maximum(m, 0.0) + jnp.where(e < 2e-3, series, jnp.log(1.0 + e))
            weight = jnp.where(target, 0.25, 0.75) * mask[pl.ds(at, step), :] * (prob * prob)
            slope = weight * (2.0 * rest * soft + prob)
            slope = jnp.where(target, -slope, slope)
            out[pl.ds(to, step), :] = (slope * factor).astype(BF16)
            term = weight * soft
            return total + sum(term[8 * i : 8 * i + 8, :] for i in range(step // 8))

        return lax.fori_loop(0, half // step, body, total)

    total = part(send, (1 - s[K]) * half, jnp.zeros((8, rows), F32))
    total = part(keep, s[K] * half, total)
    loss[...] = sum(total[:, 128 * i : 128 * i + 128] for i in range(4))


def make_focal(scalars, tables, unit, lane_f, labels, mask):
    rows = unit.shape[0] // 2
    classes = mask.shape[0]
    whole = lambda i, s: (0, 0)
    cube = lambda i, s: (0, 0, 0)
    return pl.pallas_call(
        focal_kernel,
        grid_spec=pltpu.PrefetchScalarGridSpec(
            num_scalar_prefetch=1,
            grid=(1,),
            in_specs=[pl.BlockSpec((classes, 256), whole)] * 2
            + [pl.BlockSpec((4, PART + 8, 256), cube)] * 2
            + [
                pl.BlockSpec((rows, 1024), lambda i, s: (s[K], 0)),
                pl.BlockSpec((8, rows), lambda i, s: (0, s[K])),
                pl.BlockSpec((1, rows), lambda i, s: (0, s[K])),
                pl.BlockSpec((classes, 1), whole),
            ],
            out_specs=[
                pl.BlockSpec((classes // 2, rows), whole),
                pl.BlockSpec((classes // 2, rows), whole),
                pl.BlockSpec((8, 128), whole),
                smem(),
            ],
            scratch_shapes=[pltpu.VMEM((classes, rows), F32)],
        ),
        out_shape=[
            jax.ShapeDtypeStruct((classes // 2, rows), BF16),
            jax.ShapeDtypeStruct((classes // 2, rows), BF16),
            jax.ShapeDtypeStruct((8, 128), F32),
            jax.ShapeDtypeStruct((1, 1), F32),
        ],
        compiler_params=params(24),
        cost_estimate=cost(1.4e9),
        name="focal",
    )(scalars, *tables, unit, lane_f, labels, mask)


def region_kernel(s, keep, send, t0, t1, t2, t3, a, b, c, d, inv_ref, out, acc):
    half = keep.shape[0]
    k = s[K]
    tile = acc.shape[0]
    blocks = (a, b, c, d)
    mine_at = pl.multiple_of(k * half, 32)
    theirs_at = pl.multiple_of((1 - k) * half, 32)

    def dot(g, t):
        return lax.dot_general(g, t, TN, preferred_element_type=F32)

    for i in range(keep.shape[1] // tile):
        rows = slice(tile * i, tile * i + tile)
        mine = keep[:, rows]
        theirs = send[:, rows]
        inv = inv_ref[rows, 0:1]
        along = 0.0
        for q, t in enumerate((t0, t1, t2, t3)):
            if q < 2:
                part = dot(mine, t[pl.ds(mine_at, half), :]) + dot(theirs, t[pl.ds(theirs_at, half), :])
            else:
                part = sum(
                    dot(g[PART * p : PART * p + PART, :], t[2 * at + p, 0:PART, :])
                    for g, at in ((mine, k), (theirs, 1 - k))
                    for p in range(2)
                )
            acc[:, 256 * q : 256 * q + 256] = part
            along += jnp.sum(part * blocks[q][rows, :].astype(F32), axis=1, keepdims=True)
        back = inv * inv * along
        for q, r in enumerate(blocks):
            cols = slice(256 * q, 256 * q + 256)
            grad = inv * (acc[:, cols] - r[rows, :].astype(F32) * back)
            for p in range(tile // 64):
                z = tile // 64 * i + p
                out[z, :, cols] = grad[64 * p : 64 * p + 64, :].astype(BF16)


def make_region(scalars, keep, send, tables, blocks, inv):
    half, rows = keep.shape
    flat = pl.BlockSpec((2 * half, 256), lambda i, s: (0, 0))
    cube = pl.BlockSpec((4, PART + 8, 256), lambda i, s: (0, 0, 0))
    return pl.pallas_call(
        region_kernel,
        grid_spec=pltpu.PrefetchScalarGridSpec(
            num_scalar_prefetch=1,
            grid=(1,),
            in_specs=[pl.BlockSpec((half, rows), lambda i, s: (0, 0))] * 2
            + [flat] * 2
            + [cube] * 2
            + [pl.BlockSpec((rows, 256), lambda i, s: (s[K], 0))] * 4
            + [pl.BlockSpec((rows, 128), lambda i, s: (s[K], 0))],
            out_specs=pl.BlockSpec((8, 64, 1024), lambda i, s: (0, 0, 0)),
            scratch_shapes=[pltpu.VMEM((256, 1024), F32)],
        ),
        out_shape=in_hbm((8, 64, 1024), BF16),
        compiler_params=params(24),
        cost_estimate=cost(1.4e9),
        name="region",
    )(scalars, keep, send, *tables, *blocks, inv)


def table_kernel(s, keep, other, unit, loss, *refs):
    outs, acc = refs[:8], refs[8]
    half, rows = other.shape
    mine = keep[...]
    theirs = other[...]
    mine_at = pl.multiple_of(s[K] * rows, rows)
    theirs_at = pl.multiple_of((1 - s[K]) * rows, rows)
    extra = split3(jnp.sum(loss[...]), 128).astype(BF16)
    for dy in range(4):
        cols = pl.ds(pl.multiple_of(256 * ((s[Y] + dy) % 4), 256), 256)
        acc[...] = jnp.dot(
            mine, unit[pl.ds(mine_at, rows), cols], preferred_element_type=F32
        ) + jnp.dot(theirs, unit[pl.ds(theirs_at, rows), cols], preferred_element_type=F32)
        for dx in range(2):
            at = pl.multiple_of(128 * (s[XL] ^ dx), 128)
            out = outs[2 * dy + dx]
            out[0:half, :] = acc[:, pl.ds(at, 128)].astype(BF16)
            out[half : half + 8, :] = extra


def make_table(scalars, keep, other, unit, loss):
    half = other.shape[0]
    return pl.pallas_call(
        table_kernel,
        in_specs=[smem()] + vmem(4),
        out_specs=vmem(8),
        out_shape=[jax.ShapeDtypeStruct((half + 8, 128), BF16)] * 8,
        scratch_shapes=[pltpu.VMEM((half, 256), F32)],
        compiler_params=params(),
        cost_estimate=cost(1.4e9),
        name="table",
    )(scalars, keep, other, unit, loss)


def table_sum_kernel(*refs):
    terms, (out, loss) = refs[:8], refs[8:]
    half = out.shape[0]
    out[...] = sum(t[0:half, :].astype(F32) for t in terms).astype(BF16)
    loss[...] = sum(t[half : half + 8, :].astype(F32) for t in terms)


def make_table_sum(terms):
    return pl.pallas_call(
        table_sum_kernel,
        in_specs=vmem(8),
        out_specs=vmem(2),
        out_shape=[
            jax.ShapeDtypeStruct((terms[0].shape[0] - 8, 128), BF16),
            jax.ShapeDtypeStruct((8, 128), F32),
        ],
        compiler_params=params(),
        cost_estimate=cost(1e7),
        name="table_sum",
    )(*terms)


def merge_kernel(s, terms, loss, out):
    total = sum(terms[z].astype(F32) for z in range(8)).astype(BF16)
    extra = split3(jnp.sum(loss[...]), 256).astype(BF16)
    for q in range(4):
        to = s[E] ^ q
        for near in range(2):
            out[near, to, 0:64, :] = total[:, 256 * q : 256 * q + 256]
            out[near, to, 64:72, :] = extra


def make_merge(scalars, terms, loss):
    return pl.pallas_call(
        merge_kernel,
        in_specs=[smem()] + vmem(2),
        out_specs=vmem(1)[0],
        out_shape=in_hbm((2, 4, 72, 256), BF16),
        compiler_params=params(),
        cost_estimate=cost(1e7),
        name="merge",
    )(scalars, terms, loss)


def share_kernel(pieces, chunk, out, message):
    for near in range(2):
        for k in range(2):
            both = pieces[near, 0, k, 0:64, :].astype(F32) + pieces[near, 1, k, 0:64, :].astype(F32)
            at = 128 * near + 64 * k
            out[at : at + 64, :] = both.astype(BF16)
    loss = sum(
        jnp.sum(pieces[near, x, k, 64:72, :].astype(F32))
        for near in range(2)
        for x in range(2)
        for k in range(2)
    )
    out[256:264, :] = split3(loss, 256).astype(BF16)
    rows = chunk[...]
    for j in range(8):
        message[j] = rows


def make_share(pieces, chunk):
    half = chunk.shape[0]
    return pl.pallas_call(
        share_kernel,
        in_specs=vmem(2),
        out_specs=vmem(2),
        out_shape=[jax.ShapeDtypeStruct((264, 256), BF16), in_hbm((8, half, 128), BF16)],
        compiler_params=params(),
        cost_estimate=cost(1e7),
        name="share",
    )(pieces, chunk)


def final_kernel(s, count, tables, *refs):
    regions, (region_out, table_out, loss_out) = refs[:4], refs[4:]
    total = 0.0
    for d in range(4):
        source = (s[ZH] + 4 - d) % 4
        for near in range(2):
            for k in range(2):
                at = 128 * near + 64 * k
                region_out[k, source, near] = regions[d][at : at + 64, :]
        total += jnp.sum(regions[d][256:264, :].astype(F32))
    loss_out[0, 0] = total / count[0, 0] / CLASSES
    for y in range(4):
        at = pl.multiple_of(672 * (s[E] ^ y), 32)
        for x in range(2):
            table_out[pl.ds(at, 672), 128 * x : 128 * x + 128] = tables[2 * y + x]


def make_final(scalars, count, tables, regions):
    return pl.pallas_call(
        final_kernel,
        in_specs=[smem(), smem()] + vmem(5),
        out_specs=vmem(2) + [smem()],
        out_shape=[
            jax.ShapeDtypeStruct((2, 4, 2, 64, 256), BF16),
            jax.ShapeDtypeStruct((2688, 256), BF16),
            jax.ShapeDtypeStruct((1, 1), F32),
        ],
        compiler_params=params(),
        cost_estimate=cost(1e7),
        name="final",
    )(scalars, count, tables, *regions)


def over_img(x, dy, dx):
    pairs = [
        (2 * y + xl, 2 * ((y + dy) % 4) + (xl ^ dx)) for y in range(4) for xl in range(2)
    ]
    return lax.ppermute(x, IMG, pairs)


def to_owner(x):
    axes = ("img_0",) + EMB
    return lax.ppermute(x, axes, [(4 * y + e, 4 * y + (e ^ y)) for y in range(4) for e in range(4)])


def exchange(x, axes):
    return lax.all_to_all(x, axes, split_axis=0, concat_axis=0, tiled=True)


def shards(regions, table, shift, scale, labels, valid):
    rows = regions.shape[0]
    y = lax.axis_index("img_0")
    xl = lax.axis_index("img_1")
    xh = lax.axis_index("emb_0")
    k = lax.axis_index("emb_1")
    zh = lax.axis_index("cls_0")
    z = lax.axis_index(CLS)
    scalars = jnp.stack([k, z * 2688 + xh * 1344, 2 * xh + k, y, xl, zh]).astype(jnp.int32)

    t_send = take_rows(pltpu.with_memory_space_constraint(table, pltpu.HBM), 4 * (1 - xh) + y, PART)
    t_send, regions_in = lax.optimization_barrier((t_send, regions))
    t_got = swap(t_send, "emb_0")
    r_far = swap(regions_in, "emb_0")
    r_near = swap(regions_in, "emb_1")
    local = jnp.broadcast_to(jnp.sum((labels >= 0).astype(F32)), (8, 128))
    local_other = swap(local, "img_1")
    t_far = exchange(make_message(t_got, local, local_other), "img_0")
    t_own = lax.dynamic_slice_in_dim(table, xh * 1344, 1344, 0)
    t_near = swap(t_own, "emb_1")
    r_both = swap(r_far, "emb_1")
    t_both = swap(t_far, "emb_1")
    blocks = (regions, r_near, r_far, r_both)
    tables = (t_own, t_near, t_far, t_both)
    unit, inv = make_unit(blocks)

    lane_f = jnp.concatenate([shift[None], scale[None], jnp.zeros((6, rows), F32)], axis=0)
    mask = lax.dynamic_slice(valid, (k, xh * 1344), (1, 1344)).astype(F32).T
    keep, send, loss, count = make_focal(scalars, tables, unit, lane_f, labels[None], mask)

    theirs = swap(send, "emb_1")
    terms = exchange(make_region(scalars, keep, send, tables, blocks, inv), CLS)
    chunks = list(make_table(scalars, keep, theirs, unit, loss))
    for o in range(1, 8):
        chunks[o] = over_img(chunks[o], o // 2, o % 2)
    table_part, loss_part = make_table_sum(chunks)
    table_part = to_owner(table_part)
    merged = make_merge(scalars, terms, loss_part)
    pieces = exchange(merged.reshape(8, 72, 256), NEAR).reshape(2, 2, 2, 72, 256)
    share, message = make_share(pieces, table_part)
    table_all = exchange(message, IMG)
    shares = [share] + [
        lax.ppermute(share, "cls_0", [(i, (i + d) % 4) for i in range(4)]) for d in range(1, 4)
    ]
    region_grad, table_grad, total = make_final(scalars, count, table_all, shares)
    return (total[0, 0], region_grad.reshape(rows, 256), table_grad)


def solution(mesh):
    torus = Mesh(
        mesh.devices.reshape(4, 2, 4, 2, 2, 2),
        ("img_0", "img_1", "cls_0", "cls_1", "emb_0", "emb_1"),
    )
    return jax.shard_map(
        shards,
        mesh=torus,
        in_specs=(P(IMG, EMB), P(CLS, EMB), P(IMG), P(IMG), P(IMG), P(IMG, CLS)),
        out_specs=(P(), P(IMG, EMB), P(CLS, EMB)),
        check_vma=False,
    )
```

```python
import jax
import jax.numpy as jnp
from jax import lax
from jax.experimental import pallas as pl
from jax.experimental.pallas import tpu as pltpu
from jax.sharding import Mesh
from jax.sharding import PartitionSpec as P

CLASSES = 21504
REGIONS = 8192
EMB = ("emb_0", "emb_1")
IMG = ("img_0", "img_1")
CLS = ("cls",)
F32 = jnp.float32
BF16 = jnp.bfloat16
NT = (((1,), (1,)), ((), ()))
TN = (((0,), (0,)), ((), ()))

K, BASE, E, Y, XL, Z = range(6)


PART = 336


def vmem(n):
    return [pl.BlockSpec(memory_space=pltpu.VMEM)] * n


def in_hbm(shape, dtype):
    return pltpu.HBM(shape, dtype)


def smem():
    return pl.BlockSpec(memory_space=pltpu.SMEM)


def params(mebibytes=16):
    return pltpu.CompilerParams(vmem_limit_bytes=mebibytes * 1024 * 1024)


def cost(flops):
    return pl.CostEstimate(flops=int(flops), bytes_accessed=1 << 20, transcendentals=0)


def swap(x, axis):
    return lax.ppermute(x, axis, [(0, 1), (1, 0)])


def split3(value, width):
    hi = value.astype(BF16).astype(F32)
    mid = (value - hi).astype(BF16).astype(F32)
    lo = value - hi - mid
    lane = lax.broadcasted_iota(jnp.int32, (8, width), 1)
    row = lax.broadcasted_iota(jnp.int32, (8, width), 0)
    packed = jnp.where(lane == 0, hi, jnp.where(lane == 1, mid, jnp.where(lane == 2, lo, 0.0)))
    return jnp.where(row == 0, packed, 0.0)


def unit_kernel(a, b, c, d, out, scale):
    blocks = [r[...].astype(F32) for r in (a, b, c, d)]
    squares = sum(jnp.sum(v * v, axis=1, keepdims=True) for v in blocks)
    inv = lax.rsqrt(squares + 1e-06)
    scale[...] = jnp.broadcast_to(inv, scale.shape)
    for q, v in enumerate(blocks):
        out[:, 256 * q : 256 * q + 256] = (v * inv).astype(BF16)


def make_unit(blocks):
    rows = blocks[0].shape[0]
    tile = 256
    return pl.pallas_call(
        unit_kernel,
        grid=(rows // tile,),
        in_specs=[pl.BlockSpec((tile, 256), lambda i: (i, 0))] * 4,
        out_specs=[
            pl.BlockSpec((tile, 1024), lambda i: (i, 0)),
            pl.BlockSpec((tile, 128), lambda i: (i, 0)),
        ],
        out_shape=[
            jax.ShapeDtypeStruct((rows, 1024), BF16),
            jax.ShapeDtypeStruct((rows, 128), F32),
        ],
        compiler_params=params(),
        cost_estimate=cost(2e7),
        name="unit",
    )(*blocks)


def rows_kernel(s, x, out):
    out[...] = x[...]


def take_rows(x, at, rows):
    return pl.pallas_call(
        rows_kernel,
        grid_spec=pltpu.PrefetchScalarGridSpec(
            num_scalar_prefetch=1,
            grid=(1,),
            in_specs=[pl.BlockSpec((rows, 256), lambda i, s: (s[0], 0))],
            out_specs=pl.BlockSpec((rows, 256), lambda i, s: (0, 0)),
        ),
        out_shape=jax.ShapeDtypeStruct((rows, 256), BF16),
        compiler_params=params(),
        name="rows",
    )(at.reshape(1), x)


def message_kernel(part, mine, theirs, out):
    count = mine[...] + theirs[...]
    high = jnp.floor(count / 32.0)
    lane = lax.broadcasted_iota(jnp.int32, (8, 128), 1)
    extra = jnp.where(lane == 0, high, jnp.where(lane == 1, count - 32.0 * high, 0.0))
    extra = jnp.concatenate([extra, jnp.zeros((8, 128), F32)], axis=1).astype(BF16)
    for y in range(4):
        out[y, 0:PART, :] = part[...]
        out[y, PART : PART + 8, :] = extra


def make_message(part, mine, theirs):
    return pl.pallas_call(
        message_kernel,
        in_specs=vmem(3),
        out_specs=vmem(1)[0],
        out_shape=in_hbm((4, PART + 8, 256), BF16),
        compiler_params=params(),
        name="message",
    )(part, mine, theirs)


def read_count(far):
    lane = lax.broadcasted_iota(jnp.int32, (1, 256), 1)
    row = sum(far[y, PART : PART + 8, :].astype(F32)[0:1, :] for y in range(4))
    return jnp.sum(jnp.where(lane == 0, 32.0 * row, jnp.where(lane == 1, row, 0.0)))


def focal_kernel(s, t0, t1, t2, t3, unit, lane_f, labels, mask, keep, send, loss, count_out, acc):
    rows = unit.shape[0]
    half = keep.shape[0]
    count = read_count(t2)
    count_out[0, 0] = count
    u = [unit[:, 256 * q : 256 * q + 256] for q in range(4)]

    def dot(t, q):
        return lax.dot_general(t, u[q], NT, preferred_element_type=F32)

    for c in range(4):
        at = slice(PART * c, PART * c + PART)
        acc[at, :] = (
            dot(t0[at, :], 0) + dot(t1[at, :], 1) + dot(t2[c, 0:PART, :], 2) + dot(t3[c, 0:PART, :], 3)
        )
    shift = lane_f[0:1, :]
    scale = lane_f[1:2, :]
    factor = scale * (REGIONS / count)
    step = 32

    def part(out, start, total):
        wanted = labels[...] - (s[BASE] + start)

        def body(g, total):
            to = pl.multiple_of(g * step, step)
            at = pl.multiple_of(start + to, step)
            logit = (acc[pl.ds(at, step), :] + shift) * scale
            ids = lax.broadcasted_iota(jnp.int32, (step, rows), 0)
            target = (wanted - to) == ids
            m = jnp.where(target, -logit, logit)
            e = jnp.exp(-jnp.abs(m))
            r = 1.0 / (1.0 + e)
            er = e * r
            positive = m >= 0.0
            prob = jnp.where(positive, r, er)
            rest = jnp.where(positive, er, r)
            series = e * (1.0 - e * (0.5 - e * (1.0 / 3.0 - e * 0.25)))
            soft = jnp.maximum(m, 0.0) + jnp.where(e < 2e-3, series, jnp.log(1.0 + e))
            weight = jnp.where(target, 0.25, 0.75) * mask[pl.ds(at, step), :] * (prob * prob)
            slope = weight * (2.0 * rest * soft + prob)
            slope = jnp.where(target, -slope, slope)
            out[pl.ds(to, step), :] = (slope * factor).astype(BF16)
            term = weight * soft
            return total + sum(term[8 * i : 8 * i + 8, :] for i in range(step // 8))

        return lax.fori_loop(0, half // step, body, total)

    total = part(send, (1 - s[K]) * half, jnp.zeros((8, rows), F32))
    total = part(keep, s[K] * half, total)
    loss[...] = sum(total[:, 128 * i : 128 * i + 128] for i in range(4))


def make_focal(scalars, tables, unit, lane_f, labels, mask):
    rows = unit.shape[0] // 2
    classes = mask.shape[0]
    whole = lambda i, s: (0, 0)
    cube = lambda i, s: (0, 0, 0)
    return pl.pallas_call(
        focal_kernel,
        grid_spec=pltpu.PrefetchScalarGridSpec(
            num_scalar_prefetch=1,
            grid=(1,),
            in_specs=[pl.BlockSpec((classes, 256), whole)] * 2
            + [pl.BlockSpec((4, PART + 8, 256), cube)] * 2
            + [
                pl.BlockSpec((rows, 1024), lambda i, s: (s[K], 0)),
                pl.BlockSpec((8, rows), lambda i, s: (0, s[K])),
                pl.BlockSpec((1, rows), lambda i, s: (0, s[K])),
                pl.BlockSpec((classes, 1), whole),
            ],
            out_specs=[
                pl.BlockSpec((classes // 2, rows), whole),
                pl.BlockSpec((classes // 2, rows), whole),
                pl.BlockSpec((8, 128), whole),
                smem(),
            ],
            scratch_shapes=[pltpu.VMEM((classes, rows), F32)],
        ),
        out_shape=[
            jax.ShapeDtypeStruct((classes // 2, rows), BF16),
            jax.ShapeDtypeStruct((classes // 2, rows), BF16),
            jax.ShapeDtypeStruct((8, 128), F32),
            jax.ShapeDtypeStruct((1, 1), F32),
        ],
        compiler_params=params(24),
        cost_estimate=cost(1.4e9),
        name="focal",
    )(scalars, *tables, unit, lane_f, labels, mask)


def region_kernel(s, keep, send, t0, t1, t2, t3, a, b, c, d, inv_ref, out, acc):
    half = keep.shape[0]
    k = s[K]
    tile = acc.shape[0]
    blocks = (a, b, c, d)
    mine_at = pl.multiple_of(k * half, 32)
    theirs_at = pl.multiple_of((1 - k) * half, 32)

    def dot(g, t):
        return lax.dot_general(g, t, TN, preferred_element_type=F32)

    for i in range(keep.shape[1] // tile):
        rows = slice(tile * i, tile * i + tile)
        mine = keep[:, rows]
        theirs = send[:, rows]
        here = pl.ds(pl.multiple_of(keep.shape[1] * k + tile * i, tile), tile)
        inv = inv_ref[here, 0:1]
        along = 0.0
        for q, t in enumerate((t0, t1, t2, t3)):
            if q < 2:
                part = dot(mine, t[pl.ds(mine_at, half), :]) + dot(theirs, t[pl.ds(theirs_at, half), :])
            else:
                part = sum(
                    dot(g[PART * p : PART * p + PART, :], t[2 * at + p, 0:PART, :])
                    for g, at in ((mine, k), (theirs, 1 - k))
                    for p in range(2)
                )
            acc[:, 256 * q : 256 * q + 256] = part
            along += jnp.sum(part * blocks[q][here, :].astype(F32), axis=1, keepdims=True)
        back = inv * inv * along
        for q, r in enumerate(blocks):
            cols = slice(256 * q, 256 * q + 256)
            grad = inv * (acc[:, cols] - r[here, :].astype(F32) * back)
            for p in range(tile // 64):
                z = tile // 64 * i + p
                out[z, :, cols] = grad[64 * p : 64 * p + 64, :].astype(BF16)


def make_region(scalars, keep, send, tables, blocks, inv):
    return pl.pallas_call(
        region_kernel,
        in_specs=[smem()] + vmem(11),
        out_specs=vmem(1)[0],
        out_shape=in_hbm((8, 64, 1024), BF16),
        scratch_shapes=[pltpu.VMEM((256, 1024), F32)],
        compiler_params=params(24),
        cost_estimate=cost(1.4e9),
        name="region",
    )(scalars, keep, send, *tables, *blocks, inv)


def table_kernel(s, keep, other, unit, loss, *refs):
    outs, acc = refs[:8], refs[8]
    half, rows = other.shape
    mine = keep[...]
    theirs = other[...]
    mine_at = pl.multiple_of(s[K] * rows, rows)
    theirs_at = pl.multiple_of((1 - s[K]) * rows, rows)
    extra = split3(jnp.sum(loss[...]), 128).astype(BF16)
    for dy in range(4):
        cols = pl.ds(pl.multiple_of(256 * ((s[Y] + dy) % 4), 256), 256)
        acc[...] = jnp.dot(
            mine, unit[pl.ds(mine_at, rows), cols], preferred_element_type=F32
        ) + jnp.dot(theirs, unit[pl.ds(theirs_at, rows), cols], preferred_element_type=F32)
        for dx in range(2):
            at = pl.multiple_of(128 * (s[XL] ^ dx), 128)
            out = outs[2 * dy + dx]
            out[0:half, :] = acc[:, pl.ds(at, 128)].astype(BF16)
            out[half : half + 8, :] = extra


def make_table(scalars, keep, other, unit, loss):
    half = other.shape[0]
    return pl.pallas_call(
        table_kernel,
        in_specs=[smem()] + vmem(4),
        out_specs=vmem(8),
        out_shape=[jax.ShapeDtypeStruct((half + 8, 128), BF16)] * 8,
        scratch_shapes=[pltpu.VMEM((half, 256), F32)],
        compiler_params=params(),
        cost_estimate=cost(1.4e9),
        name="table",
    )(scalars, keep, other, unit, loss)


def table_sum_kernel(*refs):
    terms, (out, loss) = refs[:8], refs[8:]
    half = out.shape[0]
    out[...] = sum(t[0:half, :].astype(F32) for t in terms).astype(BF16)
    loss[...] = sum(t[half : half + 8, :].astype(F32) for t in terms)


def make_table_sum(terms):
    return pl.pallas_call(
        table_sum_kernel,
        in_specs=vmem(8),
        out_specs=vmem(2),
        out_shape=[
            jax.ShapeDtypeStruct((terms[0].shape[0] - 8, 128), BF16),
            jax.ShapeDtypeStruct((8, 128), F32),
        ],
        compiler_params=params(),
        cost_estimate=cost(1e7),
        name="table_sum",
    )(*terms)


def merge_kernel(terms, loss, *outs):
    total = sum(terms[z].astype(F32) for z in range(8)).astype(BF16)
    extra = split3(jnp.sum(loss[...]), 256).astype(BF16)
    for q, out in enumerate(outs):
        out[0:64, :] = total[:, 256 * q : 256 * q + 256]
        out[64:72, :] = extra


def make_merge(terms, loss):
    return pl.pallas_call(
        merge_kernel,
        in_specs=vmem(2),
        out_specs=vmem(4),
        out_shape=[jax.ShapeDtypeStruct((72, 256), BF16)] * 4,
        compiler_params=params(),
        cost_estimate=cost(1e7),
        name="merge",
    )(terms, loss)


def gather_kernel(chunk, out):
    rows = chunk[...]
    for j in range(8):
        out[j] = rows


def make_gather(chunk):
    return pl.pallas_call(
        gather_kernel,
        in_specs=vmem(1),
        out_specs=vmem(1)[0],
        out_shape=in_hbm((8,) + chunk.shape, BF16),
        compiler_params=params(),
        cost_estimate=cost(1e7),
        name="gather",
    )(chunk)


def share_kernel(s, own, near, far, both, out):
    k = s[K]
    for at, a, b in ((k, own, far), (1 - k, near, both)):
        total = a[0:64, :].astype(F32) + b[0:64, :].astype(F32)
        out[pl.ds(pl.multiple_of(64 * at, 64), 64), :] = total.astype(BF16)
    loss = sum(jnp.sum(r[64:72, :].astype(F32)) for r in (own, near, far, both))
    out[128:136, :] = split3(loss, 256).astype(BF16)


def make_share(scalars, parts):
    return pl.pallas_call(
        share_kernel,
        in_specs=[smem()] + vmem(4),
        out_specs=vmem(1)[0],
        out_shape=jax.ShapeDtypeStruct((136, 256), BF16),
        compiler_params=params(),
        cost_estimate=cost(1e7),
        name="share",
    )(scalars, *parts)


def final_kernel(s, count, tables, *refs):
    regions, (region_out, table_out, loss_out) = refs[:8], refs[8:]
    total = 0.0
    for d in range(8):
        source = (s[Z] + 8 - d) % 8
        for k in range(2):
            region_out[k, source] = regions[d][64 * k : 64 * k + 64, :]
        total += jnp.sum(regions[d][128:136, :].astype(F32))
    loss_out[0, 0] = total / count[0, 0] / CLASSES
    for y in range(4):
        at = pl.multiple_of(672 * (s[E] ^ y), 32)
        for x in range(2):
            table_out[pl.ds(at, 672), 128 * x : 128 * x + 128] = tables[2 * y + x]


def make_final(scalars, count, tables, regions):
    return pl.pallas_call(
        final_kernel,
        in_specs=[smem(), smem()] + vmem(9),
        out_specs=vmem(2) + [smem()],
        out_shape=[
            jax.ShapeDtypeStruct((2, 8, 64, 256), BF16),
            jax.ShapeDtypeStruct((2688, 256), BF16),
            jax.ShapeDtypeStruct((1, 1), F32),
        ],
        compiler_params=params(),
        cost_estimate=cost(1e7),
        name="final",
    )(scalars, count, tables, *regions)


def over_img(x, dy, dx):
    pairs = [
        (2 * y + xl, 2 * ((y + dy) % 4) + (xl ^ dx)) for y in range(4) for xl in range(2)
    ]
    return lax.ppermute(x, IMG, pairs)


def to_owner(x):
    axes = ("img_0",) + EMB
    return lax.ppermute(x, axes, [(4 * y + e, 4 * y + (e ^ y)) for y in range(4) for e in range(4)])


def along_cls(x, d):
    return lax.ppermute(x, CLS, [(i, (i + d) % 8) for i in range(8)])


def exchange(x, axes):
    return lax.all_to_all(x, axes, split_axis=0, concat_axis=0, tiled=True)


def shards(regions, table, shift, scale, labels, valid):
    rows = regions.shape[0]
    y = lax.axis_index("img_0")
    xl = lax.axis_index("img_1")
    xh = lax.axis_index("emb_0")
    k = lax.axis_index("emb_1")
    z = lax.axis_index(CLS)
    scalars = jnp.stack([k, z * 2688 + xh * 1344, 2 * xh + k, y, xl, z]).astype(jnp.int32)

    t_send = take_rows(pltpu.with_memory_space_constraint(table, pltpu.HBM), 4 * (1 - xh) + y, PART)
    t_send, regions_in = lax.optimization_barrier((t_send, regions))
    t_got = swap(t_send, "emb_0")
    r_far = swap(regions_in, "emb_0")
    r_near = swap(regions_in, "emb_1")
    local = jnp.broadcast_to(jnp.sum((labels >= 0).astype(F32)), (8, 128))
    local_other = swap(local, "img_1")
    t_far = exchange(make_message(t_got, local, local_other), "img_0")
    t_own = lax.dynamic_slice_in_dim(table, xh * 1344, 1344, 0)
    t_near = swap(t_own, "emb_1")
    r_both = swap(r_far, "emb_1")
    t_both = swap(t_far, "emb_1")
    blocks = (regions, r_near, r_far, r_both)
    tables = (t_own, t_near, t_far, t_both)
    unit, inv = make_unit(blocks)

    lane_f = jnp.concatenate([shift[None], scale[None], jnp.zeros((6, rows), F32)], axis=0)
    mask = lax.dynamic_slice(valid, (k, xh * 1344), (1, 1344)).astype(F32).T
    keep, send, loss, count = make_focal(scalars, tables, unit, lane_f, labels[None], mask)

    theirs = swap(send, "emb_1")
    terms = exchange(make_region(scalars, keep, send, tables, blocks, inv), CLS)
    chunks = list(make_table(scalars, keep, theirs, unit, loss))
    for o in (3, 6, 5, 2, 7, 4, 1):
        chunks[o] = over_img(chunks[o], o // 2, o % 2)
    table_part, loss_part = make_table_sum(chunks)
    table_part = to_owner(table_part)
    parts = list(make_merge(terms, loss_part))
    for q in range(1, 4):
        parts[q] = lax.ppermute(parts[q], EMB, [(i, i ^ q) for i in range(4)])
    message = make_gather(table_part)
    table_all = exchange(message, IMG)
    share = make_share(scalars, parts)
    shares = [share] + [along_cls(share, d) for d in range(1, 8)]
    region_grad, table_grad, total = make_final(scalars, count, table_all, shares)
    return (total[0, 0], region_grad.reshape(rows, 256), table_grad)


def solution(mesh):
    torus = Mesh(
        mesh.devices.reshape(4, 2, mesh.shape["cls"], 2, 2),
        ("img_0", "img_1", "cls", "emb_0", "emb_1"),
    )
    return jax.shard_map(
        shards,
        mesh=torus,
        in_specs=(P(IMG, EMB), P(CLS, EMB), P(IMG), P(IMG), P(IMG), P(IMG, CLS)),
        out_specs=(P(), P(IMG, EMB), P(CLS, EMB)),
        check_vma=False,
    )
```

```python
import jax
import jax.numpy as jnp
from jax import lax
from jax.experimental import pallas as pl
from jax.experimental.pallas import tpu as pltpu
from jax.sharding import Mesh
from jax.sharding import PartitionSpec as P

CLASSES = 21504
REGIONS = 8192
EMB = ("emb_0", "emb_1")
IMG = ("img_0", "img_1")
CLS = ("cls",)
F32 = jnp.float32
BF16 = jnp.bfloat16
NT = (((1,), (1,)), ((), ()))
TN = (((0,), (0,)), ((), ()))

K, BASE, E, Y, XL, Z = range(6)


PART = 336


def vmem(n):
    return [pl.BlockSpec(memory_space=pltpu.VMEM)] * n


def in_hbm(shape, dtype):
    return pltpu.HBM(shape, dtype)


def smem():
    return pl.BlockSpec(memory_space=pltpu.SMEM)


def params(mebibytes=16):
    return pltpu.CompilerParams(vmem_limit_bytes=mebibytes * 1024 * 1024)


def cost(flops):
    return pl.CostEstimate(flops=int(flops), bytes_accessed=1 << 20, transcendentals=0)


def swap(x, axis):
    return lax.ppermute(x, axis, [(0, 1), (1, 0)])


def split3(value, width):
    hi = value.astype(BF16).astype(F32)
    mid = (value - hi).astype(BF16).astype(F32)
    lo = value - hi - mid
    lane = lax.broadcasted_iota(jnp.int32, (8, width), 1)
    row = lax.broadcasted_iota(jnp.int32, (8, width), 0)
    packed = jnp.where(lane == 0, hi, jnp.where(lane == 1, mid, jnp.where(lane == 2, lo, 0.0)))
    return jnp.where(row == 0, packed, 0.0)


def unit_kernel(a, b, c, d, out, raw, scale):
    blocks = [r[...].astype(F32) for r in (a, b, c, d)]
    squares = sum(jnp.sum(v * v, axis=1, keepdims=True) for v in blocks)
    inv = lax.rsqrt(squares + 1e-06)
    scale[...] = jnp.broadcast_to(inv, scale.shape)
    for q, (v, r) in enumerate(zip(blocks, (a, b, c, d))):
        out[:, 256 * q : 256 * q + 256] = (v * inv).astype(BF16)
        raw[:, 256 * q : 256 * q + 256] = r[...]


def make_unit(blocks):
    rows = blocks[0].shape[0]
    tile = 256
    return pl.pallas_call(
        unit_kernel,
        grid=(rows // tile,),
        in_specs=[pl.BlockSpec((tile, 256), lambda i: (i, 0))] * 4,
        out_specs=[
            pl.BlockSpec((tile, 1024), lambda i: (i, 0)),
            pl.BlockSpec((tile, 1024), lambda i: (i, 0)),
            pl.BlockSpec((tile, 128), lambda i: (i, 0)),
        ],
        out_shape=[
            jax.ShapeDtypeStruct((rows, 1024), BF16),
            jax.ShapeDtypeStruct((rows, 1024), BF16),
            jax.ShapeDtypeStruct((rows, 128), F32),
        ],
        compiler_params=params(),
        cost_estimate=cost(2e7),
        name="unit",
    )(*blocks)


def rows_kernel(s, x, out):
    out[...] = x[...]


def take_rows(x, at, rows):
    return pl.pallas_call(
        rows_kernel,
        grid_spec=pltpu.PrefetchScalarGridSpec(
            num_scalar_prefetch=1,
            grid=(1,),
            in_specs=[pl.BlockSpec((rows, 256), lambda i, s: (s[0], 0))],
            out_specs=pl.BlockSpec((rows, 256), lambda i, s: (0, 0)),
        ),
        out_shape=jax.ShapeDtypeStruct((rows, 256), BF16),
        compiler_params=params(),
        name="rows",
    )(at.reshape(1), x)


def message_kernel(part, mine, theirs, out):
    count = mine[...] + theirs[...]
    high = jnp.floor(count / 32.0)
    lane = lax.broadcasted_iota(jnp.int32, (8, 128), 1)
    extra = jnp.where(lane == 0, high, jnp.where(lane == 1, count - 32.0 * high, 0.0))
    extra = jnp.concatenate([extra, jnp.zeros((8, 128), F32)], axis=1).astype(BF16)
    for y in range(4):
        out[y, 0:PART, :] = part[...]
        out[y, PART : PART + 8, :] = extra


def make_message(part, mine, theirs):
    return pl.pallas_call(
        message_kernel,
        in_specs=vmem(3),
        out_specs=vmem(1)[0],
        out_shape=in_hbm((4, PART + 8, 256), BF16),
        compiler_params=params(),
        name="message",
    )(part, mine, theirs)


def read_count(far):
    lane = lax.broadcasted_iota(jnp.int32, (1, 256), 1)
    row = sum(far[y, PART : PART + 8, :].astype(F32)[0:1, :] for y in range(4))
    return jnp.sum(jnp.where(lane == 0, 32.0 * row, jnp.where(lane == 1, row, 0.0)))


def focal_kernel(s, t0, t1, t2, t3, unit, lane_f, labels, mask, keep, send, loss, count_out, acc):
    rows = unit.shape[0]
    half = keep.shape[0]
    count = read_count(t2)
    count_out[0, 0] = count
    u = [unit[:, 256 * q : 256 * q + 256] for q in range(4)]

    def dot(t, q):
        return lax.dot_general(t, u[q], NT, preferred_element_type=F32)

    for c in range(4):
        at = slice(PART * c, PART * c + PART)
        acc[at, :] = (
            dot(t0[at, :], 0) + dot(t1[at, :], 1) + dot(t2[c, 0:PART, :], 2) + dot(t3[c, 0:PART, :], 3)
        )
    shift = lane_f[0:1, :]
    scale = lane_f[1:2, :]
    factor = scale * (REGIONS / count)
    step = 32

    def part(out, start, total):
        wanted = labels[...] - (s[BASE] + start)

        def body(g, total):
            to = pl.multiple_of(g * step, step)
            at = pl.multiple_of(start + to, step)
            logit = (acc[pl.ds(at, step), :] + shift) * scale
            ids = lax.broadcasted_iota(jnp.int32, (step, rows), 0)
            target = (wanted - to) == ids
            m = jnp.where(target, -logit, logit)
            e = jnp.exp(-jnp.abs(m))
            r = 1.0 / (1.0 + e)
            er = e * r
            positive = m >= 0.0
            prob = jnp.where(positive, r, er)
            rest = jnp.where(positive, er, r)
            series = e * (1.0 - e * (0.5 - e * (1.0 / 3.0 - e * 0.25)))
            soft = jnp.maximum(m, 0.0) + jnp.where(e < 2e-3, series, jnp.log(1.0 + e))
            weight = jnp.where(target, 0.25, 0.75) * mask[pl.ds(at, step), :] * (prob * prob)
            slope = weight * (2.0 * rest * soft + prob)
            slope = jnp.where(target, -slope, slope)
            out[pl.ds(to, step), :] = (slope * factor).astype(BF16)
            term = weight * soft
            return total + sum(term[8 * i : 8 * i + 8, :] for i in range(step // 8))

        return lax.fori_loop(0, half // step, body, total)

    total = part(send, (1 - s[K]) * half, jnp.zeros((8, rows), F32))
    total = part(keep, s[K] * half, total)
    loss[...] = sum(total[:, 128 * i : 128 * i + 128] for i in range(4))


def make_focal(scalars, tables, unit, lane_f, labels, mask):
    rows = unit.shape[0] // 2
    classes = mask.shape[0]
    whole = lambda i, s: (0, 0)
    cube = lambda i, s: (0, 0, 0)
    return pl.pallas_call(
        focal_kernel,
        grid_spec=pltpu.PrefetchScalarGridSpec(
            num_scalar_prefetch=1,
            grid=(1,),
            in_specs=[pl.BlockSpec((classes, 256), whole)] * 2
            + [pl.BlockSpec((4, PART + 8, 256), cube)] * 2
            + [
                pl.BlockSpec((rows, 1024), lambda i, s: (s[K], 0)),
                pl.BlockSpec((8, rows), lambda i, s: (0, s[K])),
                pl.BlockSpec((1, rows), lambda i, s: (0, s[K])),
                pl.BlockSpec((classes, 1), whole),
            ],
            out_specs=[
                pl.BlockSpec((classes // 2, rows), whole),
                pl.BlockSpec((classes // 2, rows), whole),
                pl.BlockSpec((8, 128), whole),
                smem(),
            ],
            scratch_shapes=[pltpu.VMEM((classes, rows), F32)],
        ),
        out_shape=[
            jax.ShapeDtypeStruct((classes // 2, rows), BF16),
            jax.ShapeDtypeStruct((classes // 2, rows), BF16),
            jax.ShapeDtypeStruct((8, 128), F32),
            jax.ShapeDtypeStruct((1, 1), F32),
        ],
        compiler_params=params(24),
        cost_estimate=cost(1.4e9),
        name="focal",
    )(scalars, *tables, unit, lane_f, labels, mask)


def region_kernel(s, keep, send, t0, t1, t2, t3, raw, inv_ref, out, acc):
    half = keep.shape[0]
    k = s[K]
    tile = acc.shape[0]
    mine_at = pl.multiple_of(k * half, 32)
    theirs_at = pl.multiple_of((1 - k) * half, 32)

    def dot(g, t):
        return lax.dot_general(g, t, TN, preferred_element_type=F32)

    for i in range(keep.shape[1] // tile):
        rows = slice(tile * i, tile * i + tile)
        mine = keep[:, rows]
        theirs = send[:, rows]
        here = pl.ds(pl.multiple_of(keep.shape[1] * k + tile * i, tile), tile)
        inv = inv_ref[here, 0:1]
        along = 0.0
        for q, t in enumerate((t0, t1, t2, t3)):
            if q < 2:
                part = dot(mine, t[pl.ds(mine_at, half), :]) + dot(theirs, t[pl.ds(theirs_at, half), :])
            else:
                part = sum(
                    dot(g[PART * p : PART * p + PART, :], t[2 * at + p, 0:PART, :])
                    for g, at in ((mine, k), (theirs, 1 - k))
                    for p in range(2)
                )
            acc[:, 256 * q : 256 * q + 256] = part
            value = raw[here, 256 * q : 256 * q + 256].astype(F32)
            along += jnp.sum(part * value, axis=1, keepdims=True)
        back = inv * inv * along
        for q in range(4):
            cols = slice(256 * q, 256 * q + 256)
            grad = inv * (acc[:, cols] - raw[here, cols].astype(F32) * back)
            for p in range(tile // 64):
                z = tile // 64 * i + p
                out[z, :, cols] = grad[64 * p : 64 * p + 64, :].astype(BF16)


def make_region(scalars, keep, send, tables, raw, inv):
    return pl.pallas_call(
        region_kernel,
        in_specs=[smem()] + vmem(8),
        out_specs=vmem(1)[0],
        out_shape=in_hbm((8, 64, 1024), BF16),
        scratch_shapes=[pltpu.VMEM((256, 1024), F32)],
        compiler_params=params(24),
        cost_estimate=cost(1.4e9),
        name="region",
    )(scalars, keep, send, *tables, raw, inv)


def table_kernel(s, keep, other, unit, loss, *refs):
    outs, acc = refs[:8], refs[8]
    half, rows = other.shape
    mine = keep[...]
    theirs = other[...]
    mine_at = pl.multiple_of(s[K] * rows, rows)
    theirs_at = pl.multiple_of((1 - s[K]) * rows, rows)
    extra = split3(jnp.sum(loss[...]), 128).astype(BF16)
    for dy in range(4):
        cols = pl.ds(pl.multiple_of(256 * ((s[Y] + dy) % 4), 256), 256)
        acc[...] = jnp.dot(
            mine, unit[pl.ds(mine_at, rows), cols], preferred_element_type=F32
        ) + jnp.dot(theirs, unit[pl.ds(theirs_at, rows), cols], preferred_element_type=F32)
        for dx in range(2):
            at = pl.multiple_of(128 * (s[XL] ^ dx), 128)
            out = outs[2 * dy + dx]
            out[0:half, :] = acc[:, pl.ds(at, 128)].astype(BF16)
            out[half : half + 8, :] = extra


def make_table(scalars, keep, other, unit, loss):
    half = other.shape[0]
    return pl.pallas_call(
        table_kernel,
        in_specs=[smem()] + vmem(4),
        out_specs=vmem(8),
        out_shape=[jax.ShapeDtypeStruct((half + 8, 128), BF16)] * 8,
        scratch_shapes=[pltpu.VMEM((half, 256), F32)],
        compiler_params=params(),
        cost_estimate=cost(1.4e9),
        name="table",
    )(scalars, keep, other, unit, loss)


def table_sum_kernel(*refs):
    terms, (out, loss) = refs[:8], refs[8:]
    half = out.shape[0]
    out[...] = sum(t[0:half, :].astype(F32) for t in terms).astype(BF16)
    loss[...] = sum(t[half : half + 8, :].astype(F32) for t in terms)


def make_table_sum(terms):
    return pl.pallas_call(
        table_sum_kernel,
        in_specs=vmem(8),
        out_specs=vmem(2),
        out_shape=[
            jax.ShapeDtypeStruct((terms[0].shape[0] - 8, 128), BF16),
            jax.ShapeDtypeStruct((8, 128), F32),
        ],
        compiler_params=params(),
        cost_estimate=cost(1e7),
        name="table_sum",
    )(*terms)


def merge_kernel(terms, loss, *outs):
    total = sum(terms[z].astype(F32) for z in range(8)).astype(BF16)
    extra = split3(jnp.sum(loss[...]), 256).astype(BF16)
    for q, out in enumerate(outs):
        out[0:64, :] = total[:, 256 * q : 256 * q + 256]
        out[64:72, :] = extra


def make_merge(terms, loss):
    return pl.pallas_call(
        merge_kernel,
        in_specs=vmem(2),
        out_specs=vmem(4),
        out_shape=[jax.ShapeDtypeStruct((72, 256), BF16)] * 4,
        compiler_params=params(),
        cost_estimate=cost(1e7),
        name="merge",
    )(terms, loss)


def gather_kernel(chunk, out):
    rows = chunk[...]
    for j in range(8):
        out[j] = rows


def make_gather(chunk):
    return pl.pallas_call(
        gather_kernel,
        in_specs=vmem(1),
        out_specs=vmem(1)[0],
        out_shape=in_hbm((8,) + chunk.shape, BF16),
        compiler_params=params(),
        cost_estimate=cost(1e7),
        name="gather",
    )(chunk)


def share_kernel(s, own, near, far, both, out):
    k = s[K]
    for at, a, b in ((k, own, far), (1 - k, near, both)):
        total = a[0:64, :].astype(F32) + b[0:64, :].astype(F32)
        out[pl.ds(pl.multiple_of(64 * at, 64), 64), :] = total.astype(BF16)
    loss = sum(jnp.sum(r[64:72, :].astype(F32)) for r in (own, near, far, both))
    out[128:136, :] = split3(loss, 256).astype(BF16)


def make_share(scalars, parts):
    return pl.pallas_call(
        share_kernel,
        in_specs=[smem()] + vmem(4),
        out_specs=vmem(1)[0],
        out_shape=jax.ShapeDtypeStruct((136, 256), BF16),
        compiler_params=params(),
        cost_estimate=cost(1e7),
        name="share",
    )(scalars, *parts)


def final_kernel(s, count, tables, *refs):
    regions, (region_out, table_out, loss_out, sems) = refs[:8], refs[8:]
    copies = []
    for y in range(4):
        at = pl.multiple_of(672 * (s[E] ^ y), 32)
        for x in range(2):
            to = table_out.at[pl.ds(at, 672), pl.ds(128 * x, 128)]
            copies.append(pltpu.make_async_copy(tables.at[2 * y + x], to, sems.at[2 * y + x]))
            copies[-1].start()
    total = 0.0
    for d in range(8):
        source = (s[Z] + 8 - d) % 8
        for k in range(2):
            region_out[k, source] = regions[d][64 * k : 64 * k + 64, :]
        total += jnp.sum(regions[d][128:136, :].astype(F32))
    loss_out[0, 0] = total / count[0, 0] / CLASSES
    for copy in copies:
        copy.wait()


def make_final(scalars, count, tables, regions):
    return pl.pallas_call(
        final_kernel,
        in_specs=[smem(), smem()] + vmem(9),
        out_specs=vmem(1) + [pl.BlockSpec(memory_space=pltpu.HBM), smem()],
        scratch_shapes=[pltpu.SemaphoreType.DMA((8,))],
        out_shape=[
            jax.ShapeDtypeStruct((2, 8, 64, 256), BF16),
            jax.ShapeDtypeStruct((2688, 256), BF16),
            jax.ShapeDtypeStruct((1, 1), F32),
        ],
        compiler_params=params(),
        cost_estimate=cost(1e7),
        name="final",
    )(scalars, count, tables, *regions)


def over_img(x, dy, dx):
    pairs = [
        (2 * y + xl, 2 * ((y + dy) % 4) + (xl ^ dx)) for y in range(4) for xl in range(2)
    ]
    return lax.ppermute(x, IMG, pairs)


def to_owner(x):
    axes = ("img_0",) + EMB
    return lax.ppermute(x, axes, [(4 * y + e, 4 * y + (e ^ y)) for y in range(4) for e in range(4)])


def along_cls(x, d):
    return lax.ppermute(x, CLS, [(i, (i + d) % 8) for i in range(8)])


def exchange(x, axes):
    return lax.all_to_all(x, axes, split_axis=0, concat_axis=0, tiled=True)


def shards(regions, table, shift, scale, labels, valid):
    rows = regions.shape[0]
    y = lax.axis_index("img_0")
    xl = lax.axis_index("img_1")
    xh = lax.axis_index("emb_0")
    k = lax.axis_index("emb_1")
    z = lax.axis_index(CLS)
    scalars = jnp.stack([k, z * 2688 + xh * 1344, 2 * xh + k, y, xl, z]).astype(jnp.int32)

    t_send = take_rows(pltpu.with_memory_space_constraint(table, pltpu.HBM), 4 * (1 - xh) + y, PART)
    t_send, regions_in = lax.optimization_barrier((t_send, regions))
    t_got = swap(t_send, "emb_0")
    r_far = swap(regions_in, "emb_0")
    r_near = swap(regions_in, "emb_1")
    local = jnp.broadcast_to(jnp.sum((labels >= 0).astype(F32)), (8, 128))
    local_other = swap(local, "img_1")
    t_far = exchange(make_message(t_got, local, local_other), "img_0")
    t_own = lax.dynamic_slice_in_dim(table, xh * 1344, 1344, 0)
    t_near = swap(t_own, "emb_1")
    r_both = swap(r_far, "emb_1")
    t_both = swap(t_far, "emb_1")
    blocks = (regions, r_near, r_far, r_both)
    tables = (t_own, t_near, t_far, t_both)
    unit, raw, inv = make_unit(blocks)

    lane_f = jnp.concatenate([shift[None], scale[None], jnp.zeros((6, rows), F32)], axis=0)
    mask = lax.dynamic_slice(valid, (k, xh * 1344), (1, 1344)).astype(F32).T
    keep, send, loss, count = make_focal(scalars, tables, unit, lane_f, labels[None], mask)

    theirs = swap(send, "emb_1")
    terms = exchange(make_region(scalars, keep, send, tables, raw, inv), CLS)
    chunks = list(make_table(scalars, keep, theirs, unit, loss))
    for o in OVER_IMG:
        chunks[o] = over_img(chunks[o], o // 2, o % 2)
    table_part, loss_part = make_table_sum(chunks)
    table_part = to_owner(table_part)
    parts = list(make_merge(terms, loss_part))
    for q in range(1, 4):
        parts[q] = lax.ppermute(parts[q], EMB, [(i, i ^ q) for i in range(4)])
    message = make_gather(table_part)
    table_all = exchange(message, IMG)
    share = make_share(scalars, parts)
    shares = [share] * 8
    for d in ALONG_CLS:
        shares[d] = along_cls(share, d)
    region_grad, table_grad, total = make_final(scalars, count, table_all, shares)
    return (total[0, 0], region_grad.reshape(rows, 256), table_grad)


OVER_IMG = (3, 6, 5, 2, 7, 4, 1)
ALONG_CLS = (4, 3, 5, 2, 6, 1, 7)


def solution(mesh):
    torus = Mesh(
        mesh.devices.reshape(4, 2, mesh.shape["cls"], 2, 2),
        ("img_0", "img_1", "cls", "emb_0", "emb_1"),
    )
    return jax.shard_map(
        shards,
        mesh=torus,
        in_specs=(P(IMG, EMB), P(CLS, EMB), P(IMG), P(IMG), P(IMG), P(IMG, CLS)),
        out_specs=(P(), P(IMG, EMB), P(CLS, EMB)),
        check_vma=False,
    )
```

```python
import jax
import jax.numpy as jnp
from jax import lax
from jax.experimental import pallas as pl
from jax.experimental.pallas import tpu as pltpu
from jax.sharding import Mesh
from jax.sharding import PartitionSpec as P

CLASSES = 21504
REGIONS = 8192
EMB = ("emb_0", "emb_1")
IMG = ("img_0", "img_1")
CLS = ("cls",)
F32 = jnp.float32
BF16 = jnp.bfloat16
NT = (((1,), (1,)), ((), ()))
TN = (((0,), (0,)), ((), ()))

K, BASE, E, Y, XL, Z = range(6)


PART = 336


def vmem(n):
    return [pl.BlockSpec(memory_space=pltpu.VMEM)] * n


def in_hbm(shape, dtype):
    return pltpu.HBM(shape, dtype)


def smem():
    return pl.BlockSpec(memory_space=pltpu.SMEM)


def params(mebibytes=16):
    return pltpu.CompilerParams(vmem_limit_bytes=mebibytes * 1024 * 1024)


def cost(flops):
    return pl.CostEstimate(flops=int(flops), bytes_accessed=1 << 20, transcendentals=0)


def swap(x, axis):
    return lax.ppermute(x, axis, [(0, 1), (1, 0)])


def split3(value, width):
    hi = value.astype(BF16).astype(F32)
    mid = (value - hi).astype(BF16).astype(F32)
    lo = value - hi - mid
    lane = lax.broadcasted_iota(jnp.int32, (8, width), 1)
    row = lax.broadcasted_iota(jnp.int32, (8, width), 0)
    packed = jnp.where(lane == 0, hi, jnp.where(lane == 1, mid, jnp.where(lane == 2, lo, 0.0)))
    return jnp.where(row == 0, packed, 0.0)


def unit_kernel(a, b, c, d, out, raw, scale):
    blocks = [r[...].astype(F32) for r in (a, b, c, d)]
    squares = sum(jnp.sum(v * v, axis=1, keepdims=True) for v in blocks)
    inv = lax.rsqrt(squares + 1e-06)
    scale[...] = jnp.broadcast_to(inv, scale.shape)
    for q, (v, r) in enumerate(zip(blocks, (a, b, c, d))):
        out[:, 256 * q : 256 * q + 256] = (v * inv).astype(BF16)
        raw[:, 256 * q : 256 * q + 256] = r[...]


def make_unit(blocks):
    rows = blocks[0].shape[0]
    tile = 128
    return pl.pallas_call(
        unit_kernel,
        grid=(rows // tile,),
        in_specs=[pl.BlockSpec((tile, 256), lambda i: (i, 0))] * 4,
        out_specs=[
            pl.BlockSpec((tile, 1024), lambda i: (i, 0)),
            pl.BlockSpec((tile, 1024), lambda i: (i, 0)),
            pl.BlockSpec((tile, 128), lambda i: (i, 0)),
        ],
        out_shape=[
            jax.ShapeDtypeStruct((rows, 1024), BF16),
            jax.ShapeDtypeStruct((rows, 1024), BF16),
            jax.ShapeDtypeStruct((rows, 128), F32),
        ],
        compiler_params=params(),
        cost_estimate=cost(2e7),
        name="unit",
    )(*blocks)


def rows_kernel(s, x, out):
    out[...] = x[...]


def take_rows(x, at, rows):
    return pl.pallas_call(
        rows_kernel,
        grid_spec=pltpu.PrefetchScalarGridSpec(
            num_scalar_prefetch=1,
            grid=(1,),
            in_specs=[pl.BlockSpec((rows, 256), lambda i, s: (s[0], 0))],
            out_specs=pl.BlockSpec((rows, 256), lambda i, s: (0, 0)),
        ),
        out_shape=jax.ShapeDtypeStruct((rows, 256), BF16),
        compiler_params=params(),
        name="rows",
    )(at.reshape(1), x)


def message_kernel(part, mine, theirs, out):
    count = mine[...] + theirs[...]
    high = jnp.floor(count / 32.0)
    lane = lax.broadcasted_iota(jnp.int32, (8, 128), 1)
    extra = jnp.where(lane == 0, high, jnp.where(lane == 1, count - 32.0 * high, 0.0))
    extra = jnp.concatenate([extra, jnp.zeros((8, 128), F32)], axis=1).astype(BF16)
    for y in range(4):
        out[y, 0:PART, :] = part[...]
        out[y, PART : PART + 8, :] = extra


def make_message(part, mine, theirs):
    return pl.pallas_call(
        message_kernel,
        in_specs=vmem(3),
        out_specs=vmem(1)[0],
        out_shape=in_hbm((4, PART + 8, 256), BF16),
        compiler_params=params(),
        name="message",
    )(part, mine, theirs)


def read_count(far):
    lane = lax.broadcasted_iota(jnp.int32, (1, 256), 1)
    row = sum(far[y, PART : PART + 8, :].astype(F32)[0:1, :] for y in range(4))
    return jnp.sum(jnp.where(lane == 0, 32.0 * row, jnp.where(lane == 1, row, 0.0)))


def focal_kernel(s, t0, t1, t2, t3, unit, lane_f, labels, mask, keep, send, loss, count_out, acc):
    rows = unit.shape[0]
    half = keep.shape[0]
    count = read_count(t2)
    count_out[0, 0] = count
    u = [unit[:, 256 * q : 256 * q + 256] for q in range(4)]

    def dot(t, q):
        return lax.dot_general(t, u[q], NT, preferred_element_type=F32)

    for c in range(4):
        at = slice(PART * c, PART * c + PART)
        acc[at, :] = (
            dot(t0[at, :], 0) + dot(t1[at, :], 1) + dot(t2[c, 0:PART, :], 2) + dot(t3[c, 0:PART, :], 3)
        )
    shift = lane_f[0:1, :]
    scale = lane_f[1:2, :]
    factor = scale * (REGIONS / count)
    step = 32

    def part(out, start, total):
        wanted = labels[...] - (s[BASE] + start)

        def body(g, total):
            to = pl.multiple_of(g * step, step)
            at = pl.multiple_of(start + to, step)
            logit = (acc[pl.ds(at, step), :] + shift) * scale
            ids = lax.broadcasted_iota(jnp.int32, (step, rows), 0)
            target = (wanted - to) == ids
            m = jnp.where(target, -logit, logit)
            e = jnp.exp(-jnp.abs(m))
            r = 1.0 / (1.0 + e)
            er = e * r
            positive = m >= 0.0
            prob = jnp.where(positive, r, er)
            rest = jnp.where(positive, er, r)
            series = e * (1.0 - e * (0.5 - e * (1.0 / 3.0 - e * 0.25)))
            soft = jnp.maximum(m, 0.0) + jnp.where(e < 2e-3, series, jnp.log(1.0 + e))
            weight = jnp.where(target, 0.25, 0.75) * mask[pl.ds(at, step), :] * (prob * prob)
            slope = weight * (2.0 * rest * soft + prob)
            slope = jnp.where(target, -slope, slope)
            out[pl.ds(to, step), :] = (slope * factor).astype(BF16)
            term = weight * soft
            return total + sum(term[8 * i : 8 * i + 8, :] for i in range(step // 8))

        return lax.fori_loop(0, half // step, body, total)

    total = part(send, (1 - s[K]) * half, jnp.zeros((8, rows), F32))
    total = part(keep, s[K] * half, total)
    loss[...] = sum(total[:, 128 * i : 128 * i + 128] for i in range(4))


def make_focal(scalars, tables, unit, lane_f, labels, mask):
    rows = unit.shape[0] // 2
    classes = mask.shape[0]
    whole = lambda i, s: (0, 0)
    cube = lambda i, s: (0, 0, 0)
    return pl.pallas_call(
        focal_kernel,
        grid_spec=pltpu.PrefetchScalarGridSpec(
            num_scalar_prefetch=1,
            grid=(1,),
            in_specs=[pl.BlockSpec((classes, 256), whole)] * 2
            + [pl.BlockSpec((4, PART + 8, 256), cube)] * 2
            + [
                pl.BlockSpec((rows, 1024), lambda i, s: (s[K], 0)),
                pl.BlockSpec((8, rows), lambda i, s: (0, s[K])),
                pl.BlockSpec((1, rows), lambda i, s: (0, s[K])),
                pl.BlockSpec((classes, 1), whole),
            ],
            out_specs=[
                pl.BlockSpec((classes // 2, rows), whole),
                pl.BlockSpec((classes // 2, rows), whole),
                pl.BlockSpec((8, 128), whole),
                smem(),
            ],
            scratch_shapes=[pltpu.VMEM((classes, rows), F32)],
        ),
        out_shape=[
            jax.ShapeDtypeStruct((classes // 2, rows), BF16),
            jax.ShapeDtypeStruct((classes // 2, rows), BF16),
            jax.ShapeDtypeStruct((8, 128), F32),
            jax.ShapeDtypeStruct((1, 1), F32),
        ],
        compiler_params=params(24),
        cost_estimate=cost(1.4e9),
        name="focal",
    )(scalars, *tables, unit, lane_f, labels, mask)


def region_kernel(s, keep, send, t0, t1, t2, t3, raw, inv_ref, out, acc):
    half = keep.shape[0]
    k = s[K]
    tile = acc.shape[0]
    mine_at = pl.multiple_of(k * half, 32)
    theirs_at = pl.multiple_of((1 - k) * half, 32)

    def dot(g, t):
        return lax.dot_general(g, t, TN, preferred_element_type=F32)

    for i in range(keep.shape[1] // tile):
        rows = slice(tile * i, tile * i + tile)
        mine = keep[:, rows]
        theirs = send[:, rows]
        here = pl.ds(pl.multiple_of(keep.shape[1] * k + tile * i, tile), tile)
        inv = inv_ref[here, 0:1]
        along = 0.0
        for q, t in enumerate((t0, t1, t2, t3)):
            if q < 2:
                part = dot(mine, t[pl.ds(mine_at, half), :]) + dot(theirs, t[pl.ds(theirs_at, half), :])
            else:
                part = sum(
                    dot(g[PART * p : PART * p + PART, :], t[2 * at + p, 0:PART, :])
                    for g, at in ((mine, k), (theirs, 1 - k))
                    for p in range(2)
                )
            acc[:, 256 * q : 256 * q + 256] = part
            value = raw[here, 256 * q : 256 * q + 256].astype(F32)
            along += jnp.sum(part * value, axis=1, keepdims=True)
        back = inv * inv * along
        for q in range(4):
            cols = slice(256 * q, 256 * q + 256)
            grad = inv * (acc[:, cols] - raw[here, cols].astype(F32) * back)
            for p in range(tile // 64):
                z = tile // 64 * i + p
                out[z, :, cols] = grad[64 * p : 64 * p + 64, :].astype(BF16)


def make_region(scalars, keep, send, tables, raw, inv):
    return pl.pallas_call(
        region_kernel,
        in_specs=[smem()] + vmem(8),
        out_specs=vmem(1)[0],
        out_shape=in_hbm((8, 64, 1024), BF16),
        scratch_shapes=[pltpu.VMEM((256, 1024), F32)],
        compiler_params=params(24),
        cost_estimate=cost(1.4e9),
        name="region",
    )(scalars, keep, send, *tables, raw, inv)


def table_kernel(s, keep, other, unit, loss, *refs):
    outs, acc = refs[:8], refs[8]
    half, rows = other.shape
    mine = keep[...]
    theirs = other[...]
    mine_at = pl.multiple_of(s[K] * rows, rows)
    theirs_at = pl.multiple_of((1 - s[K]) * rows, rows)
    extra = split3(jnp.sum(loss[...]), 128).astype(BF16)
    for dy in range(4):
        cols = pl.ds(pl.multiple_of(256 * ((s[Y] + dy) % 4), 256), 256)
        acc[...] = jnp.dot(
            mine, unit[pl.ds(mine_at, rows), cols], preferred_element_type=F32
        ) + jnp.dot(theirs, unit[pl.ds(theirs_at, rows), cols], preferred_element_type=F32)
        for dx in range(2):
            at = pl.multiple_of(128 * (s[XL] ^ dx), 128)
            out = outs[2 * dy + dx]
            out[0:half, :] = acc[:, pl.ds(at, 128)].astype(BF16)
            out[half : half + 8, :] = extra


def make_table(scalars, keep, other, unit, loss):
    half = other.shape[0]
    return pl.pallas_call(
        table_kernel,
        in_specs=[smem()] + vmem(4),
        out_specs=vmem(8),
        out_shape=[jax.ShapeDtypeStruct((half + 8, 128), BF16)] * 8,
        scratch_shapes=[pltpu.VMEM((half, 256), F32)],
        compiler_params=params(),
        cost_estimate=cost(1.4e9),
        name="table",
    )(scalars, keep, other, unit, loss)


def table_sum_kernel(*refs):
    terms, (out, loss) = refs[:8], refs[8:]
    half = out.shape[0]
    out[...] = sum(t[0:half, :].astype(F32) for t in terms).astype(BF16)
    loss[...] = sum(t[half : half + 8, :].astype(F32) for t in terms)


def make_table_sum(terms):
    return pl.pallas_call(
        table_sum_kernel,
        in_specs=vmem(8),
        out_specs=vmem(2),
        out_shape=[
            jax.ShapeDtypeStruct((terms[0].shape[0] - 8, 128), BF16),
            jax.ShapeDtypeStruct((8, 128), F32),
        ],
        compiler_params=params(),
        cost_estimate=cost(1e7),
        name="table_sum",
    )(*terms)


def merge_kernel(terms, loss, *outs):
    total = sum(terms[z].astype(F32) for z in range(8)).astype(BF16)
    extra = split3(jnp.sum(loss[...]), 256).astype(BF16)
    for q, out in enumerate(outs):
        out[0:64, :] = total[:, 256 * q : 256 * q + 256]
        out[64:72, :] = extra


def make_merge(terms, loss):
    return pl.pallas_call(
        merge_kernel,
        in_specs=vmem(2),
        out_specs=vmem(4),
        out_shape=[jax.ShapeDtypeStruct((72, 256), BF16)] * 4,
        compiler_params=params(),
        cost_estimate=cost(1e7),
        name="merge",
    )(terms, loss)


def gather_kernel(chunk, out):
    rows = chunk[...]
    for j in range(8):
        out[j] = rows


def make_gather(chunk):
    return pl.pallas_call(
        gather_kernel,
        in_specs=vmem(1),
        out_specs=vmem(1)[0],
        out_shape=in_hbm((8,) + chunk.shape, BF16),
        compiler_params=params(),
        cost_estimate=cost(1e7),
        name="gather",
    )(chunk)


def share_kernel(s, own, near, far, both, out):
    k = s[K]
    for at, a, b in ((k, own, far), (1 - k, near, both)):
        total = a[0:64, :].astype(F32) + b[0:64, :].astype(F32)
        out[pl.ds(pl.multiple_of(64 * at, 64), 64), :] = total.astype(BF16)
    loss = sum(jnp.sum(r[64:72, :].astype(F32)) for r in (own, near, far, both))
    out[128:136, :] = split3(loss, 256).astype(BF16)


def make_share(scalars, parts):
    return pl.pallas_call(
        share_kernel,
        in_specs=[smem()] + vmem(4),
        out_specs=vmem(1)[0],
        out_shape=jax.ShapeDtypeStruct((136, 256), BF16),
        compiler_params=params(),
        cost_estimate=cost(1e7),
        name="share",
    )(scalars, *parts)


def table_final_kernel(s, tables, out, token):
    for y in range(4):
        at = pl.multiple_of(672 * (s[E] ^ y), 32)
        for x in range(2):
            out[pl.ds(at, 672), 128 * x : 128 * x + 128] = tables[2 * y + x]
    token[0, 0] = s[E]


def make_table_final(scalars, tables):
    return pl.pallas_call(
        table_final_kernel,
        in_specs=[smem()] + vmem(1),
        out_specs=vmem(1) + [smem()],
        out_shape=[
            jax.ShapeDtypeStruct((2688, 256), BF16),
            jax.ShapeDtypeStruct((1, 1), jnp.int32),
        ],
        compiler_params=params(),
        cost_estimate=cost(1e7),
        name="table_final",
    )(scalars, tables)


def region_final_kernel(s, token, count, *refs):
    regions, (out, loss_out) = refs[:8], refs[8:]
    total = 0.0
    for d in range(8):
        source = (s[Z] + 8 - d) % 8
        for k in range(2):
            out[k, source] = regions[d][64 * k : 64 * k + 64, :]
        total += jnp.sum(regions[d][128:136, :].astype(F32))
    loss_out[0, 0] = total / count[0, 0] / CLASSES


def make_region_final(scalars, token, count, regions):
    return pl.pallas_call(
        region_final_kernel,
        in_specs=[smem()] * 3 + vmem(8),
        out_specs=vmem(1) + [smem()],
        out_shape=[
            jax.ShapeDtypeStruct((2, 8, 64, 256), BF16),
            jax.ShapeDtypeStruct((1, 1), F32),
        ],
        compiler_params=params(),
        cost_estimate=cost(1e7),
        name="region_final",
    )(scalars, token, count, *regions)


def over_img(x, dy, dx):
    pairs = [
        (2 * y + xl, 2 * ((y + dy) % 4) + (xl ^ dx)) for y in range(4) for xl in range(2)
    ]
    return lax.ppermute(x, IMG, pairs)


def to_owner(x):
    axes = ("img_0",) + EMB
    return lax.ppermute(x, axes, [(4 * y + e, 4 * y + (e ^ y)) for y in range(4) for e in range(4)])


def along_cls(x, d):
    return lax.ppermute(x, CLS, [(i, (i + d) % 8) for i in range(8)])


def exchange(x, axes):
    return lax.all_to_all(x, axes, split_axis=0, concat_axis=0, tiled=True)


def shards(regions, table, shift, scale, labels, valid):
    rows = regions.shape[0]
    y = lax.axis_index("img_0")
    xl = lax.axis_index("img_1")
    xh = lax.axis_index("emb_0")
    k = lax.axis_index("emb_1")
    z = lax.axis_index(CLS)
    scalars = jnp.stack([k, z * 2688 + xh * 1344, 2 * xh + k, y, xl, z]).astype(jnp.int32)

    t_send = take_rows(pltpu.with_memory_space_constraint(table, pltpu.HBM), 4 * (1 - xh) + y, PART)
    t_send, regions_in = lax.optimization_barrier((t_send, regions))
    t_got = swap(t_send, "emb_0")
    r_far = swap(regions_in, "emb_0")
    r_near = swap(regions_in, "emb_1")
    local = jnp.broadcast_to(jnp.sum((labels >= 0).astype(F32)), (8, 128))
    local_other = swap(local, "img_1")
    t_far = exchange(make_message(t_got, local, local_other), "img_0")
    t_own = lax.dynamic_slice_in_dim(table, xh * 1344, 1344, 0)
    t_near = swap(t_own, "emb_1")
    r_both = swap(r_far, "emb_1")
    t_both = swap(t_far, "emb_1")
    blocks = (regions, r_near, r_far, r_both)
    tables = (t_own, t_near, t_far, t_both)
    unit, raw, inv = make_unit(blocks)

    lane_f = jnp.concatenate([shift[None], scale[None], jnp.zeros((6, rows), F32)], axis=0)
    mask = lax.dynamic_slice(valid, (k, xh * 1344), (1, 1344)).astype(F32).T
    keep, send, loss, count = make_focal(scalars, tables, unit, lane_f, labels[None], mask)

    theirs = swap(send, "emb_1")
    terms = exchange(make_region(scalars, keep, send, tables, raw, inv), CLS)
    chunks = list(make_table(scalars, keep, theirs, unit, loss))
    for o in OVER_IMG:
        chunks[o] = over_img(chunks[o], o // 2, o % 2)
    table_part, loss_part = make_table_sum(chunks)
    table_part = to_owner(table_part)
    parts = list(make_merge(terms, loss_part))
    for q in range(1, 4):
        parts[q] = lax.ppermute(parts[q], EMB, [(i, i ^ q) for i in range(4)])
    message = make_gather(table_part)
    table_all = exchange(message, IMG)
    share = make_share(scalars, parts)
    shares = [share] * 8
    for d in ALONG_CLS:
        shares[d] = along_cls(share, d)
    table_grad, token = make_table_final(scalars, table_all)
    region_grad, total = make_region_final(scalars, token, count, shares)
    return (total[0, 0], region_grad.reshape(rows, 256), table_grad)


OVER_IMG = (3, 6, 5, 2, 7, 4, 1)
ALONG_CLS = (4, 3, 5, 2, 6, 1, 7)


def solution(mesh):
    torus = Mesh(
        mesh.devices.reshape(4, 2, mesh.shape["cls"], 2, 2),
        ("img_0", "img_1", "cls", "emb_0", "emb_1"),
    )
    return jax.shard_map(
        shards,
        mesh=torus,
        in_specs=(P(IMG, EMB), P(CLS, EMB), P(IMG), P(IMG), P(IMG), P(IMG, CLS)),
        out_specs=(P(), P(IMG, EMB), P(CLS, EMB)),
        check_vma=False,
    )
```

```python
import jax
import jax.numpy as jnp
from jax import lax
from jax.experimental import pallas as pl
from jax.experimental.pallas import tpu as pltpu
from jax.sharding import Mesh
from jax.sharding import PartitionSpec as P

CLASSES = 21504
REGIONS = 8192
EMB = ("emb_0", "emb_1")
IMG = ("img_0", "img_1")
CLS = ("cls",)
F32 = jnp.float32
BF16 = jnp.bfloat16
NT = (((1,), (1,)), ((), ()))
TN = (((0,), (0,)), ((), ()))

K, BASE, E, Y, XL, Z = range(6)


PART = 336


def vmem(n):
    return [pl.BlockSpec(memory_space=pltpu.VMEM)] * n


def in_hbm(shape, dtype):
    return pltpu.HBM(shape, dtype)


def smem():
    return pl.BlockSpec(memory_space=pltpu.SMEM)


def params(mebibytes=16):
    return pltpu.CompilerParams(vmem_limit_bytes=mebibytes * 1024 * 1024)


def cost(flops):
    return pl.CostEstimate(flops=int(flops), bytes_accessed=1 << 20, transcendentals=0)


def swap(x, axis):
    return lax.ppermute(x, axis, [(0, 1), (1, 0)])


def split3(value, width):
    hi = value.astype(BF16).astype(F32)
    mid = (value - hi).astype(BF16).astype(F32)
    lo = value - hi - mid
    lane = lax.broadcasted_iota(jnp.int32, (8, width), 1)
    row = lax.broadcasted_iota(jnp.int32, (8, width), 0)
    packed = jnp.where(lane == 0, hi, jnp.where(lane == 1, mid, jnp.where(lane == 2, lo, 0.0)))
    return jnp.where(row == 0, packed, 0.0)


def unit_kernel(a, b, c, d, out, raw, scale):
    blocks = [r[...].astype(F32) for r in (a, b, c, d)]
    squares = sum(jnp.sum(v * v, axis=1, keepdims=True) for v in blocks)
    inv = lax.rsqrt(squares + 1e-06)
    scale[...] = jnp.broadcast_to(inv, scale.shape)
    for q, (v, r) in enumerate(zip(blocks, (a, b, c, d))):
        out[:, 256 * q : 256 * q + 256] = (v * inv).astype(BF16)
        raw[:, 256 * q : 256 * q + 256] = r[...]


def make_unit(blocks):
    rows = blocks[0].shape[0]
    tile = 512
    return pl.pallas_call(
        unit_kernel,
        grid=(rows // tile,),
        in_specs=[pl.BlockSpec((tile, 256), lambda i: (i, 0))] * 4,
        out_specs=[
            pl.BlockSpec((tile, 1024), lambda i: (i, 0)),
            pl.BlockSpec((tile, 1024), lambda i: (i, 0)),
            pl.BlockSpec((tile, 128), lambda i: (i, 0)),
        ],
        out_shape=[
            jax.ShapeDtypeStruct((rows, 1024), BF16),
            jax.ShapeDtypeStruct((rows, 1024), BF16),
            jax.ShapeDtypeStruct((rows, 128), F32),
        ],
        compiler_params=params(),
        cost_estimate=cost(2e7),
        name="unit",
    )(*blocks)


def rows_kernel(s, x, out):
    out[...] = x[...]


def take_rows(x, at, rows):
    return pl.pallas_call(
        rows_kernel,
        grid_spec=pltpu.PrefetchScalarGridSpec(
            num_scalar_prefetch=1,
            grid=(1,),
            in_specs=[pl.BlockSpec((rows, 256), lambda i, s: (s[0], 0))],
            out_specs=pl.BlockSpec((rows, 256), lambda i, s: (0, 0)),
        ),
        out_shape=jax.ShapeDtypeStruct((rows, 256), BF16),
        compiler_params=params(),
        name="rows",
    )(at.reshape(1), x)


def message_kernel(part, mine, theirs, out):
    count = mine[...] + theirs[...]
    high = jnp.floor(count / 32.0)
    lane = lax.broadcasted_iota(jnp.int32, (8, 128), 1)
    extra = jnp.where(lane == 0, high, jnp.where(lane == 1, count - 32.0 * high, 0.0))
    extra = jnp.concatenate([extra, jnp.zeros((8, 128), F32)], axis=1).astype(BF16)
    for y in range(4):
        out[y, 0:PART, :] = part[...]
        out[y, PART : PART + 8, :] = extra


def make_message(part, mine, theirs):
    return pl.pallas_call(
        message_kernel,
        in_specs=vmem(3),
        out_specs=vmem(1)[0],
        out_shape=in_hbm((4, PART + 8, 256), BF16),
        compiler_params=params(),
        name="message",
    )(part, mine, theirs)


def read_count(far):
    lane = lax.broadcasted_iota(jnp.int32, (1, 256), 1)
    row = sum(far[y, PART : PART + 8, :].astype(F32)[0:1, :] for y in range(4))
    return jnp.sum(jnp.where(lane == 0, 32.0 * row, jnp.where(lane == 1, row, 0.0)))


def focal_kernel(s, t0, t1, t2, t3, unit, lane_f, labels, mask, keep, send, loss, count_out, acc):
    rows = unit.shape[0]
    half = keep.shape[0]
    count = read_count(t2)
    count_out[0, 0] = count
    u = [unit[:, 256 * q : 256 * q + 256] for q in range(4)]

    def dot(t, q):
        return lax.dot_general(t, u[q], NT, preferred_element_type=F32)

    for c in range(4):
        at = slice(PART * c, PART * c + PART)
        acc[at, :] = (
            dot(t0[at, :], 0) + dot(t1[at, :], 1) + dot(t2[c, 0:PART, :], 2) + dot(t3[c, 0:PART, :], 3)
        )
    shift = lane_f[0:1, :]
    scale = lane_f[1:2, :]
    factor = scale * (REGIONS / count)
    step = 32

    def part(out, start, total):
        wanted = labels[...] - (s[BASE] + start)

        def body(g, total):
            to = pl.multiple_of(g * step, step)
            at = pl.multiple_of(start + to, step)
            logit = (acc[pl.ds(at, step), :] + shift) * scale
            ids = lax.broadcasted_iota(jnp.int32, (step, rows), 0)
            target = (wanted - to) == ids
            m = jnp.where(target, -logit, logit)
            e = jnp.exp(-jnp.abs(m))
            r = 1.0 / (1.0 + e)
            er = e * r
            positive = m >= 0.0
            prob = jnp.where(positive, r, er)
            rest = jnp.where(positive, er, r)
            series = e * (1.0 - e * (0.5 - e * (1.0 / 3.0 - e * 0.25)))
            soft = jnp.maximum(m, 0.0) + jnp.where(e < 2e-3, series, jnp.log(1.0 + e))
            weight = jnp.where(target, 0.25, 0.75) * mask[pl.ds(at, step), :] * (prob * prob)
            slope = weight * (2.0 * rest * soft + prob)
            slope = jnp.where(target, -slope, slope)
            out[pl.ds(to, step), :] = (slope * factor).astype(BF16)
            term = weight * soft
            return total + sum(term[8 * i : 8 * i + 8, :] for i in range(step // 8))

        return lax.fori_loop(0, half // step, body, total)

    total = part(send, (1 - s[K]) * half, jnp.zeros((8, rows), F32))
    total = part(keep, s[K] * half, total)
    loss[...] = sum(total[:, 128 * i : 128 * i + 128] for i in range(4))


def make_focal(scalars, tables, unit, lane_f, labels, mask):
    rows = unit.shape[0] // 2
    classes = mask.shape[0]
    whole = lambda i, s: (0, 0)
    cube = lambda i, s: (0, 0, 0)
    return pl.pallas_call(
        focal_kernel,
        grid_spec=pltpu.PrefetchScalarGridSpec(
            num_scalar_prefetch=1,
            grid=(1,),
            in_specs=[pl.BlockSpec((classes, 256), whole)] * 2
            + [pl.BlockSpec((4, PART + 8, 256), cube)] * 2
            + [
                pl.BlockSpec((rows, 1024), lambda i, s: (s[K], 0)),
                pl.BlockSpec((8, rows), lambda i, s: (0, s[K])),
                pl.BlockSpec((1, rows), lambda i, s: (0, s[K])),
                pl.BlockSpec((classes, 1), whole),
            ],
            out_specs=[
                pl.BlockSpec((classes // 2, rows), whole),
                pl.BlockSpec((classes // 2, rows), whole),
                pl.BlockSpec((8, 128), whole),
                smem(),
            ],
            scratch_shapes=[pltpu.VMEM((classes, rows), F32)],
        ),
        out_shape=[
            jax.ShapeDtypeStruct((classes // 2, rows), BF16),
            jax.ShapeDtypeStruct((classes // 2, rows), BF16),
            jax.ShapeDtypeStruct((8, 128), F32),
            jax.ShapeDtypeStruct((1, 1), F32),
        ],
        compiler_params=params(24),
        cost_estimate=cost(1.4e9),
        name="focal",
    )(scalars, *tables, unit, lane_f, labels, mask)


def region_kernel(s, keep, send, t0, t1, t2, t3, raw, inv_ref, out, acc):
    half = keep.shape[0]
    k = s[K]
    tile = acc.shape[0]
    mine_at = pl.multiple_of(k * half, 32)
    theirs_at = pl.multiple_of((1 - k) * half, 32)

    def dot(g, t):
        return lax.dot_general(g, t, TN, preferred_element_type=F32)

    for i in range(keep.shape[1] // tile):
        rows = slice(tile * i, tile * i + tile)
        mine = keep[:, rows]
        theirs = send[:, rows]
        here = pl.ds(pl.multiple_of(keep.shape[1] * k + tile * i, tile), tile)
        inv = inv_ref[here, 0:1]
        along = 0.0
        for q, t in enumerate((t0, t1, t2, t3)):
            if q < 2:
                part = dot(mine, t[pl.ds(mine_at, half), :]) + dot(theirs, t[pl.ds(theirs_at, half), :])
            else:
                part = sum(
                    dot(g[PART * p : PART * p + PART, :], t[2 * at + p, 0:PART, :])
                    for g, at in ((mine, k), (theirs, 1 - k))
                    for p in range(2)
                )
            acc[:, 256 * q : 256 * q + 256] = part
            value = raw[here, 256 * q : 256 * q + 256].astype(F32)
            along += jnp.sum(part * value, axis=1, keepdims=True)
        back = inv * inv * along
        for q in range(4):
            cols = slice(256 * q, 256 * q + 256)
            grad = inv * (acc[:, cols] - raw[here, cols].astype(F32) * back)
            for p in range(tile // 64):
                z = tile // 64 * i + p
                out[z, :, cols] = grad[64 * p : 64 * p + 64, :].astype(BF16)


def make_region(scalars, keep, send, tables, raw, inv):
    return pl.pallas_call(
        region_kernel,
        in_specs=[smem()] + vmem(8),
        out_specs=vmem(1)[0],
        out_shape=in_hbm((8, 64, 1024), BF16),
        scratch_shapes=[pltpu.VMEM((256, 1024), F32)],
        compiler_params=params(24),
        cost_estimate=cost(1.4e9),
        name="region",
    )(scalars, keep, send, *tables, raw, inv)


def table_kernel(s, keep, other, unit, loss, *refs):
    outs, acc = refs[:8], refs[8]
    half, rows = other.shape
    mine = keep[...]
    theirs = other[...]
    mine_at = pl.multiple_of(s[K] * rows, rows)
    theirs_at = pl.multiple_of((1 - s[K]) * rows, rows)
    extra = split3(jnp.sum(loss[...]), 128).astype(BF16)
    for dy in range(4):
        cols = pl.ds(pl.multiple_of(256 * ((s[Y] + dy) % 4), 256), 256)
        acc[...] = jnp.dot(
            mine, unit[pl.ds(mine_at, rows), cols], preferred_element_type=F32
        ) + jnp.dot(theirs, unit[pl.ds(theirs_at, rows), cols], preferred_element_type=F32)
        for dx in range(2):
            at = pl.multiple_of(128 * (s[XL] ^ dx), 128)
            out = outs[2 * dy + dx]
            out[0:half, :] = acc[:, pl.ds(at, 128)].astype(BF16)
            out[half : half + 8, :] = extra


def make_table(scalars, keep, other, unit, loss):
    half = other.shape[0]
    return pl.pallas_call(
        table_kernel,
        in_specs=[smem()] + vmem(4),
        out_specs=vmem(8),
        out_shape=[jax.ShapeDtypeStruct((half + 8, 128), BF16)] * 8,
        scratch_shapes=[pltpu.VMEM((half, 256), F32)],
        compiler_params=params(),
        cost_estimate=cost(1.4e9),
        name="table",
    )(scalars, keep, other, unit, loss)


def table_sum_kernel(*refs):
    terms, (out, loss) = refs[:8], refs[8:]
    half = out.shape[0]
    out[...] = sum(t[0:half, :].astype(F32) for t in terms).astype(BF16)
    loss[...] = sum(t[half : half + 8, :].astype(F32) for t in terms)


def make_table_sum(terms):
    return pl.pallas_call(
        table_sum_kernel,
        in_specs=vmem(8),
        out_specs=vmem(2),
        out_shape=[
            jax.ShapeDtypeStruct((terms[0].shape[0] - 8, 128), BF16),
            jax.ShapeDtypeStruct((8, 128), F32),
        ],
        compiler_params=params(),
        cost_estimate=cost(1e7),
        name="table_sum",
    )(*terms)


def merge_kernel(terms, loss, *outs):
    total = sum(terms[z].astype(F32) for z in range(8)).astype(BF16)
    extra = split3(jnp.sum(loss[...]), 256).astype(BF16)
    for q, out in enumerate(outs):
        out[0:64, :] = total[:, 256 * q : 256 * q + 256]
        out[64:72, :] = extra


def make_merge(terms, loss):
    return pl.pallas_call(
        merge_kernel,
        in_specs=vmem(2),
        out_specs=vmem(4),
        out_shape=[jax.ShapeDtypeStruct((72, 256), BF16)] * 4,
        compiler_params=params(),
        cost_estimate=cost(1e7),
        name="merge",
    )(terms, loss)


def gather_kernel(chunk, out):
    rows = chunk[...]
    for j in range(8):
        out[j] = rows


def make_gather(chunk):
    return pl.pallas_call(
        gather_kernel,
        in_specs=vmem(1),
        out_specs=vmem(1)[0],
        out_shape=in_hbm((8,) + chunk.shape, BF16),
        compiler_params=params(),
        cost_estimate=cost(1e7),
        name="gather",
    )(chunk)


def share_kernel(s, own, near, far, both, out):
    k = s[K]
    for at, a, b in ((k, own, far), (1 - k, near, both)):
        total = a[0:64, :].astype(F32) + b[0:64, :].astype(F32)
        out[pl.ds(pl.multiple_of(64 * at, 64), 64), :] = total.astype(BF16)
    loss = jnp.sum(sum(r[64:72, :].astype(F32) for r in (own, near, far, both)))
    out[128:136, :] = split3(loss, 256).astype(BF16)


def make_share(scalars, parts):
    return pl.pallas_call(
        share_kernel,
        in_specs=[smem()] + vmem(4),
        out_specs=vmem(1)[0],
        out_shape=jax.ShapeDtypeStruct((136, 256), BF16),
        compiler_params=params(),
        cost_estimate=cost(1e7),
        name="share",
    )(scalars, *parts)


def table_final_kernel(s, tables, out, token):
    for y in range(4):
        at = pl.multiple_of(672 * (s[E] ^ y), 32)
        for x in range(2):
            out[pl.ds(at, 672), 128 * x : 128 * x + 128] = tables[2 * y + x]
    token[0, 0] = s[E]


def make_table_final(scalars, tables):
    return pl.pallas_call(
        table_final_kernel,
        in_specs=[smem()] + vmem(1),
        out_specs=vmem(1) + [smem()],
        out_shape=[
            jax.ShapeDtypeStruct((2688, 256), BF16),
            jax.ShapeDtypeStruct((1, 1), jnp.int32),
        ],
        compiler_params=params(),
        cost_estimate=cost(1e7),
        name="table_final",
    )(scalars, tables)


def region_final_kernel(s, token, count, *refs):
    regions, (out, loss_out) = refs[:8], refs[8:]
    total = jnp.sum(sum(r[128:136, :].astype(F32) for r in regions))
    for d in range(8):
        source = (s[Z] + 8 - d) % 8
        for k in range(2):
            out[k, source] = regions[d][64 * k : 64 * k + 64, :]
    loss_out[0, 0] = total / count[0, 0] / CLASSES


def make_region_final(scalars, token, count, regions):
    return pl.pallas_call(
        region_final_kernel,
        in_specs=[smem()] * 3 + vmem(8),
        out_specs=vmem(1) + [smem()],
        out_shape=[
            jax.ShapeDtypeStruct((2, 8, 64, 256), BF16),
            jax.ShapeDtypeStruct((1, 1), F32),
        ],
        compiler_params=params(),
        cost_estimate=cost(1e7),
        name="region_final",
    )(scalars, token, count, *regions)


def over_img(x, dy, dx):
    pairs = [
        (2 * y + xl, 2 * ((y + dy) % 4) + (xl ^ dx)) for y in range(4) for xl in range(2)
    ]
    return lax.ppermute(x, IMG, pairs)


def to_owner(x):
    axes = ("img_0",) + EMB
    return lax.ppermute(x, axes, [(4 * y + e, 4 * y + (e ^ y)) for y in range(4) for e in range(4)])


def along_cls(x, d):
    return lax.ppermute(x, CLS, [(i, (i + d) % 8) for i in range(8)])


def exchange(x, axes):
    return lax.all_to_all(x, axes, split_axis=0, concat_axis=0, tiled=True)


def shards(regions, table, shift, scale, labels, valid):
    rows = regions.shape[0]
    y = lax.axis_index("img_0")
    xl = lax.axis_index("img_1")
    xh = lax.axis_index("emb_0")
    k = lax.axis_index("emb_1")
    z = lax.axis_index(CLS)
    scalars = jnp.stack([k, z * 2688 + xh * 1344, 2 * xh + k, y, xl, z]).astype(jnp.int32)

    t_send = take_rows(pltpu.with_memory_space_constraint(table, pltpu.HBM), 4 * (1 - xh) + y, PART)
    t_send, regions_in = lax.optimization_barrier((t_send, regions))
    t_got = swap(t_send, "emb_0")
    r_far = swap(regions_in, "emb_0")
    r_near = swap(regions_in, "emb_1")
    local = jnp.broadcast_to(jnp.sum((labels >= 0).astype(F32)), (8, 128))
    local_other = swap(local, "img_1")
    t_far = exchange(make_message(t_got, local, local_other), "img_0")
    t_own = lax.dynamic_slice_in_dim(table, xh * 1344, 1344, 0)
    t_near = swap(t_own, "emb_1")
    r_both = swap(r_far, "emb_1")
    t_both = swap(t_far, "emb_1")
    blocks = (regions, r_near, r_far, r_both)
    tables = (t_own, t_near, t_far, t_both)
    unit, raw, inv = make_unit(blocks)

    lane_f = jnp.concatenate([shift[None], scale[None], jnp.zeros((6, rows), F32)], axis=0)
    mask = lax.dynamic_slice(valid, (k, xh * 1344), (1, 1344)).astype(F32).T
    keep, send, loss, count = make_focal(scalars, tables, unit, lane_f, labels[None], mask)

    theirs = swap(send, "emb_1")
    terms = exchange(make_region(scalars, keep, send, tables, raw, inv), CLS)
    chunks = list(make_table(scalars, keep, theirs, unit, loss))
    for o in OVER_IMG:
        chunks[o] = over_img(chunks[o], o // 2, o % 2)
    table_part, loss_part = make_table_sum(chunks)
    table_part = to_owner(table_part)
    parts = list(make_merge(terms, loss_part))
    for q in range(1, 4):
        parts[q] = lax.ppermute(parts[q], EMB, [(i, i ^ q) for i in range(4)])
    message = make_gather(table_part)
    table_all = exchange(message, IMG)
    share = make_share(scalars, parts)
    shares = [share] * 8
    for d in ALONG_CLS:
        shares[d] = along_cls(share, d)
    table_grad, token = make_table_final(scalars, table_all)
    region_grad, total = make_region_final(scalars, token, count, shares)
    return (total[0, 0], region_grad.reshape(rows, 256), table_grad)


OVER_IMG = (5, 3, 7, 1, 4, 2, 6)
ALONG_CLS = (4, 3, 5, 2, 6, 1, 7)


def solution(mesh):
    torus = Mesh(
        mesh.devices.reshape(4, 2, mesh.shape["cls"], 2, 2),
        ("img_0", "img_1", "cls", "emb_0", "emb_1"),
    )
    return jax.shard_map(
        shards,
        mesh=torus,
        in_specs=(P(IMG, EMB), P(CLS, EMB), P(IMG), P(IMG), P(IMG), P(IMG, CLS)),
        out_specs=(P(), P(IMG, EMB), P(CLS, EMB)),
        check_vma=False,
    )
```

```python
import jax
import jax.numpy as jnp
from jax import lax
from jax.experimental import pallas as pl
from jax.experimental.pallas import tpu as pltpu
from jax.sharding import Mesh
from jax.sharding import PartitionSpec as P

CLASSES = 21504
REGIONS = 8192
EMB = ("emb_0", "emb_1")
IMG = ("img_0", "img_1")
CLS = ("cls",)
F32 = jnp.float32
BF16 = jnp.bfloat16
NT = (((1,), (1,)), ((), ()))
TN = (((0,), (0,)), ((), ()))

K, BASE, E, Y, XL, Z = range(6)


PART = 336


def vmem(n):
    return [pl.BlockSpec(memory_space=pltpu.VMEM)] * n


def in_hbm(shape, dtype):
    return pltpu.HBM(shape, dtype)


def smem():
    return pl.BlockSpec(memory_space=pltpu.SMEM)


def params(mebibytes=16):
    return pltpu.CompilerParams(vmem_limit_bytes=mebibytes * 1024 * 1024)


def cost(flops):
    return pl.CostEstimate(flops=int(flops), bytes_accessed=1 << 20, transcendentals=0)


def swap(x, axis):
    return lax.ppermute(x, axis, [(0, 1), (1, 0)])


def split3(value, width):
    hi = value.astype(BF16).astype(F32)
    mid = (value - hi).astype(BF16).astype(F32)
    lo = value - hi - mid
    lane = lax.broadcasted_iota(jnp.int32, (8, width), 1)
    row = lax.broadcasted_iota(jnp.int32, (8, width), 0)
    packed = jnp.where(lane == 0, hi, jnp.where(lane == 1, mid, jnp.where(lane == 2, lo, 0.0)))
    return jnp.where(row == 0, packed, 0.0)


def unit_kernel(a, b, c, d, out, raw, scale):
    blocks = [r[...].astype(F32) for r in (a, b, c, d)]
    squares = sum(jnp.sum(v * v, axis=1, keepdims=True) for v in blocks)
    inv = lax.rsqrt(squares + 1e-06)
    scale[...] = jnp.broadcast_to(inv, scale.shape)
    for q, (v, r) in enumerate(zip(blocks, (a, b, c, d))):
        out[:, 256 * q : 256 * q + 256] = (v * inv).astype(BF16)
        raw[:, 256 * q : 256 * q + 256] = r[...]


def make_unit(blocks):
    rows = blocks[0].shape[0]
    tile = 512
    return pl.pallas_call(
        unit_kernel,
        grid=(rows // tile,),
        in_specs=[pl.BlockSpec((tile, 256), lambda i: (i, 0))] * 4,
        out_specs=[
            pl.BlockSpec((tile, 1024), lambda i: (i, 0)),
            pl.BlockSpec((tile, 1024), lambda i: (i, 0)),
            pl.BlockSpec((tile, 128), lambda i: (i, 0)),
        ],
        out_shape=[
            jax.ShapeDtypeStruct((rows, 1024), BF16),
            jax.ShapeDtypeStruct((rows, 1024), BF16),
            jax.ShapeDtypeStruct((rows, 128), F32),
        ],
        compiler_params=params(),
        cost_estimate=cost(2e7),
        name="unit",
    )(*blocks)


def rows_kernel(s, x, out, sem):
    rows = out.shape[0]
    copy = pltpu.make_async_copy(x.at[pl.ds(pl.multiple_of(s[0] * rows, 16), rows)], out, sem)
    copy.start()
    copy.wait()


def take_rows(x, at, rows):
    return pl.pallas_call(
        rows_kernel,
        in_specs=[smem(), pl.BlockSpec(memory_space=pltpu.HBM)],
        out_specs=vmem(1)[0],
        scratch_shapes=[pltpu.SemaphoreType.DMA],
        out_shape=jax.ShapeDtypeStruct((rows, 256), BF16),
        compiler_params=params(),
        name="rows",
    )(at.reshape(1), x)


def message_kernel(part, mine, theirs, out):
    count = mine[...] + theirs[...]
    high = jnp.floor(count / 32.0)
    lane = lax.broadcasted_iota(jnp.int32, (8, 128), 1)
    extra = jnp.where(lane == 0, high, jnp.where(lane == 1, count - 32.0 * high, 0.0))
    extra = jnp.concatenate([extra, jnp.zeros((8, 128), F32)], axis=1).astype(BF16)
    for y in range(4):
        out[y, 0:PART, :] = part[...]
        out[y, PART : PART + 8, :] = extra


def make_message(part, mine, theirs):
    return pl.pallas_call(
        message_kernel,
        in_specs=vmem(3),
        out_specs=vmem(1)[0],
        out_shape=in_hbm((4, PART + 8, 256), BF16),
        compiler_params=params(),
        name="message",
    )(part, mine, theirs)


def read_count(far):
    lane = lax.broadcasted_iota(jnp.int32, (1, 256), 1)
    row = sum(far[y, PART : PART + 8, :].astype(F32)[0:1, :] for y in range(4))
    return jnp.sum(jnp.where(lane == 0, 32.0 * row, jnp.where(lane == 1, row, 0.0)))


def focal_kernel(s, t0, t1, t2, t3, unit, lane_f, labels, mask, keep, send, loss, count_out, acc):
    rows = unit.shape[0]
    half = keep.shape[0]
    count = read_count(t2)
    count_out[...] = jnp.full((1, 1), count, F32)
    u = [unit[:, 256 * q : 256 * q + 256] for q in range(4)]

    def dot(t, q):
        return lax.dot_general(t, u[q], NT, preferred_element_type=F32)

    for c in range(4):
        at = slice(PART * c, PART * c + PART)
        acc[at, :] = (
            dot(t0[at, :], 0) + dot(t1[at, :], 1) + dot(t2[c, 0:PART, :], 2) + dot(t3[c, 0:PART, :], 3)
        )
    shift = lane_f[0:1, :]
    scale = lane_f[1:2, :]
    factor = scale * (REGIONS / count)
    step = 32

    def part(out, start, total):
        wanted = labels[...] - (s[BASE] + start)

        def body(g, total):
            to = pl.multiple_of(g * step, step)
            at = pl.multiple_of(start + to, step)
            logit = (acc[pl.ds(at, step), :] + shift) * scale
            ids = lax.broadcasted_iota(jnp.int32, (step, rows), 0)
            target = (wanted - to) == ids
            m = jnp.where(target, -logit, logit)
            e = jnp.exp(-jnp.abs(m))
            r = 1.0 / (1.0 + e)
            er = e * r
            positive = m >= 0.0
            prob = jnp.where(positive, r, er)
            rest = jnp.where(positive, er, r)
            series = e * (1.0 - e * (0.5 - e * (1.0 / 3.0 - e * 0.25)))
            soft = jnp.maximum(m, 0.0) + jnp.where(e < 2e-3, series, jnp.log(1.0 + e))
            weight = jnp.where(target, 0.25, 0.75) * mask[pl.ds(at, step), :] * (prob * prob)
            slope = weight * (2.0 * rest * soft + prob)
            slope = jnp.where(target, -slope, slope)
            out[pl.ds(to, step), :] = (slope * factor).astype(BF16)
            term = weight * soft
            return total + sum(term[8 * i : 8 * i + 8, :] for i in range(step // 8))

        return lax.fori_loop(0, half // step, body, total)

    total = part(send, (1 - s[K]) * half, jnp.zeros((8, rows), F32))
    total = part(keep, s[K] * half, total)
    loss[...] = sum(total[:, 128 * i : 128 * i + 128] for i in range(4))


def make_focal(scalars, tables, unit, lane_f, labels, mask):
    rows = unit.shape[0] // 2
    classes = mask.shape[0]
    whole = lambda i, s: (0, 0)
    cube = lambda i, s: (0, 0, 0)
    return pl.pallas_call(
        focal_kernel,
        grid_spec=pltpu.PrefetchScalarGridSpec(
            num_scalar_prefetch=1,
            grid=(1,),
            in_specs=[pl.BlockSpec((classes, 256), whole)] * 2
            + [pl.BlockSpec((4, PART + 8, 256), cube)] * 2
            + [
                pl.BlockSpec((rows, 1024), lambda i, s: (s[K], 0)),
                pl.BlockSpec((8, rows), lambda i, s: (0, s[K])),
                pl.BlockSpec((1, rows), lambda i, s: (0, s[K])),
                pl.BlockSpec((classes, 1), whole),
            ],
            out_specs=[
                pl.BlockSpec((classes // 2, rows), whole),
                pl.BlockSpec((classes // 2, rows), whole),
                pl.BlockSpec((8, 128), whole),
                pl.BlockSpec((1, 1), whole),
            ],
            scratch_shapes=[pltpu.VMEM((classes, rows), F32)],
        ),
        out_shape=[
            jax.ShapeDtypeStruct((classes // 2, rows), BF16),
            jax.ShapeDtypeStruct((classes // 2, rows), BF16),
            jax.ShapeDtypeStruct((8, 128), F32),
            jax.ShapeDtypeStruct((1, 1), F32),
        ],
        compiler_params=params(24),
        cost_estimate=cost(1.4e9),
        name="focal",
    )(scalars, *tables, unit, lane_f, labels, mask)


def region_kernel(s, keep, send, t0, t1, t2, t3, raw, inv_ref, out, acc):
    half = keep.shape[0]
    k = s[K]
    tile = acc.shape[0]
    mine_at = pl.multiple_of(k * half, 32)
    theirs_at = pl.multiple_of((1 - k) * half, 32)

    def dot(g, t):
        return lax.dot_general(g, t, TN, preferred_element_type=F32)

    for i in range(keep.shape[1] // tile):
        rows = slice(tile * i, tile * i + tile)
        mine = keep[:, rows]
        theirs = send[:, rows]
        here = pl.ds(pl.multiple_of(keep.shape[1] * k + tile * i, tile), tile)
        inv = inv_ref[here, 0:1]
        along = 0.0
        for q, t in enumerate((t0, t1, t2, t3)):
            if q < 2:
                part = dot(mine, t[pl.ds(mine_at, half), :]) + dot(theirs, t[pl.ds(theirs_at, half), :])
            else:
                part = sum(
                    dot(g[PART * p : PART * p + PART, :], t[2 * at + p, 0:PART, :])
                    for g, at in ((mine, k), (theirs, 1 - k))
                    for p in range(2)
                )
            acc[:, 256 * q : 256 * q + 256] = part
            value = raw[here, 256 * q : 256 * q + 256].astype(F32)
            along += jnp.sum(part * value, axis=1, keepdims=True)
        back = inv * inv * along
        for q in range(4):
            cols = slice(256 * q, 256 * q + 256)
            grad = inv * (acc[:, cols] - raw[here, cols].astype(F32) * back)
            for p in range(tile // 64):
                z = tile // 64 * i + p
                out[z, :, cols] = grad[64 * p : 64 * p + 64, :].astype(BF16)


def make_region(scalars, keep, send, tables, raw, inv):
    return pl.pallas_call(
        region_kernel,
        in_specs=[smem()] + vmem(8),
        out_specs=vmem(1)[0],
        out_shape=in_hbm((8, 64, 1024), BF16),
        scratch_shapes=[pltpu.VMEM((256, 1024), F32)],
        compiler_params=params(24),
        cost_estimate=cost(1.4e9),
        name="region",
    )(scalars, keep, send, *tables, raw, inv)


def table_kernel(s, keep, other, unit, loss, *refs):
    outs, acc = refs[:8], refs[8]
    half, rows = other.shape
    mine = keep[...]
    theirs = other[...]
    mine_at = pl.multiple_of(s[K] * rows, rows)
    theirs_at = pl.multiple_of((1 - s[K]) * rows, rows)
    extra = split3(jnp.sum(loss[...]), 128).astype(BF16)
    for dy in range(4):
        cols = pl.ds(pl.multiple_of(256 * ((s[Y] + dy) % 4), 256), 256)
        acc[...] = jnp.dot(
            mine, unit[pl.ds(mine_at, rows), cols], preferred_element_type=F32
        ) + jnp.dot(theirs, unit[pl.ds(theirs_at, rows), cols], preferred_element_type=F32)
        for dx in range(2):
            at = pl.multiple_of(128 * (s[XL] ^ dx), 128)
            out = outs[2 * dy + dx]
            out[0:half, :] = acc[:, pl.ds(at, 128)].astype(BF16)
            out[half : half + 8, :] = extra


def make_table(scalars, keep, other, unit, loss):
    half = other.shape[0]
    return pl.pallas_call(
        table_kernel,
        in_specs=[smem()] + vmem(4),
        out_specs=vmem(8),
        out_shape=[jax.ShapeDtypeStruct((half + 8, 128), BF16)] * 8,
        scratch_shapes=[pltpu.VMEM((half, 256), F32)],
        compiler_params=params(),
        cost_estimate=cost(1.4e9),
        name="table",
    )(scalars, keep, other, unit, loss)


def table_sum_kernel(*refs):
    terms, (out, loss) = refs[:8], refs[8:]
    half = out.shape[0]
    out[...] = sum(t[0:half, :].astype(F32) for t in terms).astype(BF16)
    loss[...] = sum(t[half : half + 8, :].astype(F32) for t in terms)


def make_table_sum(terms):
    return pl.pallas_call(
        table_sum_kernel,
        in_specs=vmem(8),
        out_specs=vmem(2),
        out_shape=[
            jax.ShapeDtypeStruct((terms[0].shape[0] - 8, 128), BF16),
            jax.ShapeDtypeStruct((8, 128), F32),
        ],
        compiler_params=params(),
        cost_estimate=cost(1e7),
        name="table_sum",
    )(*terms)


def merge_kernel(terms, loss, *outs):
    total = sum(terms[z].astype(F32) for z in range(8)).astype(BF16)
    extra = split3(jnp.sum(loss[...]), 256).astype(BF16)
    for q, out in enumerate(outs):
        out[0:64, :] = total[:, 256 * q : 256 * q + 256]
        out[64:72, :] = extra


def make_merge(terms, loss):
    return pl.pallas_call(
        merge_kernel,
        in_specs=vmem(2),
        out_specs=vmem(4),
        out_shape=[jax.ShapeDtypeStruct((72, 256), BF16)] * 4,
        compiler_params=params(),
        cost_estimate=cost(1e7),
        name="merge",
    )(terms, loss)


def gather_kernel(chunk, out, sems):
    copies = [pltpu.make_async_copy(chunk, out.at[j], sems.at[j]) for j in range(8)]
    for copy in copies:
        copy.start()
    for copy in copies:
        copy.wait()


def make_gather(chunk):
    return pl.pallas_call(
        gather_kernel,
        in_specs=vmem(1),
        out_specs=pl.BlockSpec(memory_space=pltpu.HBM),
        out_shape=in_hbm((8,) + chunk.shape, BF16),
        scratch_shapes=[pltpu.SemaphoreType.DMA((8,))],
        compiler_params=params(),
        cost_estimate=cost(1e7),
        name="gather",
    )(chunk)


def share_kernel(s, own, near, far, both, out):
    k = s[K]
    for at, a, b in ((k, own, far), (1 - k, near, both)):
        total = a[0:64, :].astype(F32) + b[0:64, :].astype(F32)
        out[pl.ds(pl.multiple_of(64 * at, 64), 64), :] = total.astype(BF16)
    loss = jnp.sum(sum(r[64:72, :].astype(F32) for r in (own, near, far, both)))
    out[128:136, :] = split3(loss, 256).astype(BF16)


def make_share(scalars, parts):
    return pl.pallas_call(
        share_kernel,
        in_specs=[smem()] + vmem(4),
        out_specs=vmem(1)[0],
        out_shape=jax.ShapeDtypeStruct((136, 256), BF16),
        compiler_params=params(),
        cost_estimate=cost(1e7),
        name="share",
    )(scalars, *parts)


def table_final_kernel(s, tables, out):
    for y in range(4):
        at = pl.multiple_of(672 * (s[E] ^ y), 32)
        for x in range(2):
            out[pl.ds(at, 672), 128 * x : 128 * x + 128] = tables[2 * y + x]


def make_table_final(scalars, tables):
    return pl.pallas_call(
        table_final_kernel,
        in_specs=[smem()] + vmem(1),
        out_specs=vmem(1)[0],
        out_shape=jax.ShapeDtypeStruct((2688, 256), BF16),
        compiler_params=params(),
        cost_estimate=cost(1e7),
        name="table_final",
    )(scalars, tables)


def region_final_kernel(s, count, *refs):
    regions, (out, loss_out) = refs[:8], refs[8:]
    total = jnp.sum(sum(r[128:136, :].astype(F32) for r in regions), keepdims=True)
    for d in range(8):
        source = (s[Z] + 8 - d) % 8
        for k in range(2):
            out[k, source] = regions[d][64 * k : 64 * k + 64, :]
    loss_out[...] = total / count[...] / CLASSES


def make_region_final(scalars, count, regions):
    return pl.pallas_call(
        region_final_kernel,
        in_specs=[smem()] + vmem(9),
        out_specs=vmem(2),
        out_shape=[
            jax.ShapeDtypeStruct((2, 8, 64, 256), BF16),
            jax.ShapeDtypeStruct((1, 1), F32),
        ],
        compiler_params=params(),
        cost_estimate=cost(1e7),
        name="region_final",
    )(scalars, count, *regions)


def over_img(x, dy, dx):
    pairs = [
        (2 * y + xl, 2 * ((y + dy) % 4) + (xl ^ dx)) for y in range(4) for xl in range(2)
    ]
    return lax.ppermute(x, IMG, pairs)


def to_owner(x):
    axes = ("img_0",) + EMB
    return lax.ppermute(x, axes, [(4 * y + e, 4 * y + (e ^ y)) for y in range(4) for e in range(4)])


def along_cls(x, d):
    return lax.ppermute(x, CLS, [(i, (i + d) % 8) for i in range(8)])


def exchange(x, axes):
    return lax.all_to_all(x, axes, split_axis=0, concat_axis=0, tiled=True)


def shards(regions, table, shift, scale, labels, valid):
    rows = regions.shape[0]
    y = lax.axis_index("img_0")
    xl = lax.axis_index("img_1")
    xh = lax.axis_index("emb_0")
    k = lax.axis_index("emb_1")
    z = lax.axis_index(CLS)
    scalars = jnp.stack([k, z * 2688 + xh * 1344, 2 * xh + k, y, xl, z]).astype(jnp.int32)

    t_send = take_rows(pltpu.with_memory_space_constraint(table, pltpu.HBM), 4 * (1 - xh) + y, PART)
    t_send, regions_in = lax.optimization_barrier((t_send, regions))
    t_got = swap(t_send, "emb_0")
    r_far = swap(regions_in, "emb_0")
    r_near = swap(regions_in, "emb_1")
    local = jnp.broadcast_to(jnp.sum((labels >= 0).astype(F32)), (8, 128))
    local_other = swap(local, "img_1")
    t_far = exchange(make_message(t_got, local, local_other), "img_0")
    t_own = lax.dynamic_slice_in_dim(table, xh * 1344, 1344, 0)
    t_near = swap(t_own, "emb_1")
    r_both = swap(r_far, "emb_1")
    t_both = swap(t_far, "emb_1")
    blocks = (regions, r_near, r_far, r_both)
    tables = (t_own, t_near, t_far, t_both)
    unit, raw, inv = make_unit(blocks)

    lane_f = jnp.concatenate([shift[None], scale[None], jnp.zeros((6, rows), F32)], axis=0)
    mask = lax.dynamic_slice(valid, (k, xh * 1344), (1, 1344)).astype(F32).T
    keep, send, loss, count = make_focal(scalars, tables, unit, lane_f, labels[None], mask)

    theirs = swap(send, "emb_1")
    terms = exchange(make_region(scalars, keep, send, tables, raw, inv), CLS)
    chunks = list(make_table(scalars, keep, theirs, unit, loss))
    for o in OVER_IMG:
        chunks[o] = over_img(chunks[o], o // 2, o % 2)
    table_part, loss_part = make_table_sum(chunks)
    table_part = to_owner(table_part)
    parts = list(make_merge(terms, loss_part))
    for q in range(1, 4):
        parts[q] = lax.ppermute(parts[q], EMB, [(i, i ^ q) for i in range(4)])
    message = make_gather(table_part)
    table_all = exchange(message, IMG)
    share = make_share(scalars, parts)
    shares = [share] * 8
    for d in ALONG_CLS:
        shares[d] = along_cls(share, d)
    table_grad = make_table_final(scalars, table_all)
    region_grad, total = make_region_final(scalars, count, shares)
    return (total[0, 0], region_grad.reshape(rows, 256), table_grad)


OVER_IMG = (3, 6, 5, 2, 7, 4, 1)
ALONG_CLS = (4, 3, 5, 2, 6, 1, 7)


def solution(mesh):
    torus = Mesh(
        mesh.devices.reshape(4, 2, mesh.shape["cls"], 2, 2),
        ("img_0", "img_1", "cls", "emb_0", "emb_1"),
    )
    return jax.shard_map(
        shards,
        mesh=torus,
        in_specs=(P(IMG, EMB), P(CLS, EMB), P(IMG), P(IMG), P(IMG), P(IMG, CLS)),
        out_specs=(P(), P(IMG, EMB), P(CLS, EMB)),
        check_vma=False,
    )
```

```python
import jax
import jax.numpy as jnp
from jax import lax
from jax.experimental import pallas as pl
from jax.experimental.pallas import tpu as pltpu
from jax.sharding import Mesh
from jax.sharding import PartitionSpec as P

CLASSES = 21504
REGIONS = 8192
EMB = ("emb_0", "emb_1")
IMG = ("img_0", "img_1")
CLS = ("cls",)
F32 = jnp.float32
BF16 = jnp.bfloat16
NT = (((1,), (1,)), ((), ()))
TN = (((0,), (0,)), ((), ()))

K, BASE, E, Y, XL, Z = range(6)


PART = 336


def vmem(n):
    return [pl.BlockSpec(memory_space=pltpu.VMEM)] * n


def in_hbm(shape, dtype):
    return pltpu.HBM(shape, dtype)


def smem():
    return pl.BlockSpec(memory_space=pltpu.SMEM)


def params(mebibytes=16):
    return pltpu.CompilerParams(vmem_limit_bytes=mebibytes * 1024 * 1024)


def cost(flops):
    return pl.CostEstimate(flops=int(flops), bytes_accessed=1 << 20, transcendentals=0)


def swap(x, axis):
    return lax.ppermute(x, axis, [(0, 1), (1, 0)])


def split3(value, width):
    hi = value.astype(BF16).astype(F32)
    mid = (value - hi).astype(BF16).astype(F32)
    lo = value - hi - mid
    lane = lax.broadcasted_iota(jnp.int32, (8, width), 1)
    row = lax.broadcasted_iota(jnp.int32, (8, width), 0)
    packed = jnp.where(lane == 0, hi, jnp.where(lane == 1, mid, jnp.where(lane == 2, lo, 0.0)))
    return jnp.where(row == 0, packed, 0.0)


def unit_kernel(a, b, c, d, out, raw, scale):
    blocks = [r[...].astype(F32) for r in (a, b, c, d)]
    squares = sum(jnp.sum(v * v, axis=1, keepdims=True) for v in blocks)
    inv = lax.rsqrt(squares + 1e-06)
    scale[...] = jnp.broadcast_to(inv, scale.shape)
    for q, (v, r) in enumerate(zip(blocks, (a, b, c, d))):
        out[:, 256 * q : 256 * q + 256] = (v * inv).astype(BF16)
        raw[:, 256 * q : 256 * q + 256] = r[...]


def make_unit(blocks):
    rows = blocks[0].shape[0]
    tile = 512
    return pl.pallas_call(
        unit_kernel,
        grid=(rows // tile,),
        in_specs=[pl.BlockSpec((tile, 256), lambda i: (i, 0))] * 4,
        out_specs=[
            pl.BlockSpec((tile, 1024), lambda i: (i, 0)),
            pl.BlockSpec((tile, 1024), lambda i: (i, 0)),
            pl.BlockSpec((tile, 128), lambda i: (i, 0)),
        ],
        out_shape=[
            jax.ShapeDtypeStruct((rows, 1024), BF16),
            jax.ShapeDtypeStruct((rows, 1024), BF16),
            jax.ShapeDtypeStruct((rows, 128), F32),
        ],
        compiler_params=params(),
        cost_estimate=cost(2e7),
        name="unit",
    )(*blocks)


def rows_kernel(s, x, out, sem):
    rows = out.shape[0]
    copy = pltpu.make_async_copy(x.at[pl.ds(pl.multiple_of(s[0] * rows, 16), rows)], out, sem)
    copy.start()
    copy.wait()


def take_rows(x, at, rows):
    return pl.pallas_call(
        rows_kernel,
        in_specs=[smem(), pl.BlockSpec(memory_space=pltpu.HBM)],
        out_specs=vmem(1)[0],
        scratch_shapes=[pltpu.SemaphoreType.DMA],
        out_shape=jax.ShapeDtypeStruct((rows, 256), BF16),
        compiler_params=params(),
        name="rows",
    )(at.reshape(1), x)


def message_kernel(part, mine, theirs, out):
    count = mine[...] + theirs[...]
    high = jnp.floor(count / 32.0)
    lane = lax.broadcasted_iota(jnp.int32, (8, 128), 1)
    extra = jnp.where(lane == 0, high, jnp.where(lane == 1, count - 32.0 * high, 0.0))
    extra = jnp.concatenate([extra, jnp.zeros((8, 128), F32)], axis=1).astype(BF16)
    for y in range(4):
        out[y, 0:PART, :] = part[...]
        out[y, PART : PART + 8, :] = extra


def make_message(part, mine, theirs):
    return pl.pallas_call(
        message_kernel,
        in_specs=vmem(3),
        out_specs=vmem(1)[0],
        out_shape=in_hbm((4, PART + 8, 256), BF16),
        compiler_params=params(),
        name="message",
    )(part, mine, theirs)


def read_count(far):
    lane = lax.broadcasted_iota(jnp.int32, (1, 256), 1)
    row = sum(far[y, PART : PART + 8, :].astype(F32)[0:1, :] for y in range(4))
    return jnp.sum(jnp.where(lane == 0, 32.0 * row, jnp.where(lane == 1, row, 0.0)))


def focal_kernel(s, t0, t1, t2, t3, unit, lane_f, labels, mask, keep, send, loss, count_out, acc):
    rows = unit.shape[0]
    half = keep.shape[0]
    count = read_count(t2)
    count_out[...] = jnp.full((1, 1), count, F32)
    u = [unit[:, 256 * q : 256 * q + 256] for q in range(4)]

    def dot(t, q):
        return lax.dot_general(t, u[q], NT, preferred_element_type=F32)

    for c in range(4):
        at = slice(PART * c, PART * c + PART)
        acc[at, :] = (
            dot(t0[at, :], 0) + dot(t1[at, :], 1) + dot(t2[c, 0:PART, :], 2) + dot(t3[c, 0:PART, :], 3)
        )
    shift = lane_f[0:1, :]
    scale = lane_f[1:2, :]
    factor = scale * (REGIONS / count)
    step = 32

    def part(out, start, total):
        wanted = labels[...] - (s[BASE] + start)

        def body(g, total):
            to = pl.multiple_of(g * step, step)
            at = pl.multiple_of(start + to, step)
            logit = (acc[pl.ds(at, step), :] + shift) * scale
            ids = lax.broadcasted_iota(jnp.int32, (step, rows), 0)
            target = (wanted - to) == ids
            m = jnp.where(target, -logit, logit)
            e = jnp.exp(-jnp.abs(m))
            r = 1.0 / (1.0 + e)
            er = e * r
            positive = m >= 0.0
            prob = jnp.where(positive, r, er)
            rest = jnp.where(positive, er, r)
            series = e * (1.0 - e * (0.5 - e * (1.0 / 3.0 - e * 0.25)))
            soft = jnp.maximum(m, 0.0) + jnp.where(e < 2e-3, series, jnp.log(1.0 + e))
            weight = jnp.where(target, 0.25, 0.75) * mask[pl.ds(at, step), :] * (prob * prob)
            slope = weight * (2.0 * rest * soft + prob)
            slope = jnp.where(target, -slope, slope)
            out[pl.ds(to, step), :] = (slope * factor).astype(BF16)
            term = weight * soft
            return total + sum(term[8 * i : 8 * i + 8, :] for i in range(step // 8))

        return lax.fori_loop(0, half // step, body, total)

    total = part(send, (1 - s[K]) * half, jnp.zeros((8, rows), F32))
    total = part(keep, s[K] * half, total)
    loss[...] = sum(total[:, 128 * i : 128 * i + 128] for i in range(4))


def make_focal(scalars, tables, unit, lane_f, labels, mask):
    rows = unit.shape[0] // 2
    classes = mask.shape[0]
    whole = lambda i, s: (0, 0)
    cube = lambda i, s: (0, 0, 0)
    return pl.pallas_call(
        focal_kernel,
        grid_spec=pltpu.PrefetchScalarGridSpec(
            num_scalar_prefetch=1,
            grid=(1,),
            in_specs=[pl.BlockSpec((classes, 256), whole)] * 2
            + [pl.BlockSpec((4, PART + 8, 256), cube)] * 2
            + [
                pl.BlockSpec((rows, 1024), lambda i, s: (s[K], 0)),
                pl.BlockSpec((8, rows), lambda i, s: (0, s[K])),
                pl.BlockSpec((1, rows), lambda i, s: (0, s[K])),
                pl.BlockSpec((classes, 1), whole),
            ],
            out_specs=[
                pl.BlockSpec((classes // 2, rows), whole),
                pl.BlockSpec((classes // 2, rows), whole),
                pl.BlockSpec((8, 128), whole),
                pl.BlockSpec((1, 1), whole),
            ],
            scratch_shapes=[pltpu.VMEM((classes, rows), F32)],
        ),
        out_shape=[
            jax.ShapeDtypeStruct((classes // 2, rows), BF16),
            jax.ShapeDtypeStruct((classes // 2, rows), BF16),
            jax.ShapeDtypeStruct((8, 128), F32),
            jax.ShapeDtypeStruct((1, 1), F32),
        ],
        compiler_params=params(24),
        cost_estimate=cost(1.4e9),
        name="focal",
    )(scalars, *tables, unit, lane_f, labels, mask)


def region_kernel(s, keep, send, t0, t1, t2, t3, raw, inv_ref, out, kept, acc, sem):
    half = keep.shape[0]
    copy = pltpu.make_async_copy(keep, kept, sem)
    copy.start()
    k = s[K]
    tile = acc.shape[0]
    mine_at = pl.multiple_of(k * half, 32)
    theirs_at = pl.multiple_of((1 - k) * half, 32)

    def dot(g, t):
        return lax.dot_general(g, t, TN, preferred_element_type=F32)

    for i in range(keep.shape[1] // tile):
        rows = slice(tile * i, tile * i + tile)
        mine = keep[:, rows]
        theirs = send[:, rows]
        here = pl.ds(pl.multiple_of(keep.shape[1] * k + tile * i, tile), tile)
        inv = inv_ref[here, 0:1]
        along = 0.0
        for q, t in enumerate((t0, t1, t2, t3)):
            if q < 2:
                part = dot(mine, t[pl.ds(mine_at, half), :]) + dot(theirs, t[pl.ds(theirs_at, half), :])
            else:
                part = sum(
                    dot(g[PART * p : PART * p + PART, :], t[2 * at + p, 0:PART, :])
                    for g, at in ((mine, k), (theirs, 1 - k))
                    for p in range(2)
                )
            acc[:, 256 * q : 256 * q + 256] = part
            value = raw[here, 256 * q : 256 * q + 256].astype(F32)
            along += jnp.sum(part * value, axis=1, keepdims=True)
        back = inv * inv * along
        for q in range(4):
            cols = slice(256 * q, 256 * q + 256)
            grad = inv * (acc[:, cols] - raw[here, cols].astype(F32) * back)
            for p in range(tile // 64):
                z = tile // 64 * i + p
                out[z, :, cols] = grad[64 * p : 64 * p + 64, :].astype(BF16)
    copy.wait()


def make_region(scalars, keep, send, tables, raw, inv):
    return pl.pallas_call(
        region_kernel,
        in_specs=[smem()] + vmem(8),
        out_specs=vmem(1) + [pl.BlockSpec(memory_space=pltpu.HBM)],
        out_shape=[in_hbm((8, 64, 1024), BF16), in_hbm(keep.shape, BF16)],
        scratch_shapes=[pltpu.VMEM((256, 1024), F32), pltpu.SemaphoreType.DMA],
        compiler_params=params(24),
        cost_estimate=cost(1.4e9),
        name="region",
    )(scalars, keep, send, *tables, raw, inv)


def table_kernel(s, kept, other, unit, loss, *refs):
    outs, (acc, keep, theirs, sems) = refs[:8], refs[8:]
    half, rows = other.shape
    other_copy = pltpu.make_async_copy(other, theirs, sems.at[0])
    copy = pltpu.make_async_copy(kept, keep, sems.at[1])
    other_copy.start()
    copy.start()
    other_copy.wait()
    mine_at = pl.multiple_of(s[K] * rows, rows)
    theirs_at = pl.multiple_of((1 - s[K]) * rows, rows)
    extra = split3(jnp.sum(loss[...]), 128).astype(BF16)
    for dy in range(4):
        cols = pl.ds(pl.multiple_of(256 * ((s[Y] + dy) % 4), 256), 256)
        part = jnp.dot(theirs[...], unit[pl.ds(theirs_at, rows), cols], preferred_element_type=F32)
        if dy == 0:
            acc[...] = part
            copy.wait()
            part = acc[...]
        acc[...] = part + jnp.dot(
            keep[...], unit[pl.ds(mine_at, rows), cols], preferred_element_type=F32
        )
        for dx in range(2):
            at = pl.multiple_of(128 * (s[XL] ^ dx), 128)
            out = outs[2 * dy + dx]
            out[0:half, :] = acc[:, pl.ds(at, 128)].astype(BF16)
            out[half : half + 8, :] = extra


def make_table(scalars, kept, other, unit, loss):
    half = other.shape[0]
    return pl.pallas_call(
        table_kernel,
        in_specs=[smem()] + [pl.BlockSpec(memory_space=pltpu.HBM)] * 2 + vmem(2),
        out_specs=vmem(8),
        out_shape=[jax.ShapeDtypeStruct((half + 8, 128), BF16)] * 8,
        scratch_shapes=[
            pltpu.VMEM((half, 256), F32),
            pltpu.VMEM(other.shape, BF16),
            pltpu.VMEM(other.shape, BF16),
            pltpu.SemaphoreType.DMA((2,)),
        ],
        compiler_params=params(),
        cost_estimate=cost(1.4e9),
        name="table",
    )(scalars, kept, other, unit, loss)


def table_sum_kernel(*refs):
    terms, (out, loss) = refs[:8], refs[8:]
    half = out.shape[0]
    out[...] = sum(t[0:half, :].astype(F32) for t in terms).astype(BF16)
    loss[...] = sum(t[half : half + 8, :].astype(F32) for t in terms)


def make_table_sum(terms):
    return pl.pallas_call(
        table_sum_kernel,
        in_specs=vmem(8),
        out_specs=vmem(2),
        out_shape=[
            jax.ShapeDtypeStruct((terms[0].shape[0] - 8, 128), BF16),
            jax.ShapeDtypeStruct((8, 128), F32),
        ],
        compiler_params=params(),
        cost_estimate=cost(1e7),
        name="table_sum",
    )(*terms)


def merge_kernel(terms, loss, *outs):
    total = sum(terms[z].astype(F32) for z in range(8)).astype(BF16)
    extra = split3(jnp.sum(loss[...]), 256).astype(BF16)
    for q, out in enumerate(outs):
        out[0:64, :] = total[:, 256 * q : 256 * q + 256]
        out[64:72, :] = extra


def make_merge(terms, loss):
    return pl.pallas_call(
        merge_kernel,
        in_specs=vmem(2),
        out_specs=vmem(4),
        out_shape=[jax.ShapeDtypeStruct((72, 256), BF16)] * 4,
        compiler_params=params(),
        cost_estimate=cost(1e7),
        name="merge",
    )(terms, loss)


def gather_kernel(chunk, out, sems):
    copies = [pltpu.make_async_copy(chunk, out.at[j], sems.at[j]) for j in range(8)]
    for copy in copies:
        copy.start()
    for copy in copies:
        copy.wait()


def make_gather(chunk):
    return pl.pallas_call(
        gather_kernel,
        in_specs=vmem(1),
        out_specs=pl.BlockSpec(memory_space=pltpu.HBM),
        out_shape=in_hbm((8,) + chunk.shape, BF16),
        scratch_shapes=[pltpu.SemaphoreType.DMA((8,))],
        compiler_params=params(),
        cost_estimate=cost(1e7),
        name="gather",
    )(chunk)


def share_kernel(s, own, near, far, both, out):
    k = s[K]
    for at, a, b in ((k, own, far), (1 - k, near, both)):
        total = a[0:64, :].astype(F32) + b[0:64, :].astype(F32)
        out[pl.ds(pl.multiple_of(64 * at, 64), 64), :] = total.astype(BF16)
    loss = jnp.sum(sum(r[64:72, :].astype(F32) for r in (own, near, far, both)))
    out[128:136, :] = split3(loss, 256).astype(BF16)


def make_share(scalars, parts):
    return pl.pallas_call(
        share_kernel,
        in_specs=[smem()] + vmem(4),
        out_specs=vmem(1)[0],
        out_shape=jax.ShapeDtypeStruct((136, 256), BF16),
        compiler_params=params(),
        cost_estimate=cost(1e7),
        name="share",
    )(scalars, *parts)


def table_final_kernel(s, tables, out):
    for y in range(4):
        at = pl.multiple_of(672 * (s[E] ^ y), 32)
        for x in range(2):
            out[pl.ds(at, 672), 128 * x : 128 * x + 128] = tables[2 * y + x]


def make_table_final(scalars, tables):
    return pl.pallas_call(
        table_final_kernel,
        in_specs=[smem()] + vmem(1),
        out_specs=vmem(1)[0],
        out_shape=jax.ShapeDtypeStruct((2688, 256), BF16),
        compiler_params=params(),
        cost_estimate=cost(1e7),
        name="table_final",
    )(scalars, tables)


def region_final_kernel(s, count, *refs):
    regions, (out, loss_out) = refs[:8], refs[8:]
    total = jnp.sum(sum(r[128:136, :].astype(F32) for r in regions), keepdims=True)
    for d in range(8):
        source = (s[Z] + 8 - d) % 8
        for k in range(2):
            out[k, source] = regions[d][64 * k : 64 * k + 64, :]
    loss_out[...] = total / count[...] / CLASSES


def make_region_final(scalars, count, regions):
    return pl.pallas_call(
        region_final_kernel,
        in_specs=[smem()] + vmem(9),
        out_specs=vmem(2),
        out_shape=[
            jax.ShapeDtypeStruct((2, 8, 64, 256), BF16),
            jax.ShapeDtypeStruct((1, 1), F32),
        ],
        compiler_params=params(),
        cost_estimate=cost(1e7),
        name="region_final",
    )(scalars, count, *regions)


def over_img(x, dy, dx):
    pairs = [
        (2 * y + xl, 2 * ((y + dy) % 4) + (xl ^ dx)) for y in range(4) for xl in range(2)
    ]
    return lax.ppermute(x, IMG, pairs)


def to_owner(x):
    axes = ("img_0",) + EMB
    return lax.ppermute(x, axes, [(4 * y + e, 4 * y + (e ^ y)) for y in range(4) for e in range(4)])


def along_cls(x, d):
    return lax.ppermute(x, CLS, [(i, (i + d) % 8) for i in range(8)])


def exchange(x, axes):
    return lax.all_to_all(x, axes, split_axis=0, concat_axis=0, tiled=True)


def shards(regions, table, shift, scale, labels, valid):
    rows = regions.shape[0]
    y = lax.axis_index("img_0")
    xl = lax.axis_index("img_1")
    xh = lax.axis_index("emb_0")
    k = lax.axis_index("emb_1")
    z = lax.axis_index(CLS)
    scalars = jnp.stack([k, z * 2688 + xh * 1344, 2 * xh + k, y, xl, z]).astype(jnp.int32)

    t_send = take_rows(pltpu.with_memory_space_constraint(table, pltpu.HBM), 4 * (1 - xh) + y, PART)
    t_send, regions_in = lax.optimization_barrier((t_send, regions))
    t_got = swap(t_send, "emb_0")
    r_far = swap(regions_in, "emb_0")
    r_near = swap(regions_in, "emb_1")
    local = jnp.broadcast_to(jnp.sum((labels >= 0).astype(F32)), (8, 128))
    local_other = swap(local, "img_1")
    t_far = exchange(make_message(t_got, local, local_other), "img_0")
    t_own = lax.dynamic_slice_in_dim(table, xh * 1344, 1344, 0)
    t_near = swap(t_own, "emb_1")
    r_both = swap(r_far, "emb_1")
    t_both = swap(t_far, "emb_1")
    blocks = (regions, r_near, r_far, r_both)
    tables = (t_own, t_near, t_far, t_both)
    unit, raw, inv = make_unit(blocks)

    lane_f = jnp.concatenate([shift[None], scale[None], jnp.zeros((6, rows), F32)], axis=0)
    mask = lax.dynamic_slice(valid, (k, xh * 1344), (1, 1344)).astype(F32).T
    keep, send, loss, count = make_focal(scalars, tables, unit, lane_f, labels[None], mask)

    theirs = swap(send, "emb_1")
    terms, kept = make_region(scalars, keep, send, tables, raw, inv)
    terms = exchange(terms, CLS)
    chunks = list(make_table(scalars, kept, theirs, unit, loss))
    for o in OVER_IMG:
        chunks[o] = over_img(chunks[o], o // 2, o % 2)
    table_part, loss_part = make_table_sum(chunks)
    table_part = to_owner(table_part)
    parts = list(make_merge(terms, loss_part))
    for q in range(1, 4):
        parts[q] = lax.ppermute(parts[q], EMB, [(i, i ^ q) for i in range(4)])
    message = make_gather(table_part)
    table_all = exchange(message, IMG)
    share = make_share(scalars, parts)
    shares = [share] * 8
    for d in ALONG_CLS:
        shares[d] = along_cls(share, d)
    table_grad = make_table_final(scalars, table_all)
    region_grad, total = make_region_final(scalars, count, shares)
    return (total[0, 0], region_grad.reshape(rows, 256), table_grad)


OVER_IMG = (3, 6, 5, 2, 7, 4, 1)
ALONG_CLS = (4, 3, 5, 2, 6, 1, 7)


def solution(mesh):
    torus = Mesh(
        mesh.devices.reshape(4, 2, mesh.shape["cls"], 2, 2),
        ("img_0", "img_1", "cls", "emb_0", "emb_1"),
    )
    return jax.shard_map(
        shards,
        mesh=torus,
        in_specs=(P(IMG, EMB), P(CLS, EMB), P(IMG), P(IMG), P(IMG), P(IMG, CLS)),
        out_specs=(P(), P(IMG, EMB), P(CLS, EMB)),
        check_vma=False,
    )
```
